256 devices in a mesh: dp: 32 (over z, x), fsdp: 8 (over y, core).
Axes of the slice: x: 4, y: 4, z: 8, core: 2. Of those that a mesh axis runs over, the one named last changes fastest.
Arguments:
- latents: bfloat16 [384, 2, 4096], P('dp'), may hold values from -6 to 6
- noise: bfloat16 [384, 2, 4096], P('dp'), may hold values from -6 to 6
- behavior_velocity: bfloat16 [384, 2, 4096], P('dp'), may hold values from -6 to 6
- timestep: int32 [384, 2], P('dp'), may hold values from 0 to 9
- reward_rank_integer: int32 [384], P('dp'), may hold values from 0 to 1023
- surviving_source_index: int32 [192], replicated, may hold values from 0 to 31, as said below
- surviving_slot_index: int32 [192], replicated, may hold values from 0 to 11, as said below
- group_kept_count: int32 [48], replicated, may hold values from 1 to 24, 192 in all
- patch_input_weight: bfloat16 [64, 1536], replicated, may hold values from -0.75 to 0.75
- modulation_lookup: float32 [10, 3, 1536], replicated, may hold values from -3 to 3
- up_projection_weight: bfloat16 [1536, 8192], P(None, 'fsdp'), may hold values from -0.15625 to 0.15625
- down_projection_weight: bfloat16 [1536, 8192], P(None, 'fsdp'), may hold values from -0.0625 to 0.0625
- velocity_head_weight: bfloat16 [1536, 64], replicated, may hold values from -0.15625 to 0.15625
Outputs:
- up_weight_gradient: float32 [1536, 8192], P('dp', 'fsdp')
- down_weight_gradient: float32 [1536, 8192], P('dp', 'fsdp')
- loss: float32 [], replicated
The draws below stay inside these ranges and needn't reach their ends.
Inputs may be any that keep to these rules, and one draw needn't show every extreme that they name: `surviving_source_index`: survivors are listed by source in ascending order; survivor j is trained on dp index j // 6, and every survivor of source d is trained on dp index d or d + 1. `surviving_slot_index`: the slots of one source's survivors are distinct.
All inputs are finite; a program needn't handle non-finite values.
Results may differ from the reference program's by a relative error of at most 0.013.
Values may be sent and summed in bfloat16 or wider, within the bound.
No kernel may reach another device: no remote copies, remote signals or barrier semaphores. Data moves between devices by JAX's collectives and lax.ppermute only.
A program may use at most 128 MiB of HBM per device.

```python
import math
import jax
import jax.numpy as jnp
import numpy as np
from jax import lax

D = 1536
FF = 8192
PATCH = 64
SEQ = 64
TRAINED_STEPS = 2
KSTEPS = 10
GROUP = 24
TRAJ_DEV = 6
SLOT_CAPACITY = 12
SURV = 192
PROMPTS = 48
N_DP = 32


def surviving_arrangement(key):
    base_key = jax.random.fold_in(key, 7)
    drifts = jax.random.randint(jax.random.fold_in(base_key, 1), (N_DP - 1,), 0, TRAJ_DEV + 1).astype(jnp.int32)
    nothing = jnp.zeros((1,), jnp.int32)
    drifts = jnp.concatenate([nothing, drifts, nothing])
    group_starts = jnp.arange(N_DP + 1, dtype=jnp.int32) * TRAJ_DEV + drifts
    positions = jnp.arange(N_DP * TRAJ_DEV, dtype=jnp.int32)
    source = jnp.sum((group_starts[None, 1:N_DP] <= positions[:, None]).astype(jnp.int32), axis=1)
    offset = positions - jnp.take(group_starts, source)
    scores = jax.random.randint(jax.random.fold_in(base_key, 2), (N_DP, SLOT_CAPACITY), 0, 1 << 20).astype(jnp.int32) * SLOT_CAPACITY + jnp.arange(SLOT_CAPACITY, dtype=jnp.int32)[None, :]
    ordering = jnp.argsort(scores, axis=1, stable=True).astype(jnp.int32)
    slot_ids = ordering[source, offset]
    return (source.astype(jnp.int32), slot_ids.astype(jnp.int32))


def draw_surviving_source_index(key, part):
    return surviving_arrangement(key)[0]


def draw_surviving_slot_index(key, part):
    return surviving_arrangement(key)[1]


def set_ends(entries, stream_key, least, top_value):
    longest = entries.shape.index(max(entries.shape))
    spots = []
    for shift in (0, 1):
        where = [jax.random.randint(jax.random.fold_in(stream_key, axis), (), 0, length) for axis, length in enumerate(entries.shape)]
        where[longest] = (where[longest] + shift) % entries.shape[longest]
        spots.append(tuple(where))
    return entries.at[spots[0]].set(least).at[spots[1]].set(top_value)


def block_levels(key, extent, shards, smallest, largest):
    gain, own = 1.0, jax.random.fold_in(key, 6)
    for axis_at, parts in shards:
        steps = jnp.exp(jax.random.uniform(jax.random.fold_in(own, axis_at), (parts,), jnp.float32, smallest / len(shards), largest / len(shards)))
        gain = gain * jnp.repeat(steps, extent[axis_at] // parts).reshape([-1 if axis == axis_at else 1 for axis in range(len(extent))])
    return gain


def split_up(amount, total, reach, skew):
    weights = [(1 << 20) // math.isqrt(rank ** skew) + 1 for rank in range(2, amount + 1)]
    surplus, given = total - reach - (amount - 1), [1] * (amount - 1)
    while surplus > 0:
        movable = [i for i in range(amount - 1) if given[i] < reach]
        pool, remaining = sum([weights[i] for i in movable]), surplus
        for i in movable:
            extra = min(reach - given[i], max(1, remaining * weights[i] // pool), surplus)
            given[i] = given[i] + extra
            surplus = surplus - extra
    return np.array([reach] + given)


def ragged(key, number_of, total, limit, skew):
    if number_of == 2:
        one = jax.random.randint(key, (), max(1, total - limit), min(limit, total - 1) + 1)
        return jnp.stack([one, total - one])
    tallies = jnp.asarray(split_up(number_of, total, limit, skew), jnp.int32)
    couples = (number_of - 1) // 2
    donor, receiver = tallies[1:1 + 2 * couples:2], tallies[2:2 + 2 * couples:2]
    room = jnp.minimum(donor - 1, limit - receiver)
    passed = jax.random.randint(jax.random.fold_in(key, 1), (couples,), 0, 1 << 20) % (room + 1)
    tallies = tallies.at[1:1 + 2 * couples:2].set(donor - passed).at[2:2 + 2 * couples:2].set(receiver + passed)
    return tallies[jax.random.permutation(jax.random.fold_in(key, 2), number_of)]


def centred(rng, extent, scale, most, cuts=(), held_as=jnp.bfloat16):
    array = jax.random.normal(rng, extent, jnp.float32) * scale
    if len(cuts) > 0:
        array = block_levels(rng, extent, cuts, -0.22, 0.18) * array
    return jnp.clip(array, min=-most, max=most).astype(held_as)


def setup_inputs(seed: int = 0) -> dict:
    keys = jax.random.split(jax.random.key(seed), 14)
    return {
        "latents": centred(keys[0], (N_DP * SLOT_CAPACITY, TRAINED_STEPS, SEQ * PATCH), 1.0, 6.0, ((0, 32),)),
        "noise": centred(keys[1], (N_DP * SLOT_CAPACITY, TRAINED_STEPS, SEQ * PATCH), 1.0, 6.0, ((0, 32),)),
        "behavior_velocity": centred(keys[2], (N_DP * SLOT_CAPACITY, TRAINED_STEPS, SEQ * PATCH), 1.0, 6.0, ((0, 32),)),
        "timestep": set_ends(jax.random.randint(keys[3], (N_DP * SLOT_CAPACITY, TRAINED_STEPS), 0, KSTEPS), jax.random.fold_in(keys[3], 1), 0, KSTEPS - 1).astype(jnp.int32),
        "reward_rank_integer": set_ends(jax.random.randint(keys[4], (N_DP * SLOT_CAPACITY,), 0, 1024), jax.random.fold_in(keys[4], 1), 0, 1023).astype(jnp.int32),
        "surviving_source_index": draw_surviving_source_index(jax.random.fold_in(keys[13], 71), 0),
        "surviving_slot_index": draw_surviving_slot_index(jax.random.fold_in(keys[13], 71), 0),
        "group_kept_count": ragged(keys[7], PROMPTS, SURV, GROUP, 2).astype(jnp.int32),
        "patch_input_weight": centred(keys[8], (PATCH, D), PATCH ** -0.5, 0.75),
        "modulation_lookup": centred(keys[9], (KSTEPS, 3, D), 0.5, 3.0, (), jnp.float32),
        "up_projection_weight": centred(keys[10], (D, FF), D ** -0.5, 0.15625, ((1, 8),)),
        "down_projection_weight": centred(keys[11], (D, FF), FF ** -0.5, 0.0625, ((1, 8),)),
        "velocity_head_weight": centred(keys[12], (D, PATCH), D ** -0.5, 0.15625),
    }


clip_range = 0.2
noise_level = 0.7
norm_eps = 1e-06

def step_ratio(indices, count):
    spacing = 1.0 / count
    level = 1.0 - indices.astype(jnp.float32) * spacing
    return jnp.sqrt(spacing * (1.0 - level + spacing) / level) / noise_level

def layer_norm(values):
    center = values - lax.optimization_barrier(jnp.mean(values, axis=-1, keepdims=True))
    variance = lax.optimization_barrier(jnp.mean(center * center, axis=-1, keepdims=True))
    inverse = lax.rsqrt(variance + norm_eps)
    return (center * inverse, inverse)

def smooth_gate(values):
    return jax.nn.gelu(values, approximate=True)

def membership_matrix(surviving_identifiers, kept_mask):
    group_ends = jnp.cumsum(kept_mask).astype(jnp.int32)
    group_starts = group_ends - kept_mask
    inside_clip_mask = (surviving_identifiers[:, None] >= group_starts[None, :]) & (surviving_identifiers[:, None] < group_ends[None, :])
    return inside_clip_mask.astype(jnp.int32)

def advantages(ranks, member_mask, kept_mask, sums):
    count = lax.optimization_barrier(jnp.sum(member_mask * kept_mask[None, :], axis=1))
    first = lax.optimization_barrier(jnp.sum(member_mask * sums[0][None, :], axis=1))
    second = lax.optimization_barrier(jnp.sum(member_mask * sums[1][None, :], axis=1))
    spread = (count * second - first * first).astype(jnp.float32)
    counts = count.astype(jnp.float32)
    deviation = jnp.sqrt(spread) / counts
    return (ranks.astype(jnp.float32) - first.astype(jnp.float32) / counts) / jnp.maximum(deviation, 1.0)

def reference(latents, noise, behavior_velocity, timestep, reward_rank_integer, surviving_source_index, surviving_slot_index, group_kept_count, patch_input_weight, modulation_lookup, up_projection_weight, down_projection_weight, velocity_head_weight):
    surviving_count = surviving_source_index.shape[0]
    picked_indices = (surviving_source_index * SLOT_CAPACITY + surviving_slot_index).astype(jnp.int32)
    ranks = jnp.take(reward_rank_integer, picked_indices)
    member_mask = membership_matrix(jnp.arange(surviving_count, dtype=jnp.int32), group_kept_count)
    sums = jnp.stack([lax.optimization_barrier(jnp.sum(member_mask * ranks[:, None], axis=0)), lax.optimization_barrier(jnp.sum(member_mask * (ranks * ranks)[:, None], axis=0))]).astype(jnp.int32)
    advantage = advantages(ranks, member_mask, group_kept_count, sums)
    width = patch_input_weight.shape[1]
    hidden_width = up_projection_weight.shape[1]
    contract = (((0,), (0,)), ((), ()))

    def visit_group(carry, index):
        up_weight_gradient, down_weight_gradient, total_count = carry
        pick = picked_indices[index]
        sample = lax.dynamic_index_in_dim(latents, pick, 0, False)
        drawn = lax.dynamic_index_in_dim(noise, pick, 0, False).astype(jnp.float32)
        target = lax.dynamic_index_in_dim(behavior_velocity, pick, 0, False).astype(jnp.float32)
        stamps = lax.dynamic_index_in_dim(timestep, pick, 0, False)
        advantage_gain = advantage[index]
        modulation = jnp.take(modulation_lookup, stamps, axis=0)
        inputs = sample.reshape(TRAINED_STEPS * SEQ, PATCH)
        embedded = jnp.dot(inputs, patch_input_weight, preferred_element_type=jnp.float32).reshape(TRAINED_STEPS, SEQ, width)
        normed, unused_value = layer_norm(embedded)
        modulated = (normed * (1.0 + modulation[:, 1][:, None]) + modulation[:, 0][:, None]).astype(jnp.bfloat16).reshape(TRAINED_STEPS * SEQ, width)
        pre = jnp.dot(modulated, up_projection_weight, preferred_element_type=jnp.float32)
        activated = smooth_gate(pre).astype(jnp.bfloat16)
        projected = lax.dot_general(activated, down_projection_weight, (((1,), (1,)), ((), ())), preferred_element_type=jnp.float32).reshape(TRAINED_STEPS, SEQ, width)
        gates = modulation[:, 2][:, None]
        mixed = embedded + gates * projected
        final, inverse = layer_norm(mixed)
        velocity = jnp.dot(final.astype(jnp.bfloat16).reshape(TRAINED_STEPS * SEQ, width), velocity_head_weight, preferred_element_type=jnp.float32).reshape(TRAINED_STEPS, SEQ * PATCH)
        coeff = step_ratio(stamps, KSTEPS)[:, None]
        error = velocity - target
        terms = coeff * drawn * error + 0.5 * coeff * coeff * error * error
        logratio = -lax.optimization_barrier(jnp.mean(terms, axis=1))
        likelihood_ratio = jnp.exp(logratio)
        clipped = jnp.clip(likelihood_ratio, 1.0 - clip_range, 1.0 + clip_range)
        plain = likelihood_ratio * advantage_gain
        bounded = clipped * advantage_gain
        unit_loss = -jnp.minimum(plain, bounded)
        live_mask = (plain <= bounded).astype(jnp.float32)
        loss_slope = (-advantage_gain * likelihood_ratio * live_mask / (surviving_count * TRAINED_STEPS))[:, None]
        dvelocity = (loss_slope * (-(coeff * drawn + coeff * coeff * error) / (SEQ * PATCH))).astype(jnp.bfloat16).reshape(TRAINED_STEPS * SEQ, PATCH)
        dfinal = lax.dot_general(dvelocity, velocity_head_weight, (((1,), (1,)), ((), ())), preferred_element_type=jnp.float32).reshape(TRAINED_STEPS, SEQ, width)
        dmixed = inverse * (dfinal - lax.optimization_barrier(jnp.mean(dfinal, axis=-1, keepdims=True)) - final * lax.optimization_barrier(jnp.mean(dfinal * final, axis=-1, keepdims=True)))
        upstream = (gates * dmixed).astype(jnp.bfloat16).reshape(TRAINED_STEPS * SEQ, width)
        down_weight_gradient = down_weight_gradient + lax.dot_general(upstream, activated, contract, preferred_element_type=jnp.float32)
        dactivated = jnp.dot(upstream, down_projection_weight, preferred_element_type=jnp.float32)
        unused_value, pull = jax.vjp(smooth_gate, pre)
        dpre = pull(dactivated)[0].astype(jnp.bfloat16)
        up_weight_gradient = up_weight_gradient + lax.dot_general(modulated, dpre, contract, preferred_element_type=jnp.float32)
        return ((up_weight_gradient, down_weight_gradient, total_count + jnp.sum(unit_loss)), None)
    group_start = (jnp.zeros((width, hidden_width), jnp.float32), jnp.zeros((width, hidden_width), jnp.float32), jnp.zeros((), jnp.float32))
    (up_weight_gradient, down_weight_gradient, total_count), unused_value = lax.scan(visit_group, group_start, jnp.arange(surviving_count, dtype=jnp.int32))
    return (up_weight_gradient, down_weight_gradient, total_count / (surviving_count * TRAINED_STEPS))
```

```python
import jax
import jax.numpy as jnp
from jax import lax
from jax.sharding import Mesh
from jax.sharding import PartitionSpec as P

KSTEPS = 10
DP = ("z", "x")
clip_range = 0.2
noise_level = 0.7
norm_eps = 1e-06
bf16 = jnp.bfloat16
f32 = jnp.float32


def move(value, axis, steps):
    count = lax.axis_size(axis)
    return lax.ppermute(value, axis, [(i, (i + steps) % count) for i in range(count)])


def swap(value, axis, bit):
    count = lax.axis_size(axis)
    return lax.ppermute(value, axis, [(i, i ^ bit) for i in range(count)])


def butterfly(value):
    for axis, bits in (("x", (1, 2)), ("z", (1, 2, 4))):
        for bit in bits:
            value = value + swap(value, axis, bit)
    return value


def step_ratio(indices, count):
    spacing = 1.0 / count
    level = 1.0 - indices.astype(f32) * spacing
    return jnp.sqrt(spacing * (1.0 - level + spacing) / level) / noise_level


def layer_norm(values):
    center = values - jnp.mean(values, axis=-1, keepdims=True)
    variance = jnp.mean(center * center, axis=-1, keepdims=True)
    inverse = lax.rsqrt(variance + norm_eps)
    return (center * inverse, inverse)


def smooth_gate(values):
    return jax.nn.gelu(values, approximate=True)


def membership_matrix(identifiers, kept):
    ends = jnp.cumsum(kept)
    starts = ends - kept
    inside = (identifiers[:, None] >= starts[None, :]) & (identifiers[:, None] < ends[None, :])
    return inside.astype(jnp.int32)


def advantages(ranks, member, kept, sums):
    count = jnp.sum(member * kept[None, :], axis=1)
    first = jnp.sum(member * sums[0][None, :], axis=1)
    second = jnp.sum(member * sums[1][None, :], axis=1)
    spread = (count * second - first * first).astype(f32)
    counts = count.astype(f32)
    deviation = jnp.sqrt(spread) / counts
    return (ranks.astype(f32) - first.astype(f32) / counts) / jnp.maximum(deviation, 1.0)


def rs_four(get, axis):
    def half(v, h):
        n = v.shape[-1] // 2
        return v[..., h * n : (h + 1) * n]

    down = jnp.stack([half(get(3), 1), half(get(2), 0)]).astype(bf16)
    up = jnp.stack([half(get(1), 0), half(get(2), 1)]).astype(bf16)
    from_up = move(down, axis, -1)
    from_down = move(up, axis, 1)
    second_down = (half(get(3), 0).astype(f32) + from_up[1].astype(f32)).astype(bf16)
    second_up = (half(get(1), 1).astype(f32) + from_down[1].astype(f32)).astype(bf16)
    late_up = move(second_down, axis, -1)
    late_down = move(second_up, axis, 1)
    low = half(get(0), 0).astype(f32) + from_down[0].astype(f32) + late_up.astype(f32)
    high = half(get(0), 1).astype(f32) + from_up[0].astype(f32) + late_down.astype(f32)
    return jnp.concatenate([low, high], axis=-1)


def rs_eight(get, axis):
    n = get(0).shape[-1] // 2
    from_up = move(get(4)[..., :n].astype(bf16), axis, -1)
    from_down = move(get(4)[..., n:].astype(bf16), axis, 1)
    zero = jnp.zeros_like(from_up)
    down = (get(5).astype(f32) + jnp.concatenate([from_up, zero], axis=-1).astype(f32)).astype(bf16)
    up = (get(3).astype(f32) + jnp.concatenate([zero, from_down], axis=-1).astype(f32)).astype(bf16)
    for step in (2, 1):
        from_up = move(down, axis, -1)
        from_down = move(up, axis, 1)
        down = (get(8 - step).astype(f32) + from_up.astype(f32)).astype(bf16)
        up = (get(step).astype(f32) + from_down.astype(f32)).astype(bf16)
    from_up = move(down, axis, -1)
    from_down = move(up, axis, 1)
    return get(0).astype(f32) + from_up.astype(f32) + from_down.astype(f32)


def sum_over_hidden(projected):
    half = projected.shape[0] // 2
    width = projected.shape[1]
    got = swap(projected[:half].astype(bf16), "c", 1)
    mine = (projected[half:] + got.astype(f32)).reshape(4, half // 4, width)
    own = rs_four(lambda k: mine[k], "y").astype(bf16)
    after = move(own, "y", -1)
    before = move(own, "y", 1)
    n = width // 2
    far_low = move(after[:, :n], "y", -1)
    far_high = move(before[:, n:], "y", 1)
    far = jnp.concatenate([far_low, far_high], axis=1)
    rows = jnp.concatenate([own, after, far, before], axis=0)
    return jnp.concatenate([swap(rows, "c", 1), rows], axis=0)


def shards(
    latents,
    noise,
    behavior_velocity,
    timestep,
    reward_rank_integer,
    surviving_source_index,
    surviving_slot_index,
    group_kept_count,
    patch_input_weight,
    modulation_lookup,
    up_projection_weight,
    down_projection_weight,
    velocity_head_weight,
):
    z, x, y, c = (lax.axis_index(a) for a in ("z", "x", "y", "c"))
    owner = lax.axis_index(DP)
    ranks_dp = lax.axis_size(DP)
    surviving = surviving_source_index.shape[0]
    trajs = surviving // ranks_dp
    steps = timestep.shape[1]
    lead = owner * trajs
    sources = lax.dynamic_slice_in_dim(surviving_source_index, lead, trajs)
    slots = lax.dynamic_slice_in_dim(surviving_slot_index, lead, trajs)
    next_lead = jnp.minimum(owner + 1, ranks_dp - 1) * trajs
    next_slots = lax.dynamic_slice_in_dim(surviving_slot_index, next_lead, trajs)
    capacity = latents.shape[0]

    def pairs(a):
        return a.reshape(capacity, steps, 32, 128).transpose(0, 2, 1, 3).reshape(capacity, 64, 128)

    small = jnp.concatenate([timestep, reward_rank_integer[:, None]], axis=1)
    local = (pairs(latents), pairs(noise), pairs(behavior_velocity), small)
    outgoing = tuple(jnp.take(a, next_slots, axis=0) for a in local)
    onward = [(i, i + 1) for i in range(ranks_dp - 1)]
    arrived = tuple(lax.ppermute(a, DP, onward) for a in outgoing)
    left = sources != owner
    samples, noises, olds, small = (
        jnp.where(left.reshape((trajs,) + (1,) * (mine.ndim - 1)), came, mine)
        for came, mine in zip(arrived, (jnp.take(a, slots, axis=0) for a in local))
    )
    stamps, ranks = small[:, :steps], small[:, steps]
    member = membership_matrix(lead + jnp.arange(trajs, dtype=jnp.int32), group_kept_count)
    partial = jnp.stack(
        [jnp.sum(member * ranks[:, None], axis=0), jnp.sum(member * (ranks * ranks)[:, None], axis=0)]
    ).astype(jnp.int32)
    advantage = advantages(ranks, member, group_kept_count, butterfly(partial))

    ks = (y + jnp.arange(4, dtype=jnp.int32)) % 4 * 2
    order = jnp.concatenate([ks + (1 - c), ks + c])

    def ordered(a):
        return jnp.take(a.reshape(trajs, 8, 8, 128), order, axis=1).transpose(1, 0, 2, 3)

    width = patch_input_weight.shape[1]
    patch = patch_input_weight.shape[0]
    rows = 8 * 2 * trajs * 8
    blank = jnp.zeros_like(patch_input_weight)
    wide_in = [
        jnp.concatenate([patch_input_weight, blank], axis=0),
        jnp.concatenate([blank, patch_input_weight], axis=0),
    ]
    blank = jnp.zeros_like(velocity_head_weight)
    wide_head = [
        jnp.concatenate([velocity_head_weight, blank], axis=1),
        jnp.concatenate([blank, velocity_head_weight], axis=1),
    ]
    tokens = ordered(samples).reshape(8, trajs * 8, 128)
    embedded = jnp.stack(
        [jnp.dot(tokens, w, preferred_element_type=f32) for w in wide_in], axis=1
    ).reshape(8, 2, trajs, 8, width)
    stamp_rows = jnp.tile(stamps, (1, 4))
    modulation = jnp.take(modulation_lookup, stamp_rows, axis=0)
    shift, scale, gate = (modulation[:, :, i] for i in range(3))
    normed, _ = layer_norm(embedded)
    modulated = (normed * (1.0 + scale) + shift).astype(bf16).reshape(rows, width)
    pre = jnp.dot(modulated, up_projection_weight, preferred_element_type=f32)
    activated = smooth_gate(pre).astype(bf16)
    projected = lax.dot_general(
        activated, down_projection_weight, (((1,), (1,)), ((), ())), preferred_element_type=f32
    )
    summed = sum_over_hidden(projected).astype(f32).reshape(8, 2, trajs, 8, width)

    mixed = embedded + gate * summed
    final, inverse = layer_norm(mixed)
    final_rows = final.astype(bf16).reshape(8, 2, trajs * 8, width)
    velocity = sum(
        jnp.dot(final_rows[:, i], wide_head[i], preferred_element_type=f32) for i in range(2)
    )
    target = ordered(olds).astype(f32)
    drawn = ordered(noises).astype(f32)
    coeff = step_ratio(stamps, KSTEPS)
    coeff_rows = jnp.tile(coeff, (1, 4))[:, :, None]
    error = velocity.reshape(8, trajs, 8, 128) - target
    terms = coeff_rows * drawn * error + 0.5 * coeff_rows * coeff_rows * error * error
    unit_sums = jnp.sum(jnp.sum(terms, axis=(0, 3)).reshape(trajs, 4, steps), axis=1)
    values = 64 * patch
    gain = advantage[:, None]
    likelihood_ratio = jnp.exp(-unit_sums / values)
    clipped = jnp.clip(likelihood_ratio, 1.0 - clip_range, 1.0 + clip_range)
    plain = likelihood_ratio * gain
    bounded = clipped * gain
    live = (plain <= bounded).astype(f32)
    slope = -gain * likelihood_ratio * live / (surviving * steps)
    loss = butterfly(-jnp.sum(jnp.minimum(plain, bounded))) / (surviving * steps)
    slope_rows = jnp.tile(slope, (1, 4))[:, :, None]
    dvelocity = (
        (slope_rows * (-(coeff_rows * drawn + coeff_rows * coeff_rows * error) / values))
        .astype(bf16)
        .reshape(8, trajs * 8, 128)
    )
    dfinal = jnp.stack(
        [
            lax.dot_general(dvelocity, w, (((2,), (1,)), ((), ())), preferred_element_type=f32)
            for w in wide_head
        ],
        axis=1,
    ).reshape(8, 2, trajs, 8, width)
    dmixed = inverse * (
        dfinal
        - jnp.mean(dfinal, axis=-1, keepdims=True)
        - final * jnp.mean(dfinal * final, axis=-1, keepdims=True)
    )
    upstream = (gate * dmixed).astype(bf16).reshape(rows, width)
    contract = (((0,), (0,)), ((), ()))
    down_partial = lax.dot_general(
        upstream, activated, contract, preferred_element_type=f32
    ).astype(bf16)
    dactivated = jnp.dot(upstream, down_projection_weight, preferred_element_type=f32)
    _, pull = jax.vjp(smooth_gate, pre)
    dpre = pull(dactivated)[0].astype(bf16)
    up_partial = lax.dot_general(
        modulated, dpre, contract, preferred_element_type=f32
    ).astype(bf16)

    hidden = up_projection_weight.shape[1]
    own = width // ranks_dp
    down_parts = down_partial.reshape(8, 4, own, hidden)
    up_parts = up_partial.reshape(8, 4, own, hidden)

    def part(array, index, dim):
        return lax.dynamic_index_in_dim(array, index, dim, False)

    down_z = rs_eight(lambda k: part(down_parts, (z + k) % 8, 0), "z")
    up_x = rs_four(lambda k: part(up_parts, (x + k) % 4, 1), "x")
    down_grad = rs_four(lambda k: part(down_z, (x + k) % 4, 0), "x")
    up_grad = rs_eight(lambda k: part(up_x, (z + k) % 8, 0), "z")
    return (up_grad, down_grad, loss)


def solution(mesh):
    finer = Mesh(mesh.devices.reshape(8, 4, 4, 2), ("z", "x", "y", "c"))
    dp, fsdp = ("z", "x"), ("y", "c")
    in_specs = (
        P(dp, None, None),
        P(dp, None, None),
        P(dp, None, None),
        P(dp, None),
        P(dp),
        P(),
        P(),
        P(),
        P(),
        P(),
        P(None, fsdp),
        P(None, fsdp),
        P(),
    )
    out_specs = (P(dp, fsdp), P(dp, fsdp), P())
    return jax.shard_map(
        shards, mesh=finer, in_specs=in_specs, out_specs=out_specs, check_vma=False
    )
```

```python
import jax
import jax.numpy as jnp
from jax import lax
from jax.experimental import pallas as pl
from jax.experimental.pallas import tpu as pltpu
from jax.sharding import Mesh
from jax.sharding import PartitionSpec as P

KSTEPS = 10
DP = ("z", "x")
clip_range = 0.2
noise_level = 0.7
norm_eps = 1e-06
bf16 = jnp.bfloat16
f32 = jnp.float32


def move(value, axis, steps):
    count = lax.axis_size(axis)
    return lax.ppermute(value, axis, [(i, (i + steps) % count) for i in range(count)])


def swap(value, axis, bit):
    count = lax.axis_size(axis)
    return lax.ppermute(value, axis, [(i, i ^ bit) for i in range(count)])


def sent_to_all(value, axis):
    count = lax.axis_size(axis)
    return lax.all_to_all(jnp.broadcast_to(value[None], (count, *value.shape)), axis, 0, 0, tiled=True)


def sent_over_dp(value):
    return sent_to_all(sent_to_all(value, "x"), "z")


def smooth_gate(values):
    return jax.nn.gelu(values, approximate=True)


TRAJS = 6
PAIRS = 64
TILE = 8
BLOCK = TRAJS * TILE
CHUNKS = 8


def gather_kernel(slots, stamps, latents, noise, behavior, out_first, out_second, own_first, own_second, sems):
    copies = []
    for j in range(2 * TRAJS):
        slot = slots[j]
        first, second = (out_first, out_second) if j < TRAJS else (own_first, own_second)
        k = j % TRAJS
        for i, (source, target) in enumerate(
            ((latents, first.at[k, pl.ds(0, PAIRS)]), (noise, second.at[k, 0]), (behavior, second.at[k, 1]))
        ):
            copy = pltpu.make_async_copy(source.at[slot], target, sems.at[3 * j + i])
            copy.start()
            copies.append(copy)
    step = lax.broadcasted_iota(jnp.int32, (16, 128), 0) % 2
    for j in range(2 * TRAJS):
        slot = slots[j]
        tile = jnp.where(step == 0, stamps[slot, 0], stamps[slot, 1])
        first = out_first if j < TRAJS else own_first
        first[j % TRAJS, pl.ds(PAIRS, 16), :] = tile.astype(f32).astype(bf16)
    for copy in copies:
        copy.wait()


def modulation_rows(stamp_tile, lookup, index):
    rows = jnp.zeros((TILE, lookup.shape[2]), f32)
    for k in range(KSTEPS):
        rows = jnp.where(stamp_tile == k, lookup[k, pl.ds(index, 1), :], rows)
    return rows


def widened(weight, wide, dim):
    size = weight.shape[dim]
    wide[...] = jnp.zeros(wide.shape, wide.dtype)
    if dim == 0:
        wide[0, pl.ds(0, size), :] = weight[...]
        wide[1, pl.ds(size, size), :] = weight[...]
    else:
        wide[0, :, pl.ds(0, size)] = weight[...]
        wide[1, :, pl.ds(size, size)] = weight[...]


def embed_kernel(left, order, came, mine, weight, lookup, modulated, tokens, stamps, merged, sorted_, wide, emb, scale, shift):
    width = weight.shape[1]
    for j in range(TRAJS):
        merged[pl.ds(j * 80, 80), :] = jnp.where(left[j] != 0, came[j].astype(f32), mine[j].astype(f32))
    for q in range(CHUNKS):
        for j in range(TRAJS):
            at = pl.multiple_of(j * 80 + order[q] * TILE, TILE)
            sorted_[pl.ds(q * BLOCK + j * TILE, TILE), :] = merged[pl.ds(at, TILE), :]
    tokens[...] = sorted_[...].astype(bf16)
    widened(weight, wide, 0)
    for par in range(2):
        emb[par] = jnp.dot(tokens[...], wide[par], preferred_element_type=f32)
    for j in range(TRAJS):
        stamp = merged[pl.ds(j * 80 + PAIRS, TILE), :]
        stamps[pl.ds(j * TILE, TILE), :] = stamp
        stamp = stamp[:, :1]
        shift[pl.ds(j * TILE, TILE), :] = modulation_rows(stamp, lookup, 0)
        scale[pl.ds(j * TILE, TILE), :] = 1.0 + modulation_rows(stamp, lookup, 1)

    def chunk(q, carry):
        for par in range(2):
            values = emb[par, pl.ds(pl.multiple_of(q * BLOCK, BLOCK), BLOCK), :]
            center = values - jnp.sum(values, axis=1, keepdims=True) * (1.0 / width)
            variance = jnp.sum(center * center, axis=1, keepdims=True) * (1.0 / width)
            normed = center * lax.rsqrt(variance + norm_eps)
            at = pl.multiple_of(q * (2 * BLOCK) + par * BLOCK, BLOCK)
            modulated[pl.ds(at, BLOCK), :] = (normed * scale[...] + shift[...]).astype(bf16)
        return carry

    lax.fori_loop(0, CHUNKS, chunk, 0)


def head_kernel(
    left, order, gains, other, own, tokens, stamps, came, mine, weight, head, lookup,
    upstream, loss,
    drawn, target, wide, wide_head, emb, rounded, back, inverse, gate, error, slope, coeff,
):
    width = weight.shape[1]
    values = SEQ_VALUES
    widened(weight, wide, 0)
    widened(head, wide_head, 1)
    for j in range(TRAJS):
        stamp = stamps[pl.ds(j * TILE, TILE), :]
        gate[pl.ds(j * TILE, TILE), :] = modulation_rows(stamp[:, :1], lookup, 2)
        level = 1.0 - stamp * (1.0 / KSTEPS)
        coeff[pl.ds(j * TILE, TILE), :] = (
            jnp.sqrt((1.0 / KSTEPS) * (1.0 - level + 1.0 / KSTEPS) / level) / noise_level
        )
        picked = jnp.where(left[j] != 0, came[j].astype(f32), mine[j].astype(f32))
        emb[0, pl.ds(0, PAIRS), pl.ds(0, 128)] = picked[0]
        emb[0, pl.ds(PAIRS, PAIRS), pl.ds(0, 128)] = picked[1]
        for q in range(CHUNKS):
            at = pl.multiple_of(order[q] * TILE, TILE)
            drawn[pl.ds(q * BLOCK + j * TILE, TILE), :] = emb[0, pl.ds(at, TILE), pl.ds(0, 128)]
            at = pl.multiple_of(PAIRS + order[q] * TILE, TILE)
            target[pl.ds(q * BLOCK + j * TILE, TILE), :] = emb[0, pl.ds(at, TILE), pl.ds(0, 128)]
    for par in range(2):
        emb[par] = jnp.dot(tokens[...], wide[par], preferred_element_type=f32)

    def forward(q, summed):
        for par in range(2):
            rows = pl.ds(pl.multiple_of(q * BLOCK, BLOCK), BLOCK)
            at = pl.multiple_of((q % 4) * (2 * BLOCK) + par * BLOCK, BLOCK)
            mixed = emb[par, rows, :] + gate[...] * summed[pl.ds(at, BLOCK), :].astype(f32)
            center = mixed - jnp.sum(mixed, axis=1, keepdims=True) * (1.0 / width)
            variance = jnp.sum(center * center, axis=1, keepdims=True) * (1.0 / width)
            scale = lax.rsqrt(variance + norm_eps)
            final = center * scale
            emb[par, rows, :] = final
            rounded[par, rows, :] = final.astype(bf16)
            inverse[par, rows, :] = jnp.broadcast_to(scale, (BLOCK, 128))

    def first_half(q, carry):
        forward(q, other)
        return carry

    def second_half(q, carry):
        forward(q + 4, own)
        return carry

    lax.fori_loop(0, 4, first_half, 0)
    lax.fori_loop(0, 4, second_half, 0)
    velocity = jnp.dot(rounded[0], wide_head[0], preferred_element_type=f32)
    error[...] = velocity + jnp.dot(rounded[1], wide_head[1], preferred_element_type=f32) - target[...]
    total = jnp.zeros((BLOCK, 128), f32)
    c = coeff[...]
    for q in range(CHUNKS):
        rows = pl.ds(q * BLOCK, BLOCK)
        err = error[rows, :]
        total = total + c * drawn[rows, :] * err + 0.5 * c * c * err * err
    sums = jnp.broadcast_to(jnp.sum(total, axis=1, keepdims=True), (BLOCK, 128))
    losses = jnp.zeros((TILE, 128), f32)
    for j in range(TRAJS):
        unit = sums[j * TILE : (j + 1) * TILE]
        unit = unit + pltpu.roll(unit, 4, 0)
        unit = unit + pltpu.roll(unit, 2, 0)
        ratio = jnp.exp(-unit / values)
        clipped = jnp.clip(ratio, 1.0 - clip_range, 1.0 + clip_range)
        plain = ratio * gains[j]
        bounded = clipped * gains[j]
        losses = losses - jnp.minimum(plain, bounded)
        live = jnp.where(plain <= bounded, 1.0, 0.0)
        slope[pl.ds(j * TILE, TILE), :] = -gains[j] * ratio * live * (1.0 / UNITS)
    loss[...] = losses
    bent = slope[...]
    for q in range(CHUNKS):
        rows = pl.ds(q * BLOCK, BLOCK)
        error[rows, :] = bent * (-(c * drawn[rows, :] + c * c * error[rows, :]) / values)
    dvelocity = error[...].astype(bf16)
    for par in range(2):
        back[par] = lax.dot_general(
            dvelocity, wide_head[par], (((1,), (1,)), ((), ())), preferred_element_type=f32
        )

    def backward(q, carry):
        for par in range(2):
            rows = pl.ds(pl.multiple_of(q * BLOCK, BLOCK), BLOCK)
            d = back[par, rows, :]
            final = emb[par, rows, :]
            mean = jnp.sum(d, axis=1, keepdims=True) * (1.0 / width)
            along = jnp.sum(d * final, axis=1, keepdims=True) * (1.0 / width)
            dmixed = inverse[par, rows, :][:, :1] * (d - mean - final * along)
            at = pl.multiple_of(q * (2 * BLOCK) + par * BLOCK, BLOCK)
            upstream[pl.ds(at, BLOCK), :] = (gate[...] * dmixed).astype(bf16)
        return carry

    lax.fori_loop(0, CHUNKS, backward, 0)


SEQ_VALUES = 4096
UNITS = 384
SMEM = pl.BlockSpec(memory_space=pltpu.SMEM)
VMEM = pl.BlockSpec(memory_space=pltpu.VMEM)
HBM = pl.BlockSpec(memory_space=pl.ANY)


def rs_four(get, axis):
    def half(v, h):
        n = v.shape[-1] // 2
        return v[..., h * n : (h + 1) * n]

    down = jnp.stack([half(get(3), 1), half(get(2), 0)]).astype(bf16)
    up = jnp.stack([half(get(1), 0), half(get(2), 1)]).astype(bf16)
    from_up = move(down, axis, -1)
    from_down = move(up, axis, 1)
    second_down = (half(get(3), 0).astype(f32) + from_up[1].astype(f32)).astype(bf16)
    second_up = (half(get(1), 1).astype(f32) + from_down[1].astype(f32)).astype(bf16)
    late_up = move(second_down, axis, -1)
    late_down = move(second_up, axis, 1)
    low = half(get(0), 0).astype(f32) + from_down[0].astype(f32) + late_up.astype(f32)
    high = half(get(0), 1).astype(f32) + from_up[0].astype(f32) + late_down.astype(f32)
    return jnp.concatenate([low, high], axis=-1)


def rs_eight(get, axis):
    n = get(0).shape[-1] // 2
    from_up = move(get(4)[..., :n].astype(bf16), axis, -1)
    from_down = move(get(4)[..., n:].astype(bf16), axis, 1)
    zero = jnp.zeros_like(from_up)
    down = (get(5).astype(f32) + jnp.concatenate([from_up, zero], axis=-1).astype(f32)).astype(bf16)
    up = (get(3).astype(f32) + jnp.concatenate([zero, from_down], axis=-1).astype(f32)).astype(bf16)
    for step in (2, 1):
        from_up = move(down, axis, -1)
        from_down = move(up, axis, 1)
        down = (get(8 - step).astype(f32) + from_up.astype(f32)).astype(bf16)
        up = (get(step).astype(f32) + from_down.astype(f32)).astype(bf16)
    from_up = move(down, axis, -1)
    from_down = move(up, axis, 1)
    return get(0).astype(f32) + from_up.astype(f32) + from_down.astype(f32)


def sum_over_hidden(projected):
    half = projected.shape[0] // 2
    width = projected.shape[1]
    got = swap(projected[:half].astype(bf16), "c", 1)
    mine = (projected[half:] + got.astype(f32)).reshape(4, half // 4, width)
    own = rs_four(lambda k: mine[k], "y").astype(bf16)
    after = move(own, "y", -1)
    before = move(own, "y", 1)
    n = width // 2
    far_low = move(after[:, :n], "y", -1)
    far_high = move(before[:, n:], "y", 1)
    far = jnp.concatenate([far_low, far_high], axis=1)
    rows = jnp.concatenate([own, after, far, before], axis=0)
    return swap(rows, "c", 1), rows


def shards(
    latents,
    noise,
    behavior_velocity,
    timestep,
    reward_rank_integer,
    surviving_source_index,
    surviving_slot_index,
    group_kept_count,
    patch_input_weight,
    modulation_lookup,
    up_projection_weight,
    down_projection_weight,
    velocity_head_weight,
):
    z, x, y, c = (lax.axis_index(a) for a in ("z", "x", "y", "c"))
    owner = lax.axis_index(DP)
    ranks_dp = lax.axis_size(DP)
    surviving = surviving_source_index.shape[0]
    trajs = surviving // ranks_dp
    steps = timestep.shape[1]
    lead = owner * trajs
    sources = lax.dynamic_slice_in_dim(surviving_source_index, lead, trajs)
    slots = lax.dynamic_slice_in_dim(surviving_slot_index, lead, trajs)
    next_lead = jnp.minimum(owner + 1, ranks_dp - 1) * trajs
    next_slots = lax.dynamic_slice_in_dim(surviving_slot_index, next_lead, trajs)
    capacity = latents.shape[0]

    def pairs(a):
        return a.reshape(capacity, steps, 32, 128).transpose(0, 2, 1, 3).reshape(capacity, 64, 128)

    width = patch_input_weight.shape[1]
    rows = 8 * 2 * trajs * 8
    one = jax.ShapeDtypeStruct((TRAJS, 80, 128), bf16)
    two = jax.ShapeDtypeStruct((TRAJS, 2, PAIRS, 128), bf16)
    out_first, out_second, own_first, own_second = pl.pallas_call(
        gather_kernel,
        out_shape=(one, two, one, two),
        in_specs=[SMEM, SMEM, HBM, HBM, HBM],
        out_specs=(VMEM, VMEM, VMEM, VMEM),
        scratch_shapes=[pltpu.SemaphoreType.DMA((6 * TRAJS,))],
        name="gather_slots",
    )(
        jnp.concatenate([next_slots, slots]), timestep,
        pairs(latents), pairs(noise), pairs(behavior_velocity),
    )
    onward = [(i, i + 1) for i in range(ranks_dp - 1)]
    came = lax.ppermute(out_first, DP, onward)
    came_late = lax.ppermute(out_second, DP, onward)
    left = (sources != owner).astype(jnp.int32)
    ks = (y + jnp.arange(4, dtype=jnp.int32)) % 4 * 2
    order = jnp.concatenate([ks + (1 - c), ks + c])
    modulated, tokens, stamps = pl.pallas_call(
        embed_kernel,
        out_shape=(
            jax.ShapeDtypeStruct((rows, width), bf16),
            jax.ShapeDtypeStruct((CHUNKS * BLOCK, 128), bf16),
            jax.ShapeDtypeStruct((BLOCK, 128), f32),
        ),
        in_specs=[SMEM, SMEM, VMEM, VMEM, VMEM, VMEM],
        out_specs=(VMEM, VMEM, VMEM),
        scratch_shapes=[
            pltpu.VMEM((TRAJS * 80, 128), f32),
            pltpu.VMEM((CHUNKS * BLOCK, 128), f32),
            pltpu.VMEM((2, 128, width), bf16),
            pltpu.VMEM((2, CHUNKS * BLOCK, width), f32),
            pltpu.VMEM((BLOCK, width), f32),
            pltpu.VMEM((BLOCK, width), f32),
        ],
        compiler_params=pltpu.CompilerParams(vmem_limit_bytes=48 << 20),
        name="embed_and_modulate",
    )(left, order, came, own_first, patch_input_weight, modulation_lookup)

    table = sent_over_dp(reward_rank_integer).reshape(ranks_dp * capacity)
    ranks = jnp.take(table, surviving_source_index * capacity + surviving_slot_index)
    ends = jnp.cumsum(group_kept_count)
    begins = ends - group_kept_count
    here = lead + jnp.arange(trajs, dtype=jnp.int32)
    inside = ((here[:, None] >= begins[None, :]) & (here[:, None] < ends[None, :])).astype(jnp.int32)
    count = jnp.sum(inside * group_kept_count[None, :], axis=1)
    begin = jnp.sum(inside * begins[None, :], axis=1)
    everyone = jnp.arange(surviving, dtype=jnp.int32)[None, :]
    same = ((everyone >= begin[:, None]) & (everyone < (begin + count)[:, None])).astype(jnp.int32)
    total = jnp.sum(same * ranks[None, :], axis=1)
    squares = jnp.sum(same * (ranks * ranks)[None, :], axis=1)
    own_rank = jnp.sum((everyone == here[:, None]).astype(jnp.int32) * ranks[None, :], axis=1)
    counts = count.astype(f32)
    deviation = jnp.sqrt((count * squares - total * total).astype(f32)) / counts
    advantage = (own_rank.astype(f32) - total.astype(f32) / counts) / jnp.maximum(deviation, 1.0)

    pre = jnp.dot(modulated, up_projection_weight, preferred_element_type=f32)
    activated = smooth_gate(pre).astype(bf16)
    projected = lax.dot_general(
        activated, down_projection_weight, (((1,), (1,)), ((), ())), preferred_element_type=f32
    )
    summed_other, summed_own = sum_over_hidden(projected)
    upstream, losses = pl.pallas_call(
        head_kernel,
        out_shape=(
            jax.ShapeDtypeStruct((rows, width), bf16),
            jax.ShapeDtypeStruct((TILE, 128), f32),
        ),
        in_specs=[SMEM, SMEM, SMEM] + [VMEM] * 9,
        out_specs=(VMEM, VMEM),
        scratch_shapes=[
            pltpu.VMEM((CHUNKS * BLOCK, 128), f32),
            pltpu.VMEM((CHUNKS * BLOCK, 128), f32),
            pltpu.VMEM((2, 128, width), bf16),
            pltpu.VMEM((2, width, 128), bf16),
            pltpu.VMEM((2, CHUNKS * BLOCK, width), f32),
            pltpu.VMEM((2, CHUNKS * BLOCK, width), bf16),
            pltpu.VMEM((2, CHUNKS * BLOCK, width), f32),
            pltpu.VMEM((2, CHUNKS * BLOCK, 128), f32),
            pltpu.VMEM((BLOCK, width), f32),
            pltpu.VMEM((CHUNKS * BLOCK, 128), f32),
            pltpu.VMEM((BLOCK, 128), f32),
            pltpu.VMEM((BLOCK, 128), f32),
        ],
        compiler_params=pltpu.CompilerParams(vmem_limit_bytes=56 << 20),
        name="head_both_ways",
    )(
        left, order, advantage, summed_other, summed_own, tokens, stamps, came_late, own_second,
        patch_input_weight, velocity_head_weight, modulation_lookup,
    )
    loss = jnp.sum(sent_over_dp(losses[:2, 0])) / UNITS
    contract = (((0,), (0,)), ((), ()))
    down_partial = lax.dot_general(
        upstream, activated, contract, preferred_element_type=f32
    ).astype(bf16)
    dactivated = jnp.dot(upstream, down_projection_weight, preferred_element_type=f32)
    _, pull = jax.vjp(smooth_gate, pre)
    dpre = pull(dactivated)[0].astype(bf16)
    up_partial = lax.dot_general(
        modulated, dpre, contract, preferred_element_type=f32
    ).astype(bf16)

    hidden = up_projection_weight.shape[1]
    own = width // ranks_dp
    down_parts = down_partial.reshape(8, 4, own, hidden)
    up_parts = up_partial.reshape(8, 4, own, hidden)

    def part(array, index, dim):
        return lax.dynamic_index_in_dim(array, index, dim, False)

    down_z = rs_eight(lambda k: part(down_parts, (z + k) % 8, 0), "z")
    up_x = rs_four(lambda k: part(up_parts, (x + k) % 4, 1), "x")
    down_grad = rs_four(lambda k: part(down_z, (x + k) % 4, 0), "x")
    up_grad = rs_eight(lambda k: part(up_x, (z + k) % 8, 0), "z")
    return (up_grad, down_grad, loss)


def solution(mesh):
    finer = Mesh(mesh.devices.reshape(8, 4, 4, 2), ("z", "x", "y", "c"))
    dp, fsdp = ("z", "x"), ("y", "c")
    in_specs = (
        P(dp, None, None),
        P(dp, None, None),
        P(dp, None, None),
        P(dp, None),
        P(dp),
        P(),
        P(),
        P(),
        P(),
        P(),
        P(None, fsdp),
        P(None, fsdp),
        P(),
    )
    out_specs = (P(dp, fsdp), P(dp, fsdp), P())
    return jax.shard_map(
        shards, mesh=finer, in_specs=in_specs, out_specs=out_specs, check_vma=False
    )
```

```python
import jax
import jax.numpy as jnp
from jax import lax
from jax.experimental import pallas as pl
from jax.experimental.pallas import tpu as pltpu
from jax.sharding import Mesh
from jax.sharding import PartitionSpec as P

KSTEPS = 10
DP = ("z", "x")
clip_range = 0.2
noise_level = 0.7
norm_eps = 1e-06
bf16 = jnp.bfloat16
f32 = jnp.float32


def move(value, axis, steps):
    count = lax.axis_size(axis)
    return lax.ppermute(value, axis, [(i, (i + steps) % count) for i in range(count)])


def swap(value, axis, bit):
    count = lax.axis_size(axis)
    return lax.ppermute(value, axis, [(i, i ^ bit) for i in range(count)])


def sent_to_all(value, axis):
    count = lax.axis_size(axis)
    return lax.all_to_all(jnp.broadcast_to(value[None], (count, *value.shape)), axis, 0, 0, tiled=True)


def smooth_gate(values):
    return jax.nn.gelu(values, approximate=True)


TRAJS = 6
PAIRS = 64
TILE = 8
BLOCK = TRAJS * TILE
CHUNKS = 8


def gather_kernel(slots, stamps, latents, noise, behavior, out_first, out_second, own_first, own_second, sems):
    copies = []
    for j in range(2 * TRAJS):
        slot = slots[j]
        first, second = (out_first, out_second) if j < TRAJS else (own_first, own_second)
        k = j % TRAJS
        for i, (source, target) in enumerate(
            ((latents, first.at[k, pl.ds(0, PAIRS)]), (noise, second.at[k, 0]), (behavior, second.at[k, 1]))
        ):
            copy = pltpu.make_async_copy(source.at[slot], target, sems.at[3 * j + i])
            copy.start()
            copies.append(copy)
    step = lax.broadcasted_iota(jnp.int32, (16, 128), 0) % 2
    for j in range(2 * TRAJS):
        slot = slots[j]
        tile = jnp.where(step == 0, stamps[slot, 0], stamps[slot, 1])
        first = out_first if j < TRAJS else own_first
        first[j % TRAJS, pl.ds(PAIRS, 16), :] = tile.astype(f32).astype(bf16)
    for copy in copies:
        copy.wait()


def modulation_rows(stamp_tile, lookup, index):
    rows = jnp.zeros((TILE, lookup.shape[2]), f32)
    for k in range(KSTEPS):
        rows = jnp.where(stamp_tile == k, lookup[k, pl.ds(index, 1), :], rows)
    return rows


def widened(weight, wide, dim):
    size = weight.shape[dim]
    wide[...] = jnp.zeros(wide.shape, wide.dtype)
    if dim == 0:
        wide[0, pl.ds(0, size), :] = weight[...]
        wide[1, pl.ds(size, size), :] = weight[...]
    else:
        wide[0, :, pl.ds(0, size)] = weight[...]
        wide[1, :, pl.ds(size, size)] = weight[...]


def embed_kernel(left, order, came, mine, weight, lookup, mod_a, mod_b, tokens, stamps, merged, sorted_, wide, emb, scale, shift):
    width = weight.shape[1]
    for j in range(TRAJS):
        merged[pl.ds(j * 80, 80), :] = jnp.where(left[j] != 0, came[j].astype(f32), mine[j].astype(f32))
    for q in range(CHUNKS):
        for j in range(TRAJS):
            at = pl.multiple_of(j * 80 + order[q] * TILE, TILE)
            sorted_[pl.ds(q * BLOCK + j * TILE, TILE), :] = merged[pl.ds(at, TILE), :]
    tokens[...] = sorted_[...].astype(bf16)
    widened(weight, wide, 0)
    for par in range(2):
        emb[par] = jnp.dot(tokens[...], wide[par], preferred_element_type=f32)
    for j in range(TRAJS):
        stamp = merged[pl.ds(j * 80 + PAIRS, TILE), :]
        stamps[pl.ds(j * TILE, TILE), :] = stamp
        stamp = stamp[:, :1]
        shift[pl.ds(j * TILE, TILE), :] = modulation_rows(stamp, lookup, 0)
        scale[pl.ds(j * TILE, TILE), :] = 1.0 + modulation_rows(stamp, lookup, 1)

    def chunk(q, modulated):
        for par in range(2):
            values = emb[par, pl.ds(pl.multiple_of(q * BLOCK, BLOCK), BLOCK), :]
            center = values - jnp.sum(values, axis=1, keepdims=True) * (1.0 / width)
            variance = jnp.sum(center * center, axis=1, keepdims=True) * (1.0 / width)
            normed = center * lax.rsqrt(variance + norm_eps)
            at = pl.multiple_of((q % 4) * (2 * BLOCK) + par * BLOCK, BLOCK)
            modulated[pl.ds(at, BLOCK), :] = (normed * scale[...] + shift[...]).astype(bf16)

    def first_half(q, carry):
        chunk(q, mod_a)
        return carry

    def second_half(q, carry):
        chunk(q + 4, mod_b)
        return carry

    lax.fori_loop(0, 4, first_half, 0)
    lax.fori_loop(0, 4, second_half, 0)


def head_kernel(
    left, order, table, source, slot, kept, place, other, own, tokens, stamps, came, mine, weight, head, lookup,
    upstream, loss,
    drawn, target, wide, wide_head, emb, rounded, back, inverse, gate, error, slope, coeff,
):
    width = weight.shape[1]
    values = SEQ_VALUES
    widened(weight, wide, 0)
    widened(head, wide_head, 1)
    for j in range(TRAJS):
        stamp = stamps[pl.ds(j * TILE, TILE), :]
        gate[pl.ds(j * TILE, TILE), :] = modulation_rows(stamp[:, :1], lookup, 2)
        level = 1.0 - stamp * (1.0 / KSTEPS)
        coeff[pl.ds(j * TILE, TILE), :] = (
            jnp.sqrt((1.0 / KSTEPS) * (1.0 - level + 1.0 / KSTEPS) / level) / noise_level
        )
        picked = jnp.where(left[j] != 0, came[j].astype(f32), mine[j].astype(f32))
        emb[0, pl.ds(0, PAIRS), pl.ds(0, 128)] = picked[0]
        emb[0, pl.ds(PAIRS, PAIRS), pl.ds(0, 128)] = picked[1]
        for q in range(CHUNKS):
            at = pl.multiple_of(order[q] * TILE, TILE)
            drawn[pl.ds(q * BLOCK + j * TILE, TILE), :] = emb[0, pl.ds(at, TILE), pl.ds(0, 128)]
            at = pl.multiple_of(PAIRS + order[q] * TILE, TILE)
            target[pl.ds(q * BLOCK + j * TILE, TILE), :] = emb[0, pl.ds(at, TILE), pl.ds(0, 128)]
    for par in range(2):
        emb[par] = jnp.dot(tokens[...], wide[par], preferred_element_type=f32)

    def forward(q, summed):
        for par in range(2):
            rows = pl.ds(pl.multiple_of(q * BLOCK, BLOCK), BLOCK)
            at = pl.multiple_of((q % 4) * (2 * BLOCK) + par * BLOCK, BLOCK)
            mixed = emb[par, rows, :] + gate[...] * summed[pl.ds(at, BLOCK), :].astype(f32)
            center = mixed - jnp.sum(mixed, axis=1, keepdims=True) * (1.0 / width)
            variance = jnp.sum(center * center, axis=1, keepdims=True) * (1.0 / width)
            scale = lax.rsqrt(variance + norm_eps)
            final = center * scale
            emb[par, rows, :] = final
            rounded[par, rows, :] = final.astype(bf16)
            inverse[par, rows, :] = jnp.broadcast_to(scale, (BLOCK, 128))

    def first_half(q, carry):
        forward(q, other)
        return carry

    def second_half(q, carry):
        forward(q + 4, own)
        return carry

    lax.fori_loop(0, 4, first_half, 0)
    lax.fori_loop(0, 4, second_half, 0)
    velocity = jnp.dot(rounded[0], wide_head[0], preferred_element_type=f32)
    error[...] = velocity + jnp.dot(rounded[1], wide_head[1], preferred_element_type=f32) - target[...]
    total = jnp.zeros((BLOCK, 128), f32)
    c = coeff[...]
    for q in range(CHUNKS):
        rows = pl.ds(q * BLOCK, BLOCK)
        err = error[rows, :]
        total = total + c * drawn[rows, :] * err + 0.5 * c * c * err * err
    sums = jnp.broadcast_to(jnp.sum(total, axis=1, keepdims=True), (BLOCK, 128))
    losses = jnp.zeros((TILE, 128), f32)
    gains = advantages(table, source, slot, kept, place[0] * 4 + place[1])
    for j in range(TRAJS):
        unit = sums[j * TILE : (j + 1) * TILE]
        unit = unit + pltpu.roll(unit, 4, 0)
        unit = unit + pltpu.roll(unit, 2, 0)
        ratio = jnp.exp(-unit / values)
        clipped = jnp.clip(ratio, 1.0 - clip_range, 1.0 + clip_range)
        plain = ratio * gains[j]
        bounded = clipped * gains[j]
        losses = losses - jnp.minimum(plain, bounded)
        live = jnp.where(plain <= bounded, 1.0, 0.0)
        slope[pl.ds(j * TILE, TILE), :] = -gains[j] * ratio * live * (1.0 / UNITS)
    loss[...] = losses
    bent = slope[...]
    for q in range(CHUNKS):
        rows = pl.ds(q * BLOCK, BLOCK)
        error[rows, :] = bent * (-(c * drawn[rows, :] + c * c * error[rows, :]) / values)
    dvelocity = error[...].astype(bf16)
    for par in range(2):
        back[par] = lax.dot_general(
            dvelocity, wide_head[par], (((1,), (1,)), ((), ())), preferred_element_type=f32
        )

    def backward(q, carry):
        for par in range(2):
            rows = pl.ds(pl.multiple_of(q * BLOCK, BLOCK), BLOCK)
            d = back[par, rows, :]
            final = emb[par, rows, :]
            mean = jnp.sum(d, axis=1, keepdims=True) * (1.0 / width)
            along = jnp.sum(d * final, axis=1, keepdims=True) * (1.0 / width)
            dmixed = inverse[par, rows, :][:, :1] * (d - mean - final * along)
            at = pl.multiple_of(q * (2 * BLOCK) + par * BLOCK, BLOCK)
            upstream[pl.ds(at, BLOCK), :] = (gate[...] * dmixed).astype(bf16)
        return carry

    lax.fori_loop(0, CHUNKS, backward, 0)


def advantages(table, source, slot, kept, owner):
    def rank_of(p):
        d = source[p]
        return table[d // 4, (d % 4) * SLOTS + slot[p]]

    gains = []
    for j in range(TRAJS):
        p = owner * TRAJS + j

        def seek(g, state):
            end, begin, count = state
            here = (p >= end) & (p < end + kept[g])
            return end + kept[g], jnp.where(here, end, begin), jnp.where(here, kept[g], count)

        _, begin, count = lax.fori_loop(0, kept.shape[0], seek, (0, 0, 1))

        def add(q, state):
            rank = rank_of(q)
            return state[0] + rank, state[1] + rank * rank

        first, second = lax.fori_loop(begin, begin + count, add, (0, 0))

        def row(value):
            return jnp.full((1, 128), value, jnp.int32).astype(f32)

        counts = row(count)
        deviation = jnp.sqrt(row(count * second - first * first)) / counts
        gains.append((row(rank_of(p)) - row(first) / counts) / jnp.maximum(deviation, 1.0))
    return gains


SEQ_VALUES = 4096
SLOTS = 12
UNITS = 384
SMEM = pl.BlockSpec(memory_space=pltpu.SMEM)
VMEM = pl.BlockSpec(memory_space=pltpu.VMEM)
HBM = pl.BlockSpec(memory_space=pl.ANY)


def wide_add(*parts):
    total = parts[0].astype(f32)
    for part in parts[1:]:
        total = total + part.astype(f32)
    return total


def call(kernel, shapes, count, **kw):
    return pl.pallas_call(
        kernel,
        out_shape=tuple(jax.ShapeDtypeStruct(shape, dtype) for shape, dtype in shapes),
        in_specs=[VMEM] * count,
        out_specs=(VMEM,) * len(shapes),
        **kw,
    )


def fold_kernel(mine, got, down, up, low, high, own):
    n = mine.shape[2] // 2
    total = [mine[k].astype(f32) + got[k].astype(f32) for k in range(4)]
    down[0] = total[3][:, n:].astype(bf16)
    down[1] = total[2][:, :n].astype(bf16)
    up[0] = total[1][:, :n].astype(bf16)
    up[1] = total[2][:, n:].astype(bf16)
    low[...] = total[3][:, :n].astype(bf16)
    high[...] = total[1][:, n:].astype(bf16)
    own[...] = total[0]


def onward_kernel(low, high, own, from_up, from_down, down, up, kept):
    n = low.shape[1]
    down[...] = (low[...].astype(f32) + from_up[1].astype(f32)).astype(bf16)
    up[...] = (high[...].astype(f32) + from_down[1].astype(f32)).astype(bf16)
    kept[:, pl.ds(0, n)] = own[:, pl.ds(0, n)] + from_down[0].astype(f32)
    kept[:, pl.ds(n, n)] = own[:, pl.ds(n, n)] + from_up[0].astype(f32)


def close_kernel(kept, late_up, late_down, out):
    n = late_up.shape[1]
    out[:, pl.ds(0, n)] = (kept[:, pl.ds(0, n)] + late_up[...].astype(f32)).astype(out.dtype)
    out[:, pl.ds(n, n)] = (kept[:, pl.ds(n, n)] + late_down[...].astype(f32)).astype(out.dtype)


def half_add_kernel(part, recv, out, *, lead):
    n = recv.shape[1]
    total = (part[0, :, pl.ds(lead * n, n)].astype(f32) + recv[...].astype(f32)).astype(bf16)
    out[:, pl.ds(lead * n, n)] = total
    out[:, pl.ds((1 - lead) * n, n)] = part[0, :, pl.ds((1 - lead) * n, n)]


def half_add(parts, index, recv, lead):
    block = parts.shape[1:]
    return pl.pallas_call(
        lambda *refs: half_add_kernel(*refs, lead=lead),
        grid=(1,),
        out_shape=jax.ShapeDtypeStruct(block, bf16),
        in_specs=[
            pl.BlockSpec((1, *block), lambda i: (index, 0, 0)),
            pl.BlockSpec(recv.shape, lambda i: (0, 0)),
        ],
        out_specs=pl.BlockSpec(block, lambda i: (0, 0)),
        name="ring_second",
    )(parts, recv)


def ring_of_eight(parts, low, high, beside):
    from_up = move(low, "z", -1)
    from_down = move(high, "z", 1)
    from_up, from_down, carried = beside(0, from_up, from_down)
    down = half_add(parts, 5, from_up, 0)
    up = half_add(parts, 3, from_down, 1)
    for step in (2, 1):
        from_up = move(down, "z", -1)
        from_down = move(up, "z", 1)
        if step == 2:
            from_up, from_down, carried = beside(1, from_up, from_down, carried)
        down = wide_add(parts[8 - step], from_up).astype(bf16)
        up = wide_add(parts[step], from_down).astype(bf16)
    return move(down, "z", -1), move(up, "z", 1), carried


def alone(step, from_up, from_down, carried=None):
    return from_up, from_down, carried


def turn_kernel(place, part, from_up, from_down, rest, down, up):
    n = rest.shape[2] // 2
    own = rest.shape[1]
    for a in range(4):
        rows = pl.ds(a * own, own)
        total = part[0, rows, :].astype(f32) + from_up[rows, :].astype(f32) + from_down[rows, :].astype(f32)
        total = total.astype(bf16)
        k = (a + 4 - place[1]) % 4
        rest[k] = total

        @pl.when(k == 3)
        def _():
            down[0] = total[:, n:]

        @pl.when(k == 2)
        def _():
            down[1] = total[:, :n]
            up[1] = total[:, n:]

        @pl.when(k == 1)
        def _():
            up[0] = total[:, :n]


def down_weight_kernel(place, upstream, act_a, act_b, parts, low, high):
    n = parts.shape[2] // 2
    half = act_a.shape[0]
    own = parts.shape[1]
    contract = (((0,), (0,)), ((), ()))

    def block(i, carry):
        cols = pl.ds(pl.multiple_of(i * 2 * own, 128), 2 * own)
        total = lax.dot_general(
            upstream[pl.ds(0, half), cols], act_a[...], contract, preferred_element_type=f32
        ) + lax.dot_general(
            upstream[pl.ds(half, half), cols], act_b[...], contract, preferred_element_type=f32
        )
        total = total.astype(bf16)
        for j in range(2):
            k = (2 * i + j + 8 - place[0]) % 8
            piece = total[j * own : (j + 1) * own]
            parts[k] = piece

            @pl.when(k == 4)
            def _():
                low[...] = piece[:, :n]
                high[...] = piece[:, n:]

        return carry

    lax.fori_loop(0, 4, block, 0)


def up_weight_kernel(place, upstream, weight, pre_a, pre_b, mod_a, mod_b, parts, down, up, dpre):
    half, hidden = pre_a.shape
    n = hidden // 2
    own = parts.shape[2]
    contract = (((0,), (0,)), ((), ()))
    for i, pre in enumerate((pre_a, pre_b)):

        def rows_of(r, carry, i=i, pre=pre):
            rows = pl.ds(pl.multiple_of(r * 192, 192), 192)
            v = pre[rows, :]
            up_rows = upstream[pl.ds(pl.multiple_of(i * half + r * 192, 192), 192), :]
            d = jnp.dot(up_rows, weight[...], preferred_element_type=f32)
            k = 0.7978845608028654
            t = jnp.tanh(k * (v + 0.044715 * (v * v * v)))
            slope = 0.5 * (1.0 + t) + 0.5 * v * (1.0 - t * t) * (k * (1.0 + 3 * 0.044715 * (v * v)))
            dpre[pl.ds(pl.multiple_of(i * half + r * 192, 192), 192), :] = (d * slope).astype(bf16)
            return carry

        lax.fori_loop(0, half // 192, rows_of, 0)

    def block(i, carry):
        cols = pl.ds(pl.multiple_of(i * 8 * own, 128), 8 * own)
        total = lax.dot_general(
            mod_a[:, cols], dpre[pl.ds(0, half), :], contract, preferred_element_type=f32
        ) + lax.dot_general(
            mod_b[:, cols], dpre[pl.ds(half, half), :], contract, preferred_element_type=f32
        )
        total = total.astype(bf16)
        for j in range(8):
            k = (j % 4 + 4 - place[1]) % 4
            m = (2 * i + j // 4 + 8 - place[0]) % 8
            piece = total[j * own : (j + 1) * own]
            parts[k, m] = piece

            @pl.when(k == 3)
            def _():
                down[0, m] = piece[:, n:]

            @pl.when(k == 2)
            def _():
                down[1, m] = piece[:, :n]
                up[1, m] = piece[:, n:]

            @pl.when(k == 1)
            def _():
                up[0, m] = piece[:, :n]

        return carry

    lax.fori_loop(0, 4, block, 0)


def shards(
    latents,
    noise,
    behavior_velocity,
    timestep,
    reward_rank_integer,
    surviving_source_index,
    surviving_slot_index,
    group_kept_count,
    patch_input_weight,
    modulation_lookup,
    up_projection_weight,
    down_projection_weight,
    velocity_head_weight,
):
    z, x, y, c = (lax.axis_index(a) for a in ("z", "x", "y", "c"))
    owner = lax.axis_index(DP)
    ranks_dp = lax.axis_size(DP)
    surviving = surviving_source_index.shape[0]
    trajs = surviving // ranks_dp
    steps = timestep.shape[1]
    lead = owner * trajs
    sources = lax.dynamic_slice_in_dim(surviving_source_index, lead, trajs)
    slots = lax.dynamic_slice_in_dim(surviving_slot_index, lead, trajs)
    next_lead = jnp.minimum(owner + 1, ranks_dp - 1) * trajs
    next_slots = lax.dynamic_slice_in_dim(surviving_slot_index, next_lead, trajs)
    capacity = latents.shape[0]

    def pairs(a):
        return a.reshape(capacity, steps, 32, 128).transpose(0, 2, 1, 3).reshape(capacity, 64, 128)

    width = patch_input_weight.shape[1]
    rows = 8 * 2 * trajs * 8
    one = jax.ShapeDtypeStruct((TRAJS, 80, 128), bf16)
    two = jax.ShapeDtypeStruct((TRAJS, 2, PAIRS, 128), bf16)
    out_first, out_second, own_first, own_second = pl.pallas_call(
        gather_kernel,
        out_shape=(one, two, one, two),
        in_specs=[SMEM, SMEM, HBM, HBM, HBM],
        out_specs=(VMEM, VMEM, VMEM, VMEM),
        scratch_shapes=[pltpu.SemaphoreType.DMA((6 * TRAJS,))],
        name="gather_slots",
    )(
        jnp.concatenate([next_slots, slots]), timestep,
        pairs(latents), pairs(noise), pairs(behavior_velocity),
    )
    onward = [(i, i + 1) for i in range(ranks_dp - 1)]
    came = lax.ppermute(out_first, DP, onward)
    came_late = lax.ppermute(out_second, DP, onward)
    left = (sources != owner).astype(jnp.int32)
    ks = (y + jnp.arange(4, dtype=jnp.int32)) % 4 * 2
    order = jnp.concatenate([ks + (1 - c), ks + c])
    mod_a, mod_b, tokens, stamps = pl.pallas_call(
        embed_kernel,
        out_shape=(
            jax.ShapeDtypeStruct((rows // 2, width), bf16),
            jax.ShapeDtypeStruct((rows // 2, width), bf16),
            jax.ShapeDtypeStruct((CHUNKS * BLOCK, 128), bf16),
            jax.ShapeDtypeStruct((BLOCK, 128), f32),
        ),
        in_specs=[SMEM, SMEM, VMEM, VMEM, VMEM, VMEM],
        out_specs=(VMEM, VMEM, VMEM, VMEM),
        scratch_shapes=[
            pltpu.VMEM((TRAJS * 80, 128), f32),
            pltpu.VMEM((CHUNKS * BLOCK, 128), f32),
            pltpu.VMEM((2, 128, width), bf16),
            pltpu.VMEM((2, CHUNKS * BLOCK, width), f32),
            pltpu.VMEM((BLOCK, width), f32),
            pltpu.VMEM((BLOCK, width), f32),
        ],
        compiler_params=pltpu.CompilerParams(vmem_limit_bytes=48 << 20),
        name="embed_and_modulate",
    )(left, order, came, own_first, patch_input_weight, modulation_lookup)

    def hidden_half(mod):
        pre = jnp.dot(mod, up_projection_weight, preferred_element_type=f32)
        activated = smooth_gate(pre).astype(bf16)
        projected = lax.dot_general(
            activated, down_projection_weight, (((1,), (1,)), ((), ())), preferred_element_type=f32
        ).astype(bf16)
        return pre, activated, projected

    pre_a, act_a, proj_a = hidden_half(mod_a)
    got = swap(proj_a, "c", 1)
    pre_b, act_b, proj_b = hidden_half(mod_b)
    table = sent_to_all(reward_rank_integer, "x").reshape(4 * capacity)
    got, table = lax.optimization_barrier((got, table))
    n = width // 2
    piece = rows // 8
    down, up, low, high, own = call(
        fold_kernel,
        [((2, piece, n), bf16)] * 2 + [((piece, n), bf16)] * 2 + [((piece, width), f32)],
        2,
        name="fold",
    )(proj_b.reshape(4, piece, width), got.reshape(4, piece, width))
    from_up = move(down, "y", -1)
    from_down = move(up, "y", 1)
    table = sent_to_all(table, "z")
    from_up, from_down, table, came_late = lax.optimization_barrier((from_up, from_down, table, came_late))
    down, up, kept = call(
        onward_kernel, [((piece, n), bf16)] * 2 + [((piece, width), f32)], 5, name="onward"
    )(low, high, own, from_up, from_down)
    late_up = move(down, "y", -1)
    late_down = move(up, "y", 1)
    (own,) = call(close_kernel, [((piece, width), bf16)], 3, name="close")(kept, late_up, late_down)
    after = move(own, "y", -1)
    before = move(own, "y", 1)
    far = jnp.concatenate([move(after[:, :n], "y", -1), move(before[:, n:], "y", 1)], axis=1)
    summed_own = jnp.concatenate([own, after, far, before], axis=0)
    summed_other = swap(summed_own, "c", 1)
    place = jnp.stack([z, x]).astype(jnp.int32)
    upstream, losses = pl.pallas_call(
        head_kernel,
        out_shape=(
            jax.ShapeDtypeStruct((rows, width), bf16),
            jax.ShapeDtypeStruct((TILE, 128), f32),
        ),
        in_specs=[SMEM] * 7 + [VMEM] * 9,
        out_specs=(VMEM, VMEM),
        scratch_shapes=[
            pltpu.VMEM((CHUNKS * BLOCK, 128), f32),
            pltpu.VMEM((CHUNKS * BLOCK, 128), f32),
            pltpu.VMEM((2, 128, width), bf16),
            pltpu.VMEM((2, width, 128), bf16),
            pltpu.VMEM((2, CHUNKS * BLOCK, width), f32),
            pltpu.VMEM((2, CHUNKS * BLOCK, width), bf16),
            pltpu.VMEM((2, CHUNKS * BLOCK, width), f32),
            pltpu.VMEM((2, CHUNKS * BLOCK, 128), f32),
            pltpu.VMEM((BLOCK, width), f32),
            pltpu.VMEM((CHUNKS * BLOCK, 128), f32),
            pltpu.VMEM((BLOCK, 128), f32),
            pltpu.VMEM((BLOCK, 128), f32),
        ],
        compiler_params=pltpu.CompilerParams(vmem_limit_bytes=56 << 20),
        name="head_both_ways",
    )(
        left, order, table, surviving_source_index, surviving_slot_index, group_kept_count, place,
        summed_other, summed_own, tokens, stamps, came_late, own_second,
        patch_input_weight, velocity_head_weight, modulation_lookup,
    )
    hidden = up_projection_weight.shape[1]
    own = width // ranks_dp
    m = hidden // 2
    down_parts, down_low, down_high = pl.pallas_call(
        down_weight_kernel,
        out_shape=(
            jax.ShapeDtypeStruct((8, 4 * own, hidden), bf16),
            jax.ShapeDtypeStruct((4 * own, m), bf16),
            jax.ShapeDtypeStruct((4 * own, m), bf16),
        ),
        in_specs=[SMEM] + [VMEM] * 3,
        out_specs=(VMEM,) * 3,
        compiler_params=pltpu.CompilerParams(vmem_limit_bytes=48 << 20),
        name="down_weight",
    )(place, upstream, act_a, act_b)
    up_parts, up_first_down, up_first_up = pl.pallas_call(
        up_weight_kernel,
        out_shape=(
            jax.ShapeDtypeStruct((4, 8, own, hidden), bf16),
            jax.ShapeDtypeStruct((2, 8, own, m), bf16),
            jax.ShapeDtypeStruct((2, 8, own, m), bf16),
        ),
        in_specs=[SMEM] + [VMEM] * 6,
        out_specs=(VMEM,) * 3,
        scratch_shapes=[pltpu.VMEM((rows, hidden), bf16)],
        compiler_params=pltpu.CompilerParams(vmem_limit_bytes=56 << 20),
        name="up_weight",
    )(place, upstream, down_projection_weight, pre_a, pre_b, mod_a, mod_b)

    def with_loss(step, from_up, from_down, carried=None):
        value = sent_to_all(losses[:2, 0], "x") if step == 0 else sent_to_all(carried, "z")
        return lax.optimization_barrier((from_up, from_down, value))

    from_up = move(up_first_down, "x", -1)
    from_down = move(up_first_up, "x", 1)
    second_down = wide_add(up_parts[3, :, :, :m], from_up[1]).astype(bf16)
    second_up = wide_add(up_parts[1, :, :, m:], from_down[1]).astype(bf16)
    late_up = move(second_down, "x", -1)
    late_down = move(second_up, "x", 1)

    from_z_up, from_z_down, everyone = ring_of_eight(down_parts, down_low, down_high, with_loss)
    loss = jnp.sum(everyone) / UNITS
    rest, turn_down, turn_up = pl.pallas_call(
        turn_kernel,
        grid=(1,),
        out_shape=(
            jax.ShapeDtypeStruct((4, own, hidden), bf16),
            jax.ShapeDtypeStruct((2, own, m), bf16),
            jax.ShapeDtypeStruct((2, own, m), bf16),
        ),
        in_specs=[
            SMEM,
            pl.BlockSpec((1, 4 * own, hidden), lambda i: (0, 0, 0)),
            pl.BlockSpec((4 * own, hidden), lambda i: (0, 0)),
            pl.BlockSpec((4 * own, hidden), lambda i: (0, 0)),
        ],
        out_specs=(
            pl.BlockSpec((4, own, hidden), lambda i: (0, 0, 0)),
            pl.BlockSpec((2, own, m), lambda i: (0, 0, 0)),
            pl.BlockSpec((2, own, m), lambda i: (0, 0, 0)),
        ),
        name="turn",
    )(place, down_parts, from_z_up, from_z_down)
    up_x = jnp.concatenate(
        [
            wide_add(up_parts[0, :, :, :m], from_down[0], late_up),
            wide_add(up_parts[0, :, :, m:], from_up[0], late_down),
        ],
        axis=2,
    ).astype(bf16)
    far_up = move(turn_down, "x", -1)
    far_down = move(turn_up, "x", 1)
    second_down = wide_add(rest[3, :, :m], far_up[1]).astype(bf16)
    second_up = wide_add(rest[1, :, m:], far_down[1]).astype(bf16)
    last_up = move(second_down, "x", -1)
    last_down = move(second_up, "x", 1)
    down_grad = jnp.concatenate(
        [
            wide_add(rest[0, :, :m], far_down[0], last_up),
            wide_add(rest[0, :, m:], far_up[0], last_down),
        ],
        axis=1,
    )
    end_up, end_down, _ = ring_of_eight(up_x, up_x[4, :, :m], up_x[4, :, m:], alone)
    up_grad = wide_add(up_x[0], end_up, end_down)
    return (up_grad, down_grad, loss)


def solution(mesh):
    finer = Mesh(mesh.devices.reshape(8, 4, 4, 2), ("z", "x", "y", "c"))
    dp, fsdp = ("z", "x"), ("y", "c")
    in_specs = (
        P(dp, None, None),
        P(dp, None, None),
        P(dp, None, None),
        P(dp, None),
        P(dp),
        P(),
        P(),
        P(),
        P(),
        P(),
        P(None, fsdp),
        P(None, fsdp),
        P(),
    )
    out_specs = (P(dp, fsdp), P(dp, fsdp), P())
    return jax.shard_map(
        shards, mesh=finer, in_specs=in_specs, out_specs=out_specs, check_vma=False
    )
```

```python
import jax
import jax.numpy as jnp
from jax import lax
from jax.experimental import pallas as pl
from jax.experimental.pallas import tpu as pltpu
from jax.sharding import Mesh
from jax.sharding import PartitionSpec as P

KSTEPS = 10
DP = ("z", "x")
clip_range = 0.2
noise_level = 0.7
norm_eps = 1e-06
bf16 = jnp.bfloat16
f32 = jnp.float32


def move(value, axis, steps):
    count = lax.axis_size(axis)
    return lax.ppermute(value, axis, [(i, (i + steps) % count) for i in range(count)])


def swap(value, axis, bit):
    count = lax.axis_size(axis)
    return lax.ppermute(value, axis, [(i, i ^ bit) for i in range(count)])


TRAJS = 6
PAIRS = 64
TILE = 8
BLOCK = TRAJS * TILE
CHUNKS = 8


def gather_kernel(slots, stamps, latents, noise, behavior, out_first, out_second, own_first, own_second, sems):
    copies = []
    for j in range(2 * TRAJS):
        slot = slots[j]
        first, second = (out_first, out_second) if j < TRAJS else (own_first, own_second)
        k = j % TRAJS
        for i, (source, target) in enumerate(
            ((latents, first.at[k, pl.ds(0, PAIRS)]), (noise, second.at[k, 0]), (behavior, second.at[k, 1]))
        ):
            copy = pltpu.make_async_copy(source.at[slot], target, sems.at[3 * j + i])
            copy.start()
            copies.append(copy)
    step = lax.broadcasted_iota(jnp.int32, (16, 128), 0) % 2
    for j in range(2 * TRAJS):
        slot = slots[j]
        tile = jnp.where(step == 0, stamps[slot, 0], stamps[slot, 1])
        first = out_first if j < TRAJS else own_first
        first[j % TRAJS, pl.ds(PAIRS, 16), :] = tile.astype(f32).astype(bf16)
    for copy in copies:
        copy.wait()


def modulation_rows(stamp_tile, lookup, index):
    rows = jnp.zeros((TILE, lookup.shape[2]), f32)
    for k in range(KSTEPS):
        rows = jnp.where(stamp_tile == k, lookup[k, pl.ds(index, 1), :], rows)
    return rows


def widened(weight, wide, dim):
    size = weight.shape[dim]
    wide[...] = jnp.zeros(wide.shape, wide.dtype)
    if dim == 0:
        wide[0, pl.ds(0, size), :] = weight[...]
        wide[1, pl.ds(size, size), :] = weight[...]
    else:
        wide[0, :, pl.ds(0, size)] = weight[...]
        wide[1, :, pl.ds(size, size)] = weight[...]


def gelu_both(v):
    k = 0.7978845608028654
    square = v * v
    t = jnp.tanh(k * (v + 0.044715 * (square * v)))
    half = 0.5 * (1.0 + t)
    return v * half, half + (0.5 * k) * v * (1.0 - t * t) * (1.0 + (3 * 0.044715) * square)


def forward_kernel(
    left, order, came, mine, weight, lookup, up_weight, down_weight,
    tokens, stamps, mod_out, act_out, bend_out, proj_other, proj_own,
    merged, sorted_, wide, emb, scale, shift, up_w, down_w, modulated, activated, bend, proj, sems,
):
    width = weight.shape[1]
    load_up = pltpu.make_async_copy(up_weight, up_w, sems.at[0])
    load_down = pltpu.make_async_copy(down_weight, down_w, sems.at[1])
    load_up.start()
    load_down.start()
    for j in range(TRAJS):
        merged[pl.ds(j * 80, 80), :] = jnp.where(left[j] != 0, came[j].astype(f32), mine[j].astype(f32))
    for q in range(CHUNKS):
        for j in range(TRAJS):
            at = pl.multiple_of(j * 80 + order[q] * TILE, TILE)
            sorted_[pl.ds(q * BLOCK + j * TILE, TILE), :] = merged[pl.ds(at, TILE), :]
    tokens[...] = sorted_[...].astype(bf16)
    widened(weight, wide, 0)
    for j in range(TRAJS):
        stamp = merged[pl.ds(j * 80 + PAIRS, TILE), :]
        stamps[pl.ds(j * TILE, TILE), :] = stamp
        stamp = stamp[:, :1]
        shift[pl.ds(j * TILE, TILE), :] = modulation_rows(stamp, lookup, 0)
        scale[pl.ds(j * TILE, TILE), :] = 1.0 + modulation_rows(stamp, lookup, 1)
    for par in range(2):
        emb[par] = jnp.dot(tokens[...], wide[par], preferred_element_type=f32)

    def norm(q, carry):
        for par in range(2):
            values = emb[par, pl.ds(pl.multiple_of(q * BLOCK, BLOCK), BLOCK), :]
            center = values - jnp.sum(values, axis=1, keepdims=True) * (1.0 / width)
            variance = jnp.sum(center * center, axis=1, keepdims=True) * (1.0 / width)
            normed = center * lax.rsqrt(variance + norm_eps)
            at = pl.multiple_of(q * (2 * BLOCK) + par * BLOCK, BLOCK)
            modulated[pl.ds(at, BLOCK), :] = (normed * scale[...] + shift[...]).astype(bf16)
        return carry

    lax.fori_loop(0, CHUNKS, norm, 0)
    save_mod = pltpu.make_async_copy(modulated, mod_out, sems.at[2])
    save_mod.start()
    load_up.wait()
    load_down.wait()

    def hidden(r, carry):
        rows = pl.ds(pl.multiple_of(r * 192, 192), 192)
        pre = jnp.dot(modulated[rows, :], up_w[...], preferred_element_type=f32)
        value, slope = gelu_both(pre)
        value = value.astype(bf16)
        activated[rows, :] = value
        bend[rows, :] = slope.astype(bf16)
        proj[rows, :] = lax.dot_general(
            value, down_w[...], (((1,), (1,)), ((), ())), preferred_element_type=f32
        ).astype(bf16)
        return carry

    half = modulated.shape[0] // 2
    lax.fori_loop(0, 2, hidden, 0)
    save_other = pltpu.make_async_copy(proj.at[pl.ds(0, half)], proj_other, sems.at[3])
    save_other.start()
    lax.fori_loop(2, 4, hidden, 0)
    save_own = pltpu.make_async_copy(proj.at[pl.ds(half, half)], proj_own, sems.at[4])
    save_own.start()
    save_act = pltpu.make_async_copy(activated, act_out, sems.at[5])
    save_act.start()
    save_bend = pltpu.make_async_copy(bend, bend_out, sems.at[6])
    save_bend.start()
    for copy in (save_mod, save_other, save_own, save_act, save_bend):
        copy.wait()


def backward_kernel(
    left, order, ranks, far_ranks, source, slot, kept, place,
    other, own, tokens, stamps, came, mine, weight, head, lookup,
    act_in, bend_in, mod_in, down_in,
    down_parts, down_low, down_high, up_parts, up_down, up_up,
    drawn, target, wide, wide_head, emb, rounded, back, inverse, gate, error, slope, coeff,
    table_v, table, act, bend, mod, down_w, upstream, parts, low, high, pieces, first_down, first_up,
    sems, out_sems,
):
    loads = [
        pltpu.make_async_copy(a, b, sems.at[i])
        for i, (a, b) in enumerate(((act_in, act), (down_in, down_w), (bend_in, bend), (mod_in, mod)))
    ]
    for copy in loads:
        copy.start()
    owner = place[0] * 4 + place[1]
    for q in range(CHUNKS):
        info = (other if q < 4 else own)[pl.ds((q % 4) * 2 * BLOCK, 16), pl.ds(weight.shape[1], 128)].astype(f32)
        table_v[pl.ds(order[q], 1), :] = (info[0:1] * 32.0 + info[1:2]).astype(jnp.int32)
    fetch = pltpu.make_async_copy(table_v, table, sems.at[4])
    fetch.start()
    width = weight.shape[1]
    values = SEQ_VALUES
    widened(weight, wide, 0)
    widened(head, wide_head, 1)
    for j in range(TRAJS):
        stamp = stamps[pl.ds(j * TILE, TILE), :]
        gate[pl.ds(j * TILE, TILE), :] = modulation_rows(stamp[:, :1], lookup, 2)
        level = 1.0 - stamp * (1.0 / KSTEPS)
        coeff[pl.ds(j * TILE, TILE), :] = (
            jnp.sqrt((1.0 / KSTEPS) * (1.0 - level + 1.0 / KSTEPS) / level) / noise_level
        )
        picked = jnp.where(left[j] != 0, came[j].astype(f32), mine[j].astype(f32))
        emb[0, pl.ds(0, PAIRS), pl.ds(0, 128)] = picked[0]
        emb[0, pl.ds(PAIRS, PAIRS), pl.ds(0, 128)] = picked[1]
        for q in range(CHUNKS):
            at = pl.multiple_of(order[q] * TILE, TILE)
            drawn[pl.ds(q * BLOCK + j * TILE, TILE), :] = emb[0, pl.ds(at, TILE), pl.ds(0, 128)]
            at = pl.multiple_of(PAIRS + order[q] * TILE, TILE)
            target[pl.ds(q * BLOCK + j * TILE, TILE), :] = emb[0, pl.ds(at, TILE), pl.ds(0, 128)]
    for par in range(2):
        emb[par] = jnp.dot(tokens[...], wide[par], preferred_element_type=f32)

    def forward(q, summed):
        for par in range(2):
            rows = pl.ds(pl.multiple_of(q * BLOCK, BLOCK), BLOCK)
            at = pl.multiple_of((q % 4) * (2 * BLOCK) + par * BLOCK, BLOCK)
            mixed = emb[par, rows, :] + gate[...] * summed[pl.ds(at, BLOCK), pl.ds(0, width)].astype(f32)
            center = mixed - jnp.sum(mixed, axis=1, keepdims=True) * (1.0 / width)
            variance = jnp.sum(center * center, axis=1, keepdims=True) * (1.0 / width)
            scale = lax.rsqrt(variance + norm_eps)
            final = center * scale
            emb[par, rows, :] = final
            rounded[par, rows, :] = final.astype(bf16)
            inverse[par, rows, :] = jnp.broadcast_to(scale, (BLOCK, 128))

    def first_half(q, carry):
        forward(q, other)
        return carry

    def second_half(q, carry):
        forward(q + 4, own)
        return carry

    lax.fori_loop(0, 4, first_half, 0)
    lax.fori_loop(0, 4, second_half, 0)
    velocity = jnp.dot(rounded[0], wide_head[0], preferred_element_type=f32)
    error[...] = velocity + jnp.dot(rounded[1], wide_head[1], preferred_element_type=f32) - target[...]
    total = jnp.zeros((BLOCK, 128), f32)
    c = coeff[...]
    for q in range(CHUNKS):
        rows = pl.ds(q * BLOCK, BLOCK)
        err = error[rows, :]
        total = total + c * drawn[rows, :] * err + 0.5 * c * c * err * err
    sums = jnp.broadcast_to(jnp.sum(total, axis=1, keepdims=True), (BLOCK, 128))
    losses = jnp.zeros((TILE, 128), f32)
    fetch.wait()
    gains = advantages(table, ranks, far_ranks, source, slot, kept, owner)
    for j in range(TRAJS):
        unit = sums[j * TILE : (j + 1) * TILE]
        unit = unit + pltpu.roll(unit, 4, 0)
        unit = unit + pltpu.roll(unit, 2, 0)
        ratio = jnp.exp(-unit / values)
        clipped = jnp.clip(ratio, 1.0 - clip_range, 1.0 + clip_range)
        plain = ratio * gains[j]
        bounded = clipped * gains[j]
        losses = losses - jnp.minimum(plain, bounded)
        live = jnp.where(plain <= bounded, 1.0, 0.0)
        slope[pl.ds(j * TILE, TILE), :] = -gains[j] * ratio * live * (1.0 / UNITS)
    total = losses[0:1] + losses[1:2]
    loss_rows = in_three(total, place[0])
    bent = slope[...]
    for q in range(CHUNKS):
        rows = pl.ds(q * BLOCK, BLOCK)
        error[rows, :] = bent * (-(c * drawn[rows, :] + c * c * error[rows, :]) / values)
    dvelocity = error[...].astype(bf16)
    for par in range(2):
        back[par] = lax.dot_general(
            dvelocity, wide_head[par], (((1,), (1,)), ((), ())), preferred_element_type=f32
        )

    def backward(q, carry):
        for par in range(2):
            rows = pl.ds(pl.multiple_of(q * BLOCK, BLOCK), BLOCK)
            d = back[par, rows, :]
            final = emb[par, rows, :]
            mean = jnp.sum(d, axis=1, keepdims=True) * (1.0 / width)
            along = jnp.sum(d * final, axis=1, keepdims=True) * (1.0 / width)
            dmixed = inverse[par, rows, :][:, :1] * (d - mean - final * along)
            at = pl.multiple_of(q * (2 * BLOCK) + par * BLOCK, BLOCK)
            upstream[pl.ds(at, BLOCK), :] = (gate[...] * dmixed).astype(bf16)
        return carry

    lax.fori_loop(0, CHUNKS, backward, 0)
    loads[0].wait()
    tokens_all, hidden = act.shape
    n = hidden // 2
    share = width // 8
    contract = (((0,), (0,)), ((), ()))
    low[pl.ds(share, TILE), :] = loss_rows
    high[pl.ds(share, TILE), :] = jnp.zeros_like(loss_rows)
    for k in range(8):
        parts[k, pl.ds(share, TILE), pl.ds(0, n)] = loss_rows
        parts[k, pl.ds(share, TILE), pl.ds(n, n)] = jnp.zeros_like(loss_rows)

    def down_block(i, carry):
        cols = pl.ds(pl.multiple_of(i * 2 * share, 128), 2 * share)
        total = lax.dot_general(upstream[:, cols], act[...], contract, preferred_element_type=f32).astype(bf16)
        for j in range(2):
            k = (2 * i + j + 8 - place[0]) % 8
            piece = total[j * share : (j + 1) * share]
            parts[k, pl.ds(0, share), :] = piece

            @pl.when(k == 4)
            def _():
                low[pl.ds(0, share), :] = piece[:, :n]
                high[pl.ds(0, share), :] = piece[:, n:]

        return carry

    lax.fori_loop(0, 4, down_block, 0)
    saves = [
        pltpu.make_async_copy(a, b, sems.at[5 + i])
        for i, (a, b) in enumerate(
            ((low, down_low), (high, down_high), (parts, down_parts), (first_down, up_down), (first_up, up_up))
        )
    ]
    for copy in saves[:3]:
        copy.start()
    for copy in loads[1:]:
        copy.wait()

    def bent_rows(r, carry):
        rows = pl.ds(pl.multiple_of(r * 192, 192), 192)
        d = jnp.dot(upstream[rows, :], down_w[...], preferred_element_type=f32)
        bend[rows, :] = (d * bend[rows, :].astype(f32)).astype(bf16)
        return carry

    lax.fori_loop(0, tokens_all // 192, bent_rows, 0)
    quarter = share // 4

    def spot(i, j):
        return (j % 4 + 4 - place[1]) % 4, (2 * i + j // 4 + 8 - place[0]) % 8

    def save_piece(i, j):
        k, m = spot(i, j)
        return pltpu.make_async_copy(pieces.at[k, m], up_parts.at[k, m], out_sems.at[i * 8 + j])

    def up_block(i, carry):
        cols = pl.ds(pl.multiple_of(i * 2 * share, 128), 2 * share)
        total = lax.dot_general(mod[:, cols], bend[...], contract, preferred_element_type=f32).astype(bf16)
        for j in range(8):
            k, m = spot(i, j)
            piece = total[j * quarter : (j + 1) * quarter]
            pieces[k, m] = piece
            save_piece(i, j).start()

            @pl.when(k == 3)
            def _():
                first_down[0, m] = piece[:, n:]

            @pl.when(k == 2)
            def _():
                first_down[1, m] = piece[:, :n]
                first_up[1, m] = piece[:, n:]

            @pl.when(k == 1)
            def _():
                first_up[0, m] = piece[:, :n]

        return carry

    lax.fori_loop(0, 4, up_block, 0)
    for copy in saves[3:]:
        copy.start()

    def settle(i, carry):
        for j in range(8):
            save_piece(i, j).wait()
        return carry

    lax.fori_loop(0, 4, settle, 0)
    for copy in saves:
        copy.wait()


def in_three(value, lane):
    rows = jnp.broadcast_to(value, (TILE, 128))
    first = rows.astype(bf16).astype(f32)
    second = (rows - first).astype(bf16).astype(f32)
    third = (rows - first - second).astype(bf16).astype(f32)
    row = lax.broadcasted_iota(jnp.int32, (TILE, 128), 0)
    col = lax.broadcasted_iota(jnp.int32, (TILE, 128), 1)
    chosen = jnp.where(row == 0, first, jnp.where(row == 1, second, jnp.where(row == 2, third, 0.0)))
    tile = jnp.where(col == lane, chosen, 0.0)
    return jnp.concatenate([tile, jnp.zeros((TILE, 384), f32)], axis=1).astype(bf16)


def advantages(table, ranks, far_ranks, source, slot, kept, owner):
    def rank_of(p):
        d = source[p] - owner
        s = slot[p]
        f = jnp.clip(jnp.where(d < 0, d + 5, d + 4), 0, 7)
        return jnp.where(d == 0, ranks[s], jnp.where(d == 4, far_ranks[s], table[f, s]))

    def seek(g, state):
        end = state[0]
        after = end + kept[g]
        out = [after]
        for j in range(TRAJS):
            p = owner * TRAJS + j
            here = (p >= end) & (p < after)
            out.append(jnp.where(here, end, state[1 + 2 * j]))
            out.append(jnp.where(here, kept[g], state[2 + 2 * j]))
        return tuple(out)

    state = lax.fori_loop(0, kept.shape[0], seek, (jnp.int32(0),) + (jnp.int32(0), jnp.int32(1)) * TRAJS)
    gains = []
    for j in range(TRAJS):
        begin, count = state[1 + 2 * j], state[2 + 2 * j]

        def add(q, sums):
            rank = rank_of(q)
            return sums[0] + rank, sums[1] + rank * rank

        first, second = lax.fori_loop(begin, begin + count, add, (jnp.int32(0), jnp.int32(0)))

        def row(value):
            return jnp.full((1, 128), value, jnp.int32).astype(f32)

        counts = row(count)
        deviation = jnp.sqrt(row(count * second - first * first)) / counts
        gains.append((row(rank_of(owner * TRAJS + j)) - row(first) / counts) / jnp.maximum(deviation, 1.0))
    return gains


NEAR = (-5, -4, -3, -2, -1, 1, 2, 3)
SEQ_VALUES = 4096
UNITS = 384
SMEM = pl.BlockSpec(memory_space=pltpu.SMEM)
VMEM = pl.BlockSpec(memory_space=pltpu.VMEM)
HBM = pl.BlockSpec(memory_space=pl.ANY)


def wide_add(*parts):
    total = parts[0].astype(f32)
    for part in parts[1:]:
        total = total + part.astype(f32)
    return total


def call(kernel, shapes, count, **kw):
    return pl.pallas_call(
        kernel,
        out_shape=tuple(jax.ShapeDtypeStruct(shape, dtype) for shape, dtype in shapes),
        in_specs=[VMEM] * count,
        out_specs=(VMEM,) * len(shapes),
        **kw,
    )


def fold_kernel(mine, got, down, up, low, high, own):
    n = mine.shape[2] // 2
    total = [mine[k].astype(f32) + got[k].astype(f32) for k in range(4)]
    down[0] = total[3][:, n:].astype(bf16)
    down[1] = total[2][:, :n].astype(bf16)
    up[0] = total[1][:, :n].astype(bf16)
    up[1] = total[2][:, n:].astype(bf16)
    low[...] = total[3][:, :n].astype(bf16)
    high[...] = total[1][:, n:].astype(bf16)
    own[...] = total[0]


def onward_kernel(low, high, own, from_up, from_down, down, up, kept):
    n = low.shape[1]
    down[...] = (low[...].astype(f32) + from_up[1].astype(f32)).astype(bf16)
    up[...] = (high[...].astype(f32) + from_down[1].astype(f32)).astype(bf16)
    kept[:, pl.ds(0, n)] = own[:, pl.ds(0, n)] + from_down[0].astype(f32)
    kept[:, pl.ds(n, n)] = own[:, pl.ds(n, n)] + from_up[0].astype(f32)


def close_kernel(ranks, kept, late_up, late_down, out):
    n = late_up.shape[1]
    out[:, pl.ds(0, n)] = (kept[:, pl.ds(0, n)] + late_up[...].astype(f32)).astype(bf16)
    out[:, pl.ds(n, n)] = (kept[:, pl.ds(n, n)] + late_down[...].astype(f32)).astype(bf16)
    col = lax.broadcasted_iota(jnp.int32, (16, 128), 1)
    row = lax.broadcasted_iota(jnp.int32, (16, 128), 0)
    values = jnp.zeros((16, 128), jnp.int32)
    for i in range(ranks.shape[0]):
        values = jnp.where(col == i, ranks[i], values)
    values = jnp.where(row == 0, values // 32, jnp.where(row == 1, values % 32, 0))
    out[:, pl.ds(2 * n, 128)] = jnp.zeros((out.shape[0], 128), bf16)
    out[pl.ds(0, 16), pl.ds(2 * n, 128)] = values.astype(f32).astype(bf16)


def half_add_kernel(part, recv, out, *, lead):
    n = recv.shape[1]
    total = (part[0, :, pl.ds(lead * n, n)].astype(f32) + recv[...].astype(f32)).astype(bf16)
    out[:, pl.ds(lead * n, n)] = total
    out[:, pl.ds((1 - lead) * n, n)] = part[0, :, pl.ds((1 - lead) * n, n)]


def half_add(parts, index, recv, lead):
    block = parts.shape[1:]
    return pl.pallas_call(
        lambda *refs: half_add_kernel(*refs, lead=lead),
        grid=(1,),
        out_shape=jax.ShapeDtypeStruct(block, bf16),
        in_specs=[
            pl.BlockSpec((1, *block), lambda i: (index, 0, 0)),
            pl.BlockSpec(recv.shape, lambda i: (0, 0)),
        ],
        out_specs=pl.BlockSpec(block, lambda i: (0, 0)),
        name="ring_second",
    )(parts, recv)


def ring_of_eight(parts, low, high):
    down = half_add(parts, 5, move(low, "z", -1), 0)
    up = half_add(parts, 3, move(high, "z", 1), 1)
    for step in (2, 1):
        from_up = move(down, "z", -1)
        from_down = move(up, "z", 1)
        down = wide_add(parts[8 - step], from_up).astype(bf16)
        up = wide_add(parts[step], from_down).astype(bf16)
    return move(down, "z", -1), move(up, "z", 1)


def turn_kernel(place, part, from_up, from_down, rest, down, up):
    n = rest.shape[2] // 2
    own = rest.shape[1] - TILE

    def summed(rows):
        return part[0, rows, :].astype(f32) + from_up[rows, :].astype(f32) + from_down[rows, :].astype(f32)

    loss = jnp.sum(jnp.sum(summed(pl.ds(4 * own, TILE))[:, :128], axis=1, keepdims=True), axis=0, keepdims=True)
    loss_rows = in_three(jnp.broadcast_to(loss, (1, 128)), place[1])
    blank = jnp.zeros_like(loss_rows)
    last = pl.ds(own, TILE)
    for k in range(4):
        rest[k, last, pl.ds(0, n)] = loss_rows
        rest[k, last, pl.ds(n, n)] = blank
    down[0, last, :] = blank
    down[1, last, :] = loss_rows
    up[0, last, :] = loss_rows
    up[1, last, :] = blank
    first = pl.ds(0, own)
    for a in range(4):
        total = summed(pl.ds(a * own, own)).astype(bf16)
        k = (a + 4 - place[1]) % 4
        rest[k, first, :] = total

        @pl.when(k == 3)
        def _():
            down[0, first, :] = total[:, n:]

        @pl.when(k == 2)
        def _():
            down[1, first, :] = total[:, :n]
            up[1, first, :] = total[:, n:]

        @pl.when(k == 1)
        def _():
            up[0, first, :] = total[:, :n]


def last_kernel(part, from_down, from_up, late_up, late_down, grad, loss):
    n = late_up.shape[1]
    own = grad.shape[0]
    low = part[0, :, pl.ds(0, n)].astype(f32) + from_down[0].astype(f32) + late_up[...].astype(f32)
    grad[:, pl.ds(0, n)] = low[:own]
    rows = pl.ds(0, own)
    grad[:, pl.ds(n, n)] = (
        part[0, rows, pl.ds(n, n)].astype(f32) + from_up[0, rows, :].astype(f32) + late_down[rows, :].astype(f32)
    )
    total = jnp.sum(jnp.sum(low[own:, :128], axis=1, keepdims=True), axis=0, keepdims=True)
    loss[...] = jnp.broadcast_to(total * (1.0 / UNITS), loss.shape)


def shards(
    latents,
    noise,
    behavior_velocity,
    timestep,
    reward_rank_integer,
    surviving_source_index,
    surviving_slot_index,
    group_kept_count,
    patch_input_weight,
    modulation_lookup,
    up_projection_weight,
    down_projection_weight,
    velocity_head_weight,
):
    z, x, y, c = (lax.axis_index(a) for a in ("z", "x", "y", "c"))
    owner = lax.axis_index(DP)
    ranks_dp = lax.axis_size(DP)
    surviving = surviving_source_index.shape[0]
    trajs = surviving // ranks_dp
    steps = timestep.shape[1]
    lead = owner * trajs
    sources = lax.dynamic_slice_in_dim(surviving_source_index, lead, trajs)
    slots = lax.dynamic_slice_in_dim(surviving_slot_index, lead, trajs)
    next_lead = jnp.minimum(owner + 1, ranks_dp - 1) * trajs
    next_slots = lax.dynamic_slice_in_dim(surviving_slot_index, next_lead, trajs)
    capacity = latents.shape[0]

    def pairs(a):
        return a.reshape(capacity, steps, 32, 128).transpose(0, 2, 1, 3).reshape(capacity, 64, 128)

    width = patch_input_weight.shape[1]
    rows = 8 * 2 * trajs * 8
    one = jax.ShapeDtypeStruct((TRAJS, 80, 128), bf16)
    two = jax.ShapeDtypeStruct((TRAJS, 2, PAIRS, 128), bf16)
    out_first, out_second, own_first, own_second = pl.pallas_call(
        gather_kernel,
        out_shape=(one, two, one, two),
        in_specs=[SMEM, SMEM, HBM, HBM, HBM],
        out_specs=(VMEM, VMEM, VMEM, VMEM),
        scratch_shapes=[pltpu.SemaphoreType.DMA((6 * TRAJS,))],
        name="gather_slots",
    )(
        jnp.concatenate([next_slots, slots]), timestep,
        pairs(latents), pairs(noise), pairs(behavior_velocity),
    )
    onward = [(i, i + 1) for i in range(ranks_dp - 1)]
    near = [
        ((d + hop) * 8 + f, d * 8 + f) for d in range(ranks_dp) for f, hop in enumerate(NEAR) if 0 <= d + hop < ranks_dp
    ]
    near_ranks = lax.ppermute(reward_rank_integer, ("z", "x", "y", "c"), near)
    far_ranks = lax.ppermute(reward_rank_integer, DP, [(d + 4, d) for d in range(ranks_dp - 4)])
    came = lax.ppermute(out_first, DP, onward)
    came_late = lax.ppermute(out_second, DP, onward)
    left = (sources != owner).astype(jnp.int32)
    ks = (y + jnp.arange(4, dtype=jnp.int32)) % 4 * 2
    order = jnp.concatenate([ks + (1 - c), ks + c])
    hidden = up_projection_weight.shape[1]
    half = rows // 2
    tokens, stamps, modulated, activated, bend, proj_other, proj_own = pl.pallas_call(
        forward_kernel,
        out_shape=(
            jax.ShapeDtypeStruct((CHUNKS * BLOCK, 128), bf16),
            jax.ShapeDtypeStruct((BLOCK, 128), f32),
            jax.ShapeDtypeStruct((rows, width), bf16),
            jax.ShapeDtypeStruct((rows, hidden), bf16),
            jax.ShapeDtypeStruct((rows, hidden), bf16),
            jax.ShapeDtypeStruct((half, width), bf16),
            jax.ShapeDtypeStruct((half, width), bf16),
        ),
        in_specs=[SMEM, SMEM, VMEM, VMEM, VMEM, VMEM, HBM, HBM],
        out_specs=(VMEM, VMEM, HBM, HBM, HBM, HBM, HBM),
        scratch_shapes=[
            pltpu.VMEM((TRAJS * 80, 128), f32),
            pltpu.VMEM((CHUNKS * BLOCK, 128), f32),
            pltpu.VMEM((2, 128, width), bf16),
            pltpu.VMEM((2, CHUNKS * BLOCK, width), f32),
            pltpu.VMEM((BLOCK, width), f32),
            pltpu.VMEM((BLOCK, width), f32),
            pltpu.VMEM((width, hidden), bf16),
            pltpu.VMEM((width, hidden), bf16),
            pltpu.VMEM((rows, width), bf16),
            pltpu.VMEM((rows, hidden), bf16),
            pltpu.VMEM((rows, hidden), bf16),
            pltpu.VMEM((rows, width), bf16),
            pltpu.SemaphoreType.DMA((7,)),
        ],
        compiler_params=pltpu.CompilerParams(vmem_limit_bytes=50 << 20),
        name="forward",
    )(left, order, came, own_first, patch_input_weight, modulation_lookup, up_projection_weight, down_projection_weight)
    got = swap(proj_other, "c", 1)
    n = width // 2
    piece = rows // 8
    down, up, low, high, own = call(
        fold_kernel,
        [((2, piece, n), bf16)] * 2 + [((piece, n), bf16)] * 2 + [((piece, width), f32)],
        2,
        name="fold",
    )(proj_own.reshape(4, piece, width), got.reshape(4, piece, width))
    from_up = move(down, "y", -1)
    from_down = move(up, "y", 1)
    from_up, from_down, came_late = lax.optimization_barrier((from_up, from_down, came_late))
    down, up, kept = call(
        onward_kernel, [((piece, n), bf16)] * 2 + [((piece, width), f32)], 5, name="onward"
    )(low, high, own, from_up, from_down)
    late_up = move(down, "y", -1)
    late_down = move(up, "y", 1)
    own = pl.pallas_call(
        close_kernel,
        out_shape=jax.ShapeDtypeStruct((piece, width + 128), bf16),
        in_specs=[SMEM] + [VMEM] * 3,
        out_specs=VMEM,
        name="close",
    )(near_ranks, kept, late_up, late_down)
    after = move(own, "y", -1)
    before = move(own, "y", 1)
    far = jnp.concatenate([move(after[:, :n], "y", -1), move(before[:, n:], "y", 1)], axis=1)
    summed_own = jnp.concatenate([own, after, far, before], axis=0)
    summed_other = swap(summed_own, "c", 1)
    place = jnp.stack([z, x]).astype(jnp.int32)
    own_rows = width // ranks_dp
    m = hidden // 2
    share = 4 * own_rows
    down_parts, down_low, down_high, up_parts, up_first_down, up_first_up = pl.pallas_call(
        backward_kernel,
        out_shape=(
            jax.ShapeDtypeStruct((8, share + TILE, hidden), bf16),
            jax.ShapeDtypeStruct((share + TILE, m), bf16),
            jax.ShapeDtypeStruct((share + TILE, m), bf16),
            jax.ShapeDtypeStruct((4, 8, own_rows, hidden), bf16),
            jax.ShapeDtypeStruct((2, 8, own_rows, m), bf16),
            jax.ShapeDtypeStruct((2, 8, own_rows, m), bf16),
        ),
        in_specs=[SMEM] * 8 + [VMEM] * 9 + [HBM] * 4,
        out_specs=(HBM,) * 6,
        scratch_shapes=[
            pltpu.VMEM((CHUNKS * BLOCK, 128), f32),
            pltpu.VMEM((CHUNKS * BLOCK, 128), f32),
            pltpu.VMEM((2, 128, width), bf16),
            pltpu.VMEM((2, width, 128), bf16),
            pltpu.VMEM((2, CHUNKS * BLOCK, width), f32),
            pltpu.VMEM((2, CHUNKS * BLOCK, width), bf16),
            pltpu.VMEM((2, CHUNKS * BLOCK, width), f32),
            pltpu.VMEM((2, CHUNKS * BLOCK, 128), f32),
            pltpu.VMEM((BLOCK, width), f32),
            pltpu.VMEM((CHUNKS * BLOCK, 128), f32),
            pltpu.VMEM((BLOCK, 128), f32),
            pltpu.VMEM((BLOCK, 128), f32),
            pltpu.VMEM((8, 128), jnp.int32),
            pltpu.SMEM((8, 128), jnp.int32),
            pltpu.VMEM((rows, hidden), bf16),
            pltpu.VMEM((rows, hidden), bf16),
            pltpu.VMEM((rows, width), bf16),
            pltpu.VMEM((width, hidden), bf16),
            pltpu.VMEM((rows, width), bf16),
            pltpu.VMEM((8, share + TILE, hidden), bf16),
            pltpu.VMEM((share + TILE, m), bf16),
            pltpu.VMEM((share + TILE, m), bf16),
            pltpu.VMEM((4, 8, own_rows, hidden), bf16),
            pltpu.VMEM((2, 8, own_rows, m), bf16),
            pltpu.VMEM((2, 8, own_rows, m), bf16),
            pltpu.SemaphoreType.DMA((10,)),
            pltpu.SemaphoreType.DMA((32,)),
        ],
        compiler_params=pltpu.CompilerParams(vmem_limit_bytes=60 << 20),
        name="backward",
    )(
        left, order, reward_rank_integer, far_ranks, surviving_source_index, surviving_slot_index, group_kept_count,
        place, summed_other, summed_own, tokens, stamps, came_late, own_second,
        patch_input_weight, velocity_head_weight, modulation_lookup,
        activated, bend, modulated, down_projection_weight,
    )

    from_up = move(up_first_down, "x", -1)
    from_down = move(up_first_up, "x", 1)
    second_down = wide_add(up_parts[3, :, :, :m], from_up[1]).astype(bf16)
    second_up = wide_add(up_parts[1, :, :, m:], from_down[1]).astype(bf16)
    late_up = move(second_down, "x", -1)
    late_down = move(second_up, "x", 1)

    from_z_up, from_z_down = ring_of_eight(down_parts, down_low, down_high)
    tall = share + TILE
    short = own_rows + TILE
    rest, turn_down, turn_up = pl.pallas_call(
        turn_kernel,
        grid=(1,),
        out_shape=(
            jax.ShapeDtypeStruct((4, short, hidden), bf16),
            jax.ShapeDtypeStruct((2, short, m), bf16),
            jax.ShapeDtypeStruct((2, short, m), bf16),
        ),
        in_specs=[
            SMEM,
            pl.BlockSpec((1, tall, hidden), lambda i: (0, 0, 0)),
            pl.BlockSpec((tall, hidden), lambda i: (0, 0)),
            pl.BlockSpec((tall, hidden), lambda i: (0, 0)),
        ],
        out_specs=(
            pl.BlockSpec((4, short, hidden), lambda i: (0, 0, 0)),
            pl.BlockSpec((2, short, m), lambda i: (0, 0, 0)),
            pl.BlockSpec((2, short, m), lambda i: (0, 0, 0)),
        ),
        name="turn",
    )(place, down_parts, from_z_up, from_z_down)
    up_x = jnp.concatenate(
        [
            wide_add(up_parts[0, :, :, :m], from_down[0], late_up),
            wide_add(up_parts[0, :, :, m:], from_up[0], late_down),
        ],
        axis=2,
    ).astype(bf16)
    far_up = move(turn_down, "x", -1)
    far_down = move(turn_up, "x", 1)
    second_down = wide_add(rest[3, :, :m], far_up[1]).astype(bf16)
    second_up = wide_add(rest[1, :, m:], far_down[1]).astype(bf16)
    last_up = move(second_down, "x", -1)
    last_down = move(second_up, "x", 1)
    down_grad, loss = pl.pallas_call(
        last_kernel,
        grid=(1,),
        out_shape=(
            jax.ShapeDtypeStruct((own_rows, hidden), f32),
            jax.ShapeDtypeStruct((TILE, 128), f32),
        ),
        in_specs=[
            pl.BlockSpec((1, short, hidden), lambda i: (0, 0, 0)),
            pl.BlockSpec((1, short, m), lambda i: (0, 0, 0)),
            pl.BlockSpec((1, short, m), lambda i: (0, 0, 0)),
            pl.BlockSpec((short, m), lambda i: (0, 0)),
            pl.BlockSpec((short, m), lambda i: (0, 0)),
        ],
        out_specs=(
            pl.BlockSpec((own_rows, hidden), lambda i: (0, 0)),
            pl.BlockSpec((TILE, 128), lambda i: (0, 0)),
        ),
        name="last",
    )(rest, far_down, far_up, last_up, last_down)
    end_up, end_down = ring_of_eight(up_x, up_x[4, :, :m], up_x[4, :, m:])
    up_grad = wide_add(up_x[0], end_up, end_down)
    return (up_grad, down_grad, loss[0, 0])


def solution(mesh):
    finer = Mesh(mesh.devices.reshape(8, 4, 4, 2), ("z", "x", "y", "c"))
    dp, fsdp = ("z", "x"), ("y", "c")
    in_specs = (
        P(dp, None, None),
        P(dp, None, None),
        P(dp, None, None),
        P(dp, None),
        P(dp),
        P(),
        P(),
        P(),
        P(),
        P(),
        P(None, fsdp),
        P(None, fsdp),
        P(),
    )
    out_specs = (P(dp, fsdp), P(dp, fsdp), P())
    return jax.shard_map(
        shards, mesh=finer, in_specs=in_specs, out_specs=out_specs, check_vma=False
    )
```

```python
import jax
import jax.numpy as jnp
from jax import lax
from jax.experimental import pallas as pl
from jax.experimental.pallas import tpu as pltpu
from jax.sharding import Mesh
from jax.sharding import PartitionSpec as P

KSTEPS = 10
DP = ("z", "x")
clip_range = 0.2
noise_level = 0.7
norm_eps = 1e-06
bf16 = jnp.bfloat16
f32 = jnp.float32


def move(value, axis, steps):
    count = lax.axis_size(axis)
    return lax.ppermute(value, axis, [(i, (i + steps) % count) for i in range(count)])


def swap(value, axis, bit):
    count = lax.axis_size(axis)
    return lax.ppermute(value, axis, [(i, i ^ bit) for i in range(count)])


TRAJS = 6
PAIRS = 64
TILE = 8
BLOCK = TRAJS * TILE
CHUNKS = 8


def position():
    z, x, y, c = (lax.axis_index(a) for a in ("z", "x", "y", "c"))
    return z, x, y, c, z * 4 + x


def chunk_owner(q):
    _, _, y, c, _ = position()
    return (y + q % 4) % 4 * 2 + (1 - c if q < 4 else c)


def gather_kernel(slot_table, stamps, latents, noise, behavior, out_first, out_second, own_first, own_second, sems):
    copies = []
    owner = position()[4]
    following = jnp.minimum(owner + 1, 31)
    slots = [slot_table[following * TRAJS + j] for j in range(TRAJS)]
    slots += [slot_table[owner * TRAJS + j] for j in range(TRAJS)]
    for j in range(2 * TRAJS):
        slot = slots[j]
        first, second = (out_first, out_second) if j < TRAJS else (own_first, own_second)
        k = j % TRAJS
        for i, (source, target) in enumerate(
            ((latents, first.at[k, pl.ds(0, PAIRS)]), (noise, second.at[k, 0]), (behavior, second.at[k, 1]))
        ):
            copy = pltpu.make_async_copy(source.at[slot], target, sems.at[3 * j + i])
            copy.start()
            copies.append(copy)
    step = lax.broadcasted_iota(jnp.int32, (16, 128), 0) % 2
    for j in range(2 * TRAJS):
        slot = slots[j]
        tile = jnp.where(step == 0, stamps[0, slot], stamps[1, slot])
        first = out_first if j < TRAJS else own_first
        first[j % TRAJS, pl.ds(PAIRS, 16), :] = tile.astype(f32).astype(bf16)
    for copy in copies:
        copy.wait()


def modulation_rows(stamp_tile, lookup, index):
    rows = jnp.zeros((TILE, lookup.shape[2]), f32)
    for k in range(KSTEPS):
        rows = jnp.where(stamp_tile == k, lookup[k, pl.ds(index, 1), :], rows)
    return rows


def widened(weight, wide, dim):
    size = weight.shape[dim]
    wide[...] = jnp.zeros(wide.shape, wide.dtype)
    if dim == 0:
        wide[0, pl.ds(0, size), :] = weight[...]
        wide[1, pl.ds(size, size), :] = weight[...]
    else:
        wide[0, :, pl.ds(0, size)] = weight[...]
        wide[1, :, pl.ds(size, size)] = weight[...]


def gelu_both(v):
    k = 0.7978845608028654
    square = v * v
    t = jnp.tanh(k * (v + 0.044715 * (square * v)))
    half = 0.5 * (1.0 + t)
    return v * half, half + (0.5 * k) * v * (1.0 - t * t) * (1.0 + (3 * 0.044715) * square)


def forward_kernel(
    source, came, mine, weight_in, lookup_in, up_weight, down_weight,
    tokens, stamps, mod_out, act_out, bend_out, proj_other, proj_own,
    weight, lookup, merged, sorted_, wide, emb, scale, shift, up_w, down_w, modulated, activated, bend, proj, sems,
):
    width = weight.shape[1]
    owner = position()[4]
    load_weight = pltpu.make_async_copy(weight_in, weight, sems.at[7])
    load_lookup = pltpu.make_async_copy(lookup_in, lookup, sems.at[8])
    load_weight.start()
    load_lookup.start()
    load_up = pltpu.make_async_copy(up_weight, up_w, sems.at[0])
    load_down = pltpu.make_async_copy(down_weight, down_w, sems.at[1])
    load_up.start()
    load_down.start()
    for j in range(TRAJS):
        away = source[owner * TRAJS + j] != owner
        merged[pl.ds(j * 80, 80), :] = jnp.where(away, came[j].astype(f32), mine[j].astype(f32))
    for q in range(CHUNKS):
        at_owner = chunk_owner(q)
        for j in range(TRAJS):
            at = pl.multiple_of(j * 80 + at_owner * TILE, TILE)
            sorted_[pl.ds(q * BLOCK + j * TILE, TILE), :] = merged[pl.ds(at, TILE), :]
    tokens[...] = sorted_[...].astype(bf16)
    load_weight.wait()
    load_lookup.wait()
    widened(weight, wide, 0)
    for j in range(TRAJS):
        stamp = merged[pl.ds(j * 80 + PAIRS, TILE), :]
        stamps[pl.ds(j * TILE, TILE), :] = stamp
        stamp = stamp[:, :1]
        shift[pl.ds(j * TILE, TILE), :] = modulation_rows(stamp, lookup, 0)
        scale[pl.ds(j * TILE, TILE), :] = 1.0 + modulation_rows(stamp, lookup, 1)
    for par in range(2):
        emb[par] = jnp.dot(tokens[...], wide[par], preferred_element_type=f32)

    def norm(q, carry):
        for par in range(2):
            values = emb[par, pl.ds(pl.multiple_of(q * BLOCK, BLOCK), BLOCK), :]
            center = values - jnp.sum(values, axis=1, keepdims=True) * (1.0 / width)
            variance = jnp.sum(center * center, axis=1, keepdims=True) * (1.0 / width)
            normed = center * lax.rsqrt(variance + norm_eps)
            at = pl.multiple_of(q * (2 * BLOCK) + par * BLOCK, BLOCK)
            modulated[pl.ds(at, BLOCK), :] = (normed * scale[...] + shift[...]).astype(bf16)
        return carry

    lax.fori_loop(0, CHUNKS, norm, 0)
    save_mod = pltpu.make_async_copy(modulated, mod_out, sems.at[2])
    save_mod.start()
    load_up.wait()
    load_down.wait()

    def hidden(r, carry):
        rows = pl.ds(pl.multiple_of(r * 192, 192), 192)
        pre = jnp.dot(modulated[rows, :], up_w[...], preferred_element_type=f32)
        value, slope = gelu_both(pre)
        value = value.astype(bf16)
        activated[rows, :] = value
        bend[rows, :] = slope.astype(bf16)
        proj[rows, :] = lax.dot_general(
            value, down_w[...], (((1,), (1,)), ((), ())), preferred_element_type=f32
        ).astype(bf16)
        return carry

    half = modulated.shape[0] // 2
    lax.fori_loop(0, 2, hidden, 0)
    save_other = pltpu.make_async_copy(proj.at[pl.ds(0, half)], proj_other, sems.at[3])
    save_other.start()
    lax.fori_loop(2, 4, hidden, 0)
    save_own = pltpu.make_async_copy(proj.at[pl.ds(half, half)], proj_own, sems.at[4])
    save_own.start()
    save_act = pltpu.make_async_copy(activated, act_out, sems.at[5])
    save_act.start()
    save_bend = pltpu.make_async_copy(bend, bend_out, sems.at[6])
    save_bend.start()
    for copy in (save_mod, save_other, save_own, save_act, save_bend):
        copy.wait()


def backward_kernel(
    ranks, far_ranks, source, slot, kept,
    other, own, tokens, stamps, came, mine, weight_in, head, lookup_in,
    act_in, bend_in, mod_in, down_in,
    down_parts, down_low, down_high, up_parts,
    weight, lookup, drawn, target, wide, wide_head, emb, rounded, back, inverse, gate, error, slope, coeff,
    table_v, table, act, bend, mod, down_w, upstream, parts, low, high, pieces,
    sems, out_sems,
):
    z, x, y, c, owner = position()
    place = (z, x)
    load_weight = pltpu.make_async_copy(weight_in, weight, sems.at[10])
    load_lookup = pltpu.make_async_copy(lookup_in, lookup, sems.at[11])
    load_weight.start()
    load_lookup.start()
    loads = [
        pltpu.make_async_copy(a, b, sems.at[i])
        for i, (a, b) in enumerate(((act_in, act), (down_in, down_w), (bend_in, bend), (mod_in, mod)))
    ]
    for copy in loads:
        copy.start()
    for q in range(CHUNKS):
        info = (other if q < 4 else own)[(q + y) % 4, pl.ds(0, 16), pl.ds(weight.shape[1], 128)].astype(f32)
        table_v[pl.ds(chunk_owner(q), 1), :] = (info[0:1] * 32.0 + info[1:2]).astype(jnp.int32)
    fetch = pltpu.make_async_copy(table_v, table, sems.at[4])
    fetch.start()
    width = weight.shape[1]
    values = SEQ_VALUES
    load_weight.wait()
    load_lookup.wait()
    widened(weight, wide, 0)
    widened(head, wide_head, 1)
    for j in range(TRAJS):
        stamp = stamps[pl.ds(j * TILE, TILE), :]
        gate[pl.ds(j * TILE, TILE), :] = modulation_rows(stamp[:, :1], lookup, 2)
        level = 1.0 - stamp * (1.0 / KSTEPS)
        coeff[pl.ds(j * TILE, TILE), :] = (
            jnp.sqrt((1.0 / KSTEPS) * (1.0 - level + 1.0 / KSTEPS) / level) / noise_level
        )
        away = source[owner * TRAJS + j] != owner
        picked = jnp.where(away, came[j].astype(f32), mine[j].astype(f32))
        emb[0, pl.ds(0, PAIRS), pl.ds(0, 128)] = picked[0]
        emb[0, pl.ds(PAIRS, PAIRS), pl.ds(0, 128)] = picked[1]
        for q in range(CHUNKS):
            at = pl.multiple_of(chunk_owner(q) * TILE, TILE)
            drawn[pl.ds(q * BLOCK + j * TILE, TILE), :] = emb[0, pl.ds(at, TILE), pl.ds(0, 128)]
            at = pl.multiple_of(PAIRS + chunk_owner(q) * TILE, TILE)
            target[pl.ds(q * BLOCK + j * TILE, TILE), :] = emb[0, pl.ds(at, TILE), pl.ds(0, 128)]
    for par in range(2):
        emb[par] = jnp.dot(tokens[...], wide[par], preferred_element_type=f32)

    def forward(q, summed):
        for par in range(2):
            rows = pl.ds(pl.multiple_of(q * BLOCK, BLOCK), BLOCK)
            mixed = emb[par, rows, :] + gate[...] * summed[
                (q + y) % 4, pl.ds(par * BLOCK, BLOCK), pl.ds(0, width)
            ].astype(f32)
            center = mixed - jnp.sum(mixed, axis=1, keepdims=True) * (1.0 / width)
            variance = jnp.sum(center * center, axis=1, keepdims=True) * (1.0 / width)
            scale = lax.rsqrt(variance + norm_eps)
            final = center * scale
            emb[par, rows, :] = final
            rounded[par, rows, :] = final.astype(bf16)
            inverse[par, rows, :] = jnp.broadcast_to(scale, (BLOCK, 128))

    def first_half(q, carry):
        forward(q, other)
        return carry

    def second_half(q, carry):
        forward(q + 4, own)
        return carry

    lax.fori_loop(0, 4, first_half, 0)
    lax.fori_loop(0, 4, second_half, 0)
    velocity = jnp.dot(rounded[0], wide_head[0], preferred_element_type=f32)
    error[...] = velocity + jnp.dot(rounded[1], wide_head[1], preferred_element_type=f32) - target[...]
    total = jnp.zeros((BLOCK, 128), f32)
    c = coeff[...]
    for q in range(CHUNKS):
        rows = pl.ds(q * BLOCK, BLOCK)
        err = error[rows, :]
        total = total + c * drawn[rows, :] * err + 0.5 * c * c * err * err
    sums = jnp.broadcast_to(jnp.sum(total, axis=1, keepdims=True), (BLOCK, 128))
    losses = jnp.zeros((TILE, 128), f32)
    fetch.wait()
    gains = advantages(table, ranks, far_ranks, source, slot, kept, owner)
    for j in range(TRAJS):
        unit = sums[j * TILE : (j + 1) * TILE]
        unit = unit + pltpu.roll(unit, 4, 0)
        unit = unit + pltpu.roll(unit, 2, 0)
        ratio = jnp.exp(-unit / values)
        clipped = jnp.clip(ratio, 1.0 - clip_range, 1.0 + clip_range)
        plain = ratio * gains[j]
        bounded = clipped * gains[j]
        losses = losses - jnp.minimum(plain, bounded)
        live = jnp.where(plain <= bounded, 1.0, 0.0)
        slope[pl.ds(j * TILE, TILE), :] = -gains[j] * ratio * live * (1.0 / UNITS)
    total = losses[0:1] + losses[1:2]
    loss_rows = in_three(total, place[0])
    bent = slope[...]
    for q in range(CHUNKS):
        rows = pl.ds(q * BLOCK, BLOCK)
        error[rows, :] = bent * (-(c * drawn[rows, :] + c * c * error[rows, :]) / values)
    dvelocity = error[...].astype(bf16)
    for par in range(2):
        back[par] = lax.dot_general(
            dvelocity, wide_head[par], (((1,), (1,)), ((), ())), preferred_element_type=f32
        )

    def backward(q, carry):
        for par in range(2):
            rows = pl.ds(pl.multiple_of(q * BLOCK, BLOCK), BLOCK)
            d = back[par, rows, :]
            final = emb[par, rows, :]
            mean = jnp.sum(d, axis=1, keepdims=True) * (1.0 / width)
            along = jnp.sum(d * final, axis=1, keepdims=True) * (1.0 / width)
            dmixed = inverse[par, rows, :][:, :1] * (d - mean - final * along)
            at = pl.multiple_of(q * (2 * BLOCK) + par * BLOCK, BLOCK)
            upstream[pl.ds(at, BLOCK), :] = (gate[...] * dmixed).astype(bf16)
        return carry

    lax.fori_loop(0, CHUNKS, backward, 0)
    loads[0].wait()
    tokens_all, hidden = act.shape
    n = hidden // 2
    share = width // 8
    contract = (((0,), (0,)), ((), ()))
    low[pl.ds(share, TILE), :] = loss_rows
    high[pl.ds(share, TILE), :] = jnp.zeros_like(loss_rows)
    for k in range(8):
        parts[k, pl.ds(share, TILE), pl.ds(0, n)] = loss_rows
        parts[k, pl.ds(share, TILE), pl.ds(n, n)] = jnp.zeros_like(loss_rows)

    def down_block(i, carry):
        cols = pl.ds(pl.multiple_of(i * 2 * share, 128), 2 * share)
        total = lax.dot_general(upstream[:, cols], act[...], contract, preferred_element_type=f32).astype(bf16)
        for j in range(2):
            k = (2 * i + j + 8 - place[0]) % 8
            piece = total[j * share : (j + 1) * share]
            parts[k, pl.ds(0, share), :] = piece

            @pl.when(k == 4)
            def _():
                low[pl.ds(0, share), :] = piece[:, :n]
                high[pl.ds(0, share), :] = piece[:, n:]

        return carry

    lax.fori_loop(0, 4, down_block, 0)
    saves = [
        pltpu.make_async_copy(a, b, sems.at[5 + i])
        for i, (a, b) in enumerate(((low, down_low), (high, down_high), (parts, down_parts)))
    ]
    for copy in saves:
        copy.start()
    for copy in loads[1:]:
        copy.wait()

    def bent_rows(r, carry):
        rows = pl.ds(pl.multiple_of(r * 192, 192), 192)
        d = jnp.dot(upstream[rows, :], down_w[...], preferred_element_type=f32)
        bend[rows, :] = (d * bend[rows, :].astype(f32)).astype(bf16)
        return carry

    lax.fori_loop(0, tokens_all // 192, bent_rows, 0)
    quarter = share // 4

    def save_pieces(i):
        rows = pl.ds(2 * i, 2)
        return pltpu.make_async_copy(pieces.at[:, rows], up_parts.at[:, rows], out_sems.at[i])

    def up_block(i, carry):
        cols = pl.ds(pl.multiple_of(i * 2 * share, 128), 2 * share)
        total = lax.dot_general(mod[:, cols], bend[...], contract, preferred_element_type=f32).astype(bf16)
        for j in range(8):
            pieces[j % 4, 2 * i + j // 4] = total[j * quarter : (j + 1) * quarter]
        save_pieces(i).start()
        return carry

    lax.fori_loop(0, 4, up_block, 0)
    for i in range(4):
        save_pieces(i).wait()
    for copy in saves:
        copy.wait()


def in_three(value, lane):
    rows = jnp.broadcast_to(value, (TILE, 128))
    first = rows.astype(bf16).astype(f32)
    second = (rows - first).astype(bf16).astype(f32)
    third = (rows - first - second).astype(bf16).astype(f32)
    row = lax.broadcasted_iota(jnp.int32, (TILE, 128), 0)
    col = lax.broadcasted_iota(jnp.int32, (TILE, 128), 1)
    chosen = jnp.where(row == 0, first, jnp.where(row == 1, second, jnp.where(row == 2, third, 0.0)))
    tile = jnp.where(col == lane, chosen, 0.0)
    return jnp.concatenate([tile, jnp.zeros((TILE, 384), f32)], axis=1).astype(bf16)


def advantages(table, ranks, far_ranks, source, slot, kept, owner):
    def rank_of(p):
        d = source[p] - owner
        s = slot[p]
        f = jnp.clip(jnp.where(d < 0, d + 5, d + 4), 0, 7)
        return jnp.where(d == 0, ranks[s], jnp.where(d == 4, far_ranks[s], table[f, s]))

    def seek(g, state):
        end = state[0]
        after = end + kept[g]
        out = [after]
        for j in range(TRAJS):
            p = owner * TRAJS + j
            here = (p >= end) & (p < after)
            out.append(jnp.where(here, end, state[1 + 2 * j]))
            out.append(jnp.where(here, kept[g], state[2 + 2 * j]))
        return tuple(out)

    state = lax.fori_loop(0, kept.shape[0], seek, (jnp.int32(0),) + (jnp.int32(0), jnp.int32(1)) * TRAJS)
    gains = []
    for j in range(TRAJS):
        begin, count = state[1 + 2 * j], state[2 + 2 * j]

        def add(q, sums):
            rank = rank_of(q)
            return sums[0] + rank, sums[1] + rank * rank

        first, second = lax.fori_loop(begin, begin + count, add, (jnp.int32(0), jnp.int32(0)))

        def row(value):
            return jnp.full((1, 128), value, jnp.int32).astype(f32)

        counts = row(count)
        deviation = jnp.sqrt(row(count * second - first * first)) / counts
        gains.append((row(rank_of(owner * TRAJS + j)) - row(first) / counts) / jnp.maximum(deviation, 1.0))
    return gains


NEAR = (-5, -4, -3, -2, -1, 1, 2, 3)
SEQ_VALUES = 4096
UNITS = 384
SMEM = pl.BlockSpec(memory_space=pltpu.SMEM)
VMEM = pl.BlockSpec(memory_space=pltpu.VMEM)
HBM = pl.BlockSpec(memory_space=pltpu.HBM)


def wide_add(*parts):
    total = parts[0].astype(f32)
    for part in parts[1:]:
        total = total + part.astype(f32)
    return total


def call(kernel, shapes, count, **kw):
    return pl.pallas_call(
        kernel,
        out_shape=tuple(jax.ShapeDtypeStruct(shape, dtype) for shape, dtype in shapes),
        in_specs=[VMEM] * count,
        out_specs=(VMEM,) * len(shapes),
        **kw,
    )


def fold_kernel(mine, got, out):
    y = position()[2]
    for k in range(4):
        out[(y + k) % 4] = (mine[k].astype(f32) + got[k].astype(f32)).astype(bf16)


def close_kernel(ranks, parts, out):
    width = parts.shape[2]
    col = lax.broadcasted_iota(jnp.int32, (16, 128), 1)
    row = lax.broadcasted_iota(jnp.int32, (16, 128), 0)
    values = jnp.zeros((16, 128), jnp.int32)
    for i in range(ranks.shape[0]):
        values = jnp.where(col == i, ranks[i], values)
    values = jnp.where(row == 0, values // 32, jnp.where(row == 1, values % 32, 0)).astype(f32).astype(bf16)
    total = parts[0].astype(f32)
    for k in range(1, 4):
        total = total + parts[k].astype(f32)
    total = total.astype(bf16)
    for k in range(4):
        out[k, :, pl.ds(0, width)] = total
        out[k, :, pl.ds(width, 128)] = jnp.zeros((out.shape[1], 128), bf16)
        out[k, pl.ds(0, 16), pl.ds(width, 128)] = values


def sum_kernel(parts, out):
    total = parts[0].astype(f32)
    for k in range(1, parts.shape[0]):
        total = total + parts[k].astype(f32)
    out[...] = total.astype(out.dtype)


def swapped(value, axis):
    return lax.all_to_all(value, axis, 0, 0, tiled=True)


def half_add_kernel(part, recv, out, *, lead):
    n = recv.shape[1]
    total = (part[0, :, pl.ds(lead * n, n)].astype(f32) + recv[...].astype(f32)).astype(bf16)
    out[:, pl.ds(lead * n, n)] = total
    out[:, pl.ds((1 - lead) * n, n)] = part[0, :, pl.ds((1 - lead) * n, n)]


def half_add(parts, index, recv, lead):
    block = parts.shape[1:]
    return pl.pallas_call(
        lambda *refs: half_add_kernel(*refs, lead=lead),
        grid=(1,),
        out_shape=jax.ShapeDtypeStruct(block, bf16),
        in_specs=[
            pl.BlockSpec((1, *block), lambda i: (index, 0, 0)),
            pl.BlockSpec(recv.shape, lambda i: (0, 0)),
        ],
        out_specs=pl.BlockSpec(block, lambda i: (0, 0)),
        name="ring_second",
    )(parts, recv)


def ring_of_eight(parts, low, high):
    def both(down, up):
        return lax.optimization_barrier((move(down, "z", -1), move(up, "z", 1)))

    from_up, from_down = both(low, high)
    down = half_add(parts, 5, from_up, 0)
    up = half_add(parts, 3, from_down, 1)
    for step in (2, 1):
        from_up, from_down = both(down, up)
        down = wide_add(parts[8 - step], from_up).astype(bf16)
        up = wide_add(parts[step], from_down).astype(bf16)
    return both(down, up)


def turn_kernel(part, from_up, from_down, rest, down, up):
    n = rest.shape[2] // 2
    own = rest.shape[1] - TILE
    place = position()[:2]

    def summed(rows):
        return part[0, rows, :].astype(f32) + from_up[rows, :].astype(f32) + from_down[rows, :].astype(f32)

    loss = jnp.sum(jnp.sum(summed(pl.ds(4 * own, TILE))[:, :128], axis=1, keepdims=True), axis=0, keepdims=True)
    loss_rows = in_three(jnp.broadcast_to(loss, (1, 128)), place[1])
    blank = jnp.zeros_like(loss_rows)
    last = pl.ds(own, TILE)
    for k in range(4):
        rest[k, last, pl.ds(0, n)] = loss_rows
        rest[k, last, pl.ds(n, n)] = blank
    down[0, last, :] = blank
    down[1, last, :] = loss_rows
    up[0, last, :] = loss_rows
    up[1, last, :] = blank
    first = pl.ds(0, own)
    for a in range(4):
        total = summed(pl.ds(a * own, own)).astype(bf16)
        k = (a + 4 - place[1]) % 4
        rest[k, first, :] = total

        @pl.when(k == 3)
        def _():
            down[0, first, :] = total[:, n:]

        @pl.when(k == 2)
        def _():
            down[1, first, :] = total[:, :n]
            up[1, first, :] = total[:, n:]

        @pl.when(k == 1)
        def _():
            up[0, first, :] = total[:, :n]


def last_kernel(part, from_down, from_up, late_up, late_down, grad, loss):
    n = late_up.shape[1]
    own = grad.shape[0]
    low = part[0, :, pl.ds(0, n)].astype(f32) + from_down[0].astype(f32) + late_up[...].astype(f32)
    grad[:, pl.ds(0, n)] = low[:own]
    rows = pl.ds(0, own)
    grad[:, pl.ds(n, n)] = (
        part[0, rows, pl.ds(n, n)].astype(f32) + from_up[0, rows, :].astype(f32) + late_down[rows, :].astype(f32)
    )
    total = jnp.sum(jnp.sum(low[own:, :128], axis=1, keepdims=True), axis=0, keepdims=True)
    loss[...] = jnp.broadcast_to(total * (1.0 / UNITS), loss.shape)


def shards(
    latents,
    noise,
    behavior_velocity,
    timestep,
    reward_rank_integer,
    surviving_source_index,
    surviving_slot_index,
    group_kept_count,
    patch_input_weight,
    modulation_lookup,
    up_projection_weight,
    down_projection_weight,
    velocity_head_weight,
):
    ranks_dp = lax.axis_size(DP)
    surviving = surviving_source_index.shape[0]
    trajs = surviving // ranks_dp
    steps = timestep.shape[1]
    capacity = latents.shape[0]

    def pairs(a):
        return a.reshape(capacity, steps, 32, 128).transpose(0, 2, 1, 3).reshape(capacity, 64, 128)

    width = patch_input_weight.shape[1]
    rows = 8 * 2 * trajs * 8
    one = jax.ShapeDtypeStruct((TRAJS, 80, 128), bf16)
    two = jax.ShapeDtypeStruct((TRAJS, 2, PAIRS, 128), bf16)
    out_first, out_second, own_first, own_second = pl.pallas_call(
        gather_kernel,
        out_shape=(one, two, one, two),
        in_specs=[SMEM, SMEM, HBM, HBM, HBM],
        out_specs=(VMEM, VMEM, VMEM, VMEM),
        scratch_shapes=[pltpu.SemaphoreType.DMA((6 * TRAJS,))],
        name="gather_slots",
    )(
        surviving_slot_index, timestep.T,
        pairs(latents), pairs(noise), pairs(behavior_velocity),
    )
    onward = [(i, i + 1) for i in range(ranks_dp - 1)]
    near = [
        ((d + hop) * 8 + f, d * 8 + f) for d in range(ranks_dp) for f, hop in enumerate(NEAR) if 0 <= d + hop < ranks_dp
    ]
    near_ranks = lax.ppermute(reward_rank_integer, ("z", "x", "y", "c"), near)
    far_ranks = lax.ppermute(reward_rank_integer, DP, [(d + 4, d) for d in range(ranks_dp - 4)])
    came = lax.ppermute(out_first, DP, onward)
    came_late = lax.ppermute(out_second, DP, onward)
    hidden = up_projection_weight.shape[1]
    half = rows // 2
    tokens, stamps, modulated, activated, bend, proj_other, proj_own = pl.pallas_call(
        forward_kernel,
        out_shape=(
            jax.ShapeDtypeStruct((CHUNKS * BLOCK, 128), bf16),
            jax.ShapeDtypeStruct((BLOCK, 128), f32),
            jax.ShapeDtypeStruct((rows, width), bf16),
            jax.ShapeDtypeStruct((rows, hidden), bf16),
            jax.ShapeDtypeStruct((rows, hidden), bf16),
            jax.ShapeDtypeStruct((half, width), bf16),
            jax.ShapeDtypeStruct((half, width), bf16),
        ),
        in_specs=[SMEM, VMEM, VMEM, HBM, HBM, HBM, HBM],
        out_specs=(VMEM, VMEM, HBM, HBM, HBM, HBM, HBM),
        scratch_shapes=[
            pltpu.VMEM(patch_input_weight.shape, bf16),
            pltpu.VMEM(modulation_lookup.shape, f32),
            pltpu.VMEM((TRAJS * 80, 128), f32),
            pltpu.VMEM((CHUNKS * BLOCK, 128), f32),
            pltpu.VMEM((2, 128, width), bf16),
            pltpu.VMEM((2, CHUNKS * BLOCK, width), f32),
            pltpu.VMEM((BLOCK, width), f32),
            pltpu.VMEM((BLOCK, width), f32),
            pltpu.VMEM((width, hidden), bf16),
            pltpu.VMEM((width, hidden), bf16),
            pltpu.VMEM((rows, width), bf16),
            pltpu.VMEM((rows, hidden), bf16),
            pltpu.VMEM((rows, hidden), bf16),
            pltpu.VMEM((rows, width), bf16),
            pltpu.SemaphoreType.DMA((9,)),
        ],
        compiler_params=pltpu.CompilerParams(vmem_limit_bytes=50 << 20),
        name="forward",
    )(surviving_source_index, came, own_first, patch_input_weight, modulation_lookup, up_projection_weight, down_projection_weight)
    got = swap(proj_other, "c", 1)
    piece = rows // 8
    (folded,) = call(fold_kernel, [((4, piece, width), bf16)], 2, name="fold")(
        proj_own.reshape(4, piece, width), got.reshape(4, piece, width)
    )
    gathered = swapped(folded, "y")
    gathered, came_late, near_ranks, far_ranks = lax.optimization_barrier((gathered, came_late, near_ranks, far_ranks))
    closed = pl.pallas_call(
        close_kernel,
        out_shape=jax.ShapeDtypeStruct((4, piece, width + 128), bf16),
        in_specs=[SMEM, VMEM],
        out_specs=VMEM,
        name="close",
    )(near_ranks, gathered)
    summed_own = swapped(closed, "y")
    summed_other = swap(summed_own, "c", 1)
    own_rows = width // ranks_dp
    m = hidden // 2
    share = 4 * own_rows
    down_parts, down_low, down_high, up_parts = pl.pallas_call(
        backward_kernel,
        out_shape=(
            jax.ShapeDtypeStruct((8, share + TILE, hidden), bf16),
            jax.ShapeDtypeStruct((share + TILE, m), bf16),
            jax.ShapeDtypeStruct((share + TILE, m), bf16),
            jax.ShapeDtypeStruct((4, 8, own_rows, hidden), bf16),
        ),
        in_specs=[SMEM] * 5 + [VMEM] * 6 + [HBM, VMEM, HBM] + [HBM] * 4,
        out_specs=(HBM,) * 4,
        scratch_shapes=[
            pltpu.VMEM(patch_input_weight.shape, bf16),
            pltpu.VMEM(modulation_lookup.shape, f32),
            pltpu.VMEM((CHUNKS * BLOCK, 128), f32),
            pltpu.VMEM((CHUNKS * BLOCK, 128), f32),
            pltpu.VMEM((2, 128, width), bf16),
            pltpu.VMEM((2, width, 128), bf16),
            pltpu.VMEM((2, CHUNKS * BLOCK, width), f32),
            pltpu.VMEM((2, CHUNKS * BLOCK, width), bf16),
            pltpu.VMEM((2, CHUNKS * BLOCK, width), f32),
            pltpu.VMEM((2, CHUNKS * BLOCK, 128), f32),
            pltpu.VMEM((BLOCK, width), f32),
            pltpu.VMEM((CHUNKS * BLOCK, 128), f32),
            pltpu.VMEM((BLOCK, 128), f32),
            pltpu.VMEM((BLOCK, 128), f32),
            pltpu.VMEM((8, 128), jnp.int32),
            pltpu.SMEM((8, 128), jnp.int32),
            pltpu.VMEM((rows, hidden), bf16),
            pltpu.VMEM((rows, hidden), bf16),
            pltpu.VMEM((rows, width), bf16),
            pltpu.VMEM((width, hidden), bf16),
            pltpu.VMEM((rows, width), bf16),
            pltpu.VMEM((8, share + TILE, hidden), bf16),
            pltpu.VMEM((share + TILE, m), bf16),
            pltpu.VMEM((share + TILE, m), bf16),
            pltpu.VMEM((4, 8, own_rows, hidden), bf16),
            pltpu.SemaphoreType.DMA((12,)),
            pltpu.SemaphoreType.DMA((4,)),
        ],
        compiler_params=pltpu.CompilerParams(vmem_limit_bytes=60 << 20),
        name="backward",
    )(
        reward_rank_integer, far_ranks, surviving_source_index, surviving_slot_index, group_kept_count,
        summed_other, summed_own, tokens, stamps, came_late, own_second,
        patch_input_weight, velocity_head_weight, modulation_lookup,
        activated, bend, modulated, down_projection_weight,
    )

    up_gathered = swapped(up_parts, "x")

    from_z_up, from_z_down = ring_of_eight(down_parts, down_low, down_high)
    tall = share + TILE
    short = own_rows + TILE
    rest, turn_down, turn_up = pl.pallas_call(
        turn_kernel,
        grid=(1,),
        out_shape=(
            jax.ShapeDtypeStruct((4, short, hidden), bf16),
            jax.ShapeDtypeStruct((2, short, m), bf16),
            jax.ShapeDtypeStruct((2, short, m), bf16),
        ),
        in_specs=[
            pl.BlockSpec((1, tall, hidden), lambda i: (0, 0, 0)),
            pl.BlockSpec((tall, hidden), lambda i: (0, 0)),
            pl.BlockSpec((tall, hidden), lambda i: (0, 0)),
        ],
        out_specs=(
            pl.BlockSpec((4, short, hidden), lambda i: (0, 0, 0)),
            pl.BlockSpec((2, short, m), lambda i: (0, 0, 0)),
            pl.BlockSpec((2, short, m), lambda i: (0, 0, 0)),
        ),
        name="turn",
    )(down_parts, from_z_up, from_z_down)
    up_x = pl.pallas_call(
        sum_kernel,
        grid=(2,),
        out_shape=jax.ShapeDtypeStruct((8, own_rows, hidden), bf16),
        in_specs=[pl.BlockSpec((4, 4, own_rows, hidden), lambda i: (0, i, 0, 0))],
        out_specs=pl.BlockSpec((4, own_rows, hidden), lambda i: (i, 0, 0)),
        name="sum_along_x",
    )(up_gathered)
    up_last = swapped(up_x, "z")
    far_up = move(turn_down, "x", -1)
    far_down = move(turn_up, "x", 1)
    second_down = wide_add(rest[3, :, :m], far_up[1]).astype(bf16)
    second_up = wide_add(rest[1, :, m:], far_down[1]).astype(bf16)
    last_up = move(second_down, "x", -1)
    last_down = move(second_up, "x", 1)
    down_grad, loss = pl.pallas_call(
        last_kernel,
        grid=(1,),
        out_shape=(
            jax.ShapeDtypeStruct((own_rows, hidden), f32),
            jax.ShapeDtypeStruct((TILE, 128), f32),
        ),
        in_specs=[
            pl.BlockSpec((1, short, hidden), lambda i: (0, 0, 0)),
            pl.BlockSpec((1, short, m), lambda i: (0, 0, 0)),
            pl.BlockSpec((1, short, m), lambda i: (0, 0, 0)),
            pl.BlockSpec((short, m), lambda i: (0, 0)),
            pl.BlockSpec((short, m), lambda i: (0, 0)),
        ],
        out_specs=(
            pl.BlockSpec((own_rows, hidden), lambda i: (0, 0)),
            pl.BlockSpec((TILE, 128), lambda i: (0, 0)),
        ),
        name="last",
    )(rest, far_down, far_up, last_up, last_down)
    (up_grad,) = call(sum_kernel, [((own_rows, hidden), f32)], 1, name="sum_along_z")(up_last)
    return (up_grad, down_grad, loss[0, 0])


def solution(mesh):
    finer = Mesh(mesh.devices.reshape(8, 4, 4, 2), ("z", "x", "y", "c"))
    dp, fsdp = ("z", "x"), ("y", "c")
    in_specs = (
        P(dp, None, None),
        P(dp, None, None),
        P(dp, None, None),
        P(dp, None),
        P(dp),
        P(),
        P(),
        P(),
        P(),
        P(),
        P(None, fsdp),
        P(None, fsdp),
        P(),
    )
    out_specs = (P(dp, fsdp), P(dp, fsdp), P())
    return jax.shard_map(
        shards, mesh=finer, in_specs=in_specs, out_specs=out_specs, check_vma=False
    )
```

```python
import jax
import jax.numpy as jnp
from jax import lax
from jax.experimental import pallas as pl
from jax.experimental.pallas import tpu as pltpu
from jax.sharding import Mesh
from jax.sharding import PartitionSpec as P

KSTEPS = 10
DP = ("z", "x")
clip_range = 0.2
noise_level = 0.7
norm_eps = 1e-06
bf16 = jnp.bfloat16
f32 = jnp.float32


def move(value, axis, steps):
    count = lax.axis_size(axis)
    return lax.ppermute(value, axis, [(i, (i + steps) % count) for i in range(count)])


def swap(value, axis, bit):
    count = lax.axis_size(axis)
    return lax.ppermute(value, axis, [(i, i ^ bit) for i in range(count)])


TRAJS = 6
PAIRS = 64
TILE = 8
BLOCK = TRAJS * TILE
CHUNKS = 8


def position():
    z, x, y, c = (lax.axis_index(a) for a in ("z", "x", "y", "c"))
    return z, x, y, c, z * 4 + x


def chunk_owner(q):
    _, _, y, c, _ = position()
    return (y + q % 4) % 4 * 2 + (1 - c if q < 4 else c)


def gather_kernel(slot_table, stamps, latents, noise, behavior, out_first, out_second, own_first, own_second, sems):
    copies = []
    owner = position()[4]
    following = jnp.minimum(owner + 1, 31)
    slots = [slot_table[following * TRAJS + j] for j in range(TRAJS)]
    slots += [slot_table[owner * TRAJS + j] for j in range(TRAJS)]
    for j in range(2 * TRAJS):
        slot = slots[j]
        first, second = (out_first, out_second) if j < TRAJS else (own_first, own_second)
        k = j % TRAJS
        for i, (source, target) in enumerate(
            ((latents, first.at[k, pl.ds(0, PAIRS)]), (noise, second.at[k, 0]), (behavior, second.at[k, 1]))
        ):
            copy = pltpu.make_async_copy(source.at[slot], target, sems.at[3 * j + i])
            copy.start()
            copies.append(copy)
    step = lax.broadcasted_iota(jnp.int32, (16, 128), 0) % 2
    for j in range(2 * TRAJS):
        slot = slots[j]
        tile = jnp.where(step == 0, stamps[0, slot], stamps[1, slot])
        first = out_first if j < TRAJS else own_first
        first[j % TRAJS, pl.ds(PAIRS, 16), :] = tile.astype(f32).astype(bf16)
    for copy in copies:
        copy.wait()


def modulation_rows(stamp_tile, lookup, index):
    rows = jnp.zeros((TILE, lookup.shape[2]), f32)
    for k in range(KSTEPS):
        rows = jnp.where(stamp_tile == k, lookup[k, pl.ds(index, 1), :], rows)
    return rows


def widened(weight, wide, dim):
    size = weight.shape[dim]
    wide[...] = jnp.zeros(wide.shape, wide.dtype)
    if dim == 0:
        wide[0, pl.ds(0, size), :] = weight[...]
        wide[1, pl.ds(size, size), :] = weight[...]
    else:
        wide[0, :, pl.ds(0, size)] = weight[...]
        wide[1, :, pl.ds(size, size)] = weight[...]


def gelu_both(v):
    k = 0.7978845608028654
    square = v * v
    t = jnp.tanh(k * (v + 0.044715 * (square * v)))
    half = 0.5 * (1.0 + t)
    return v * half, half + (0.5 * k) * v * (1.0 - t * t) * (1.0 + (3 * 0.044715) * square)


def forward_kernel(
    source, came, mine, weight_in, lookup_in, up_weight, down_weight,
    tokens, stamps, mod_out, act_out, bend_out, proj_other, proj_own,
    weight, lookup, merged, sorted_, wide, emb, scale, shift, up_w, down_w, modulated, activated, bend, proj, sems,
):
    width = weight.shape[1]
    owner = position()[4]
    load_weight = pltpu.make_async_copy(weight_in, weight, sems.at[7])
    load_lookup = pltpu.make_async_copy(lookup_in, lookup, sems.at[8])
    load_weight.start()
    load_lookup.start()
    load_up = pltpu.make_async_copy(up_weight, up_w, sems.at[0])
    load_down = pltpu.make_async_copy(down_weight, down_w, sems.at[1])
    load_up.start()
    load_down.start()
    for j in range(TRAJS):
        away = source[owner * TRAJS + j] != owner
        merged[pl.ds(j * 80, 80), :] = jnp.where(away, came[j].astype(f32), mine[j].astype(f32))
    for q in range(CHUNKS):
        at_owner = chunk_owner(q)
        for j in range(TRAJS):
            at = pl.multiple_of(j * 80 + at_owner * TILE, TILE)
            sorted_[pl.ds(q * BLOCK + j * TILE, TILE), :] = merged[pl.ds(at, TILE), :]
    tokens[...] = sorted_[...].astype(bf16)
    load_weight.wait()
    load_lookup.wait()
    widened(weight, wide, 0)
    for j in range(TRAJS):
        stamp = merged[pl.ds(j * 80 + PAIRS, TILE), :]
        stamps[pl.ds(j * TILE, TILE), :] = stamp
        stamp = stamp[:, :1]
        shift[pl.ds(j * TILE, TILE), :] = modulation_rows(stamp, lookup, 0)
        scale[pl.ds(j * TILE, TILE), :] = 1.0 + modulation_rows(stamp, lookup, 1)
    for par in range(2):
        emb[par] = jnp.dot(tokens[...], wide[par], preferred_element_type=f32)

    def norm(q, carry):
        for par in range(2):
            values = emb[par, pl.ds(pl.multiple_of(q * BLOCK, BLOCK), BLOCK), :]
            center = values - jnp.sum(values, axis=1, keepdims=True) * (1.0 / width)
            variance = jnp.sum(center * center, axis=1, keepdims=True) * (1.0 / width)
            normed = center * lax.rsqrt(variance + norm_eps)
            at = pl.multiple_of(q * (2 * BLOCK) + par * BLOCK, BLOCK)
            modulated[pl.ds(at, BLOCK), :] = (normed * scale[...] + shift[...]).astype(bf16)
        return carry

    lax.fori_loop(0, CHUNKS, norm, 0)
    save_mod = pltpu.make_async_copy(modulated, mod_out, sems.at[2])
    save_mod.start()
    load_up.wait()
    load_down.wait()

    def hidden(r, carry):
        rows = pl.ds(pl.multiple_of(r * 192, 192), 192)
        pre = jnp.dot(modulated[rows, :], up_w[...], preferred_element_type=f32)
        value, slope = gelu_both(pre)
        value = value.astype(bf16)
        activated[rows, :] = value
        bend[rows, :] = slope.astype(bf16)
        proj[rows, :] = lax.dot_general(
            value, down_w[...], (((1,), (1,)), ((), ())), preferred_element_type=f32
        ).astype(bf16)
        return carry

    half = modulated.shape[0] // 2
    lax.fori_loop(0, 2, hidden, 0)
    save_other = pltpu.make_async_copy(proj.at[pl.ds(0, half)], proj_other, sems.at[3])
    save_other.start()
    lax.fori_loop(2, 4, hidden, 0)
    save_own = pltpu.make_async_copy(proj.at[pl.ds(half, half)], proj_own, sems.at[4])
    save_own.start()
    save_act = pltpu.make_async_copy(activated, act_out, sems.at[5])
    save_act.start()
    save_bend = pltpu.make_async_copy(bend, bend_out, sems.at[6])
    save_bend.start()
    for copy in (save_mod, save_other, save_own, save_act, save_bend):
        copy.wait()


def backward_kernel(
    ranks, far_ranks, source, slot, kept,
    other, own, tokens, stamps, came, mine, weight_in, head, lookup_in,
    act_in, bend_in, mod_in, down_in,
    down_parts, down_low, down_high, up_parts,
    weight, lookup, drawn, target, wide, wide_head, emb, rounded, back, inverse, gate, error, slope, coeff,
    table_v, table, act, bend, mod, down_w, upstream, parts, low, high, pieces,
    sems, out_sems,
):
    z, x, y, c, owner = position()
    place = (z, x)
    load_weight = pltpu.make_async_copy(weight_in, weight, sems.at[10])
    load_lookup = pltpu.make_async_copy(lookup_in, lookup, sems.at[11])
    load_weight.start()
    load_lookup.start()
    loads = [
        pltpu.make_async_copy(a, b, sems.at[i])
        for i, (a, b) in enumerate(((act_in, act), (down_in, down_w), (bend_in, bend), (mod_in, mod)))
    ]
    for copy in loads:
        copy.start()
    for q in range(CHUNKS):
        info = (other if q < 4 else own)[(q + y) % 4, pl.ds(0, 16), pl.ds(weight.shape[1], 128)].astype(f32)
        table_v[pl.ds(chunk_owner(q), 1), :] = (info[0:1] * 32.0 + info[1:2]).astype(jnp.int32)
    fetch = pltpu.make_async_copy(table_v, table, sems.at[4])
    fetch.start()
    width = weight.shape[1]
    values = SEQ_VALUES
    load_weight.wait()
    load_lookup.wait()
    widened(weight, wide, 0)
    widened(head, wide_head, 1)
    for j in range(TRAJS):
        stamp = stamps[pl.ds(j * TILE, TILE), :]
        gate[pl.ds(j * TILE, TILE), :] = modulation_rows(stamp[:, :1], lookup, 2)
        level = 1.0 - stamp * (1.0 / KSTEPS)
        coeff[pl.ds(j * TILE, TILE), :] = (
            jnp.sqrt((1.0 / KSTEPS) * (1.0 - level + 1.0 / KSTEPS) / level) / noise_level
        )
        away = source[owner * TRAJS + j] != owner
        picked = jnp.where(away, came[j].astype(f32), mine[j].astype(f32))
        emb[0, pl.ds(0, PAIRS), pl.ds(0, 128)] = picked[0]
        emb[0, pl.ds(PAIRS, PAIRS), pl.ds(0, 128)] = picked[1]
        for q in range(CHUNKS):
            at = pl.multiple_of(chunk_owner(q) * TILE, TILE)
            drawn[pl.ds(q * BLOCK + j * TILE, TILE), :] = emb[0, pl.ds(at, TILE), pl.ds(0, 128)]
            at = pl.multiple_of(PAIRS + chunk_owner(q) * TILE, TILE)
            target[pl.ds(q * BLOCK + j * TILE, TILE), :] = emb[0, pl.ds(at, TILE), pl.ds(0, 128)]
    for par in range(2):
        emb[par] = jnp.dot(tokens[...], wide[par], preferred_element_type=f32)

    def forward(q, summed):
        for par in range(2):
            rows = pl.ds(pl.multiple_of(q * BLOCK, BLOCK), BLOCK)
            mixed = emb[par, rows, :] + gate[...] * summed[
                (q + y) % 4, pl.ds(par * BLOCK, BLOCK), pl.ds(0, width)
            ].astype(f32)
            center = mixed - jnp.sum(mixed, axis=1, keepdims=True) * (1.0 / width)
            variance = jnp.sum(center * center, axis=1, keepdims=True) * (1.0 / width)
            scale = lax.rsqrt(variance + norm_eps)
            final = center * scale
            emb[par, rows, :] = final
            rounded[par, rows, :] = final.astype(bf16)
            inverse[par, rows, :] = jnp.broadcast_to(scale, (BLOCK, 128))

    def first_half(q, carry):
        forward(q, other)
        return carry

    def second_half(q, carry):
        forward(q + 4, own)
        return carry

    lax.fori_loop(0, 4, first_half, 0)
    lax.fori_loop(0, 4, second_half, 0)
    velocity = jnp.dot(rounded[0], wide_head[0], preferred_element_type=f32)
    error[...] = velocity + jnp.dot(rounded[1], wide_head[1], preferred_element_type=f32) - target[...]
    total = jnp.zeros((BLOCK, 128), f32)
    c = coeff[...]
    for q in range(CHUNKS):
        rows = pl.ds(q * BLOCK, BLOCK)
        err = error[rows, :]
        total = total + c * drawn[rows, :] * err + 0.5 * c * c * err * err
    sums = jnp.broadcast_to(jnp.sum(total, axis=1, keepdims=True), (BLOCK, 128))
    losses = jnp.zeros((TILE, 128), f32)
    fetch.wait()
    gains = advantages(table, ranks, far_ranks, source, slot, kept, owner)
    for j in range(TRAJS):
        unit = sums[j * TILE : (j + 1) * TILE]
        unit = unit + pltpu.roll(unit, 4, 0)
        unit = unit + pltpu.roll(unit, 2, 0)
        ratio = jnp.exp(-unit / values)
        clipped = jnp.clip(ratio, 1.0 - clip_range, 1.0 + clip_range)
        plain = ratio * gains[j]
        bounded = clipped * gains[j]
        losses = losses - jnp.minimum(plain, bounded)
        live = jnp.where(plain <= bounded, 1.0, 0.0)
        slope[pl.ds(j * TILE, TILE), :] = -gains[j] * ratio * live * (1.0 / UNITS)
    total = losses[0:1] + losses[1:2]
    loss_rows = in_three(total, place[0])
    bent = slope[...]
    for q in range(CHUNKS):
        rows = pl.ds(q * BLOCK, BLOCK)
        error[rows, :] = bent * (-(c * drawn[rows, :] + c * c * error[rows, :]) / values)
    dvelocity = error[...].astype(bf16)
    for par in range(2):
        back[par] = lax.dot_general(
            dvelocity, wide_head[par], (((1,), (1,)), ((), ())), preferred_element_type=f32
        )

    def backward(q, carry):
        for par in range(2):
            rows = pl.ds(pl.multiple_of(q * BLOCK, BLOCK), BLOCK)
            d = back[par, rows, :]
            final = emb[par, rows, :]
            mean = jnp.sum(d, axis=1, keepdims=True) * (1.0 / width)
            along = jnp.sum(d * final, axis=1, keepdims=True) * (1.0 / width)
            dmixed = inverse[par, rows, :][:, :1] * (d - mean - final * along)
            at = pl.multiple_of(q * (2 * BLOCK) + par * BLOCK, BLOCK)
            upstream[pl.ds(at, BLOCK), :] = (gate[...] * dmixed).astype(bf16)
        return carry

    lax.fori_loop(0, CHUNKS, backward, 0)
    loads[0].wait()
    tokens_all, hidden = act.shape
    n = hidden // 2
    share = width // 8
    contract = (((0,), (0,)), ((), ()))
    low[pl.ds(share, TILE), :] = loss_rows
    high[pl.ds(share, TILE), :] = jnp.zeros_like(loss_rows)
    for k in range(8):
        parts[k, pl.ds(share, TILE), pl.ds(0, n)] = loss_rows
        parts[k, pl.ds(share, TILE), pl.ds(n, n)] = jnp.zeros_like(loss_rows)

    def down_block(i, carry):
        cols = pl.ds(pl.multiple_of(i * 2 * share, 128), 2 * share)
        total = lax.dot_general(upstream[:, cols], act[...], contract, preferred_element_type=f32).astype(bf16)
        for j in range(2):
            k = (2 * i + j + 8 - place[0]) % 8
            piece = total[j * share : (j + 1) * share]
            parts[k, pl.ds(0, share), :] = piece

            @pl.when(k == 4)
            def _():
                low[pl.ds(0, share), :] = piece[:, :n]
                high[pl.ds(0, share), :] = piece[:, n:]

        return carry

    lax.fori_loop(0, 4, down_block, 0)
    saves = [
        pltpu.make_async_copy(a, b, sems.at[5 + i])
        for i, (a, b) in enumerate(((low, down_low), (high, down_high), (parts, down_parts)))
    ]
    for copy in saves:
        copy.start()
    for copy in loads[1:]:
        copy.wait()

    def bent_rows(r, carry):
        rows = pl.ds(pl.multiple_of(r * 192, 192), 192)
        d = jnp.dot(upstream[rows, :], down_w[...], preferred_element_type=f32)
        bend[rows, :] = (d * bend[rows, :].astype(f32)).astype(bf16)
        return carry

    lax.fori_loop(0, tokens_all // 192, bent_rows, 0)
    quarter = share // 4

    def save_pieces(i):
        rows = pl.ds(2 * i, 2)
        return pltpu.make_async_copy(pieces.at[:, rows], up_parts.at[:, rows], out_sems.at[i])

    def up_block(i, carry):
        cols = pl.ds(pl.multiple_of(i * 2 * share, 128), 2 * share)
        total = lax.dot_general(mod[:, cols], bend[...], contract, preferred_element_type=f32).astype(bf16)
        for j in range(8):
            pieces[j % 4, 2 * i + j // 4] = total[j * quarter : (j + 1) * quarter]
        save_pieces(i).start()
        return carry

    lax.fori_loop(0, 4, up_block, 0)
    for i in range(4):
        save_pieces(i).wait()
    for copy in saves:
        copy.wait()


def in_three(value, lane):
    rows = jnp.broadcast_to(value, (TILE, 128))
    first = rows.astype(bf16).astype(f32)
    second = (rows - first).astype(bf16).astype(f32)
    third = (rows - first - second).astype(bf16).astype(f32)
    row = lax.broadcasted_iota(jnp.int32, (TILE, 128), 0)
    col = lax.broadcasted_iota(jnp.int32, (TILE, 128), 1)
    chosen = jnp.where(row == 0, first, jnp.where(row == 1, second, jnp.where(row == 2, third, 0.0)))
    tile = jnp.where(col == lane, chosen, 0.0)
    return jnp.concatenate([tile, jnp.zeros((TILE, 384), f32)], axis=1).astype(bf16)


def advantages(table, ranks, far_ranks, source, slot, kept, owner):
    def rank_of(p):
        d = source[p] - owner
        s = slot[p]
        f = jnp.clip(jnp.where(d < 0, d + 5, d + 4), 0, 7)
        return jnp.where(d == 0, ranks[s], jnp.where(d == 4, far_ranks[s], table[f, s]))

    def seek(g, state):
        end = state[0]
        after = end + kept[g]
        out = [after]
        for j in range(TRAJS):
            p = owner * TRAJS + j
            here = (p >= end) & (p < after)
            out.append(jnp.where(here, end, state[1 + 2 * j]))
            out.append(jnp.where(here, kept[g], state[2 + 2 * j]))
        return tuple(out)

    state = lax.fori_loop(0, kept.shape[0], seek, (jnp.int32(0),) + (jnp.int32(0), jnp.int32(1)) * TRAJS)
    gains = []
    for j in range(TRAJS):
        begin, count = state[1 + 2 * j], state[2 + 2 * j]

        def add(q, sums):
            rank = rank_of(q)
            return sums[0] + rank, sums[1] + rank * rank

        first, second = lax.fori_loop(begin, begin + count, add, (jnp.int32(0), jnp.int32(0)))

        def row(value):
            return jnp.full((1, 128), value, jnp.int32).astype(f32)

        counts = row(count)
        deviation = jnp.sqrt(row(count * second - first * first)) / counts
        gains.append((row(rank_of(owner * TRAJS + j)) - row(first) / counts) / jnp.maximum(deviation, 1.0))
    return gains


NEAR = (-5, -4, -3, -2, -1, 1, 2, 3)
SEQ_VALUES = 4096
UNITS = 384
SMEM = pl.BlockSpec(memory_space=pltpu.SMEM)
VMEM = pl.BlockSpec(memory_space=pltpu.VMEM)
HBM = pl.BlockSpec(memory_space=pltpu.HBM)


def wide_add(*parts):
    total = parts[0].astype(f32)
    for part in parts[1:]:
        total = total + part.astype(f32)
    return total


def call(kernel, shapes, count, **kw):
    return pl.pallas_call(
        kernel,
        out_shape=tuple(jax.ShapeDtypeStruct(shape, dtype) for shape, dtype in shapes),
        in_specs=[VMEM] * count,
        out_specs=(VMEM,) * len(shapes),
        compiler_params=pltpu.CompilerParams(vmem_limit_bytes=6 << 20),
        **kw,
    )


def fold_kernel(mine, got, out):
    y = position()[2]
    for k in range(4):
        out[(y + k) % 4] = (mine[k].astype(f32) + got[k].astype(f32)).astype(bf16)


def close_kernel(ranks, parts, out):
    width = parts.shape[2]
    col = lax.broadcasted_iota(jnp.int32, (16, 128), 1)
    row = lax.broadcasted_iota(jnp.int32, (16, 128), 0)
    values = jnp.zeros((16, 128), jnp.int32)
    for i in range(ranks.shape[0]):
        values = jnp.where(col == i, ranks[i], values)
    values = jnp.where(row == 0, values // 32, jnp.where(row == 1, values % 32, 0)).astype(f32).astype(bf16)
    total = parts[0].astype(f32)
    for k in range(1, 4):
        total = total + parts[k].astype(f32)
    total = total.astype(bf16)
    for k in range(4):
        out[k, :, pl.ds(0, width)] = total
        out[k, :, pl.ds(width, 128)] = jnp.zeros((out.shape[1], 128), bf16)
        out[k, pl.ds(0, 16), pl.ds(width, 128)] = values


def sum_kernel(parts, out):
    total = parts[0].astype(f32)
    for k in range(1, parts.shape[0]):
        total = total + parts[k].astype(f32)
    out[...] = total.astype(out.dtype)


def swapped(value, axis):
    return lax.all_to_all(value, axis, 0, 0, tiled=True)


def half_add_kernel(part, recv, out, *, lead):
    n = recv.shape[1]
    total = (part[0, :, pl.ds(lead * n, n)].astype(f32) + recv[...].astype(f32)).astype(bf16)
    out[:, pl.ds(lead * n, n)] = total
    out[:, pl.ds((1 - lead) * n, n)] = part[0, :, pl.ds((1 - lead) * n, n)]


def half_add(parts, index, recv, lead):
    block = parts.shape[1:]
    return pl.pallas_call(
        lambda *refs: half_add_kernel(*refs, lead=lead),
        grid=(1,),
        out_shape=jax.ShapeDtypeStruct(block, bf16),
        in_specs=[
            pl.BlockSpec((1, *block), lambda i: (index, 0, 0)),
            pl.BlockSpec(recv.shape, lambda i: (0, 0)),
        ],
        out_specs=pl.BlockSpec(block, lambda i: (0, 0)),
        compiler_params=pltpu.CompilerParams(vmem_limit_bytes=6 << 20),
        name="ring_second",
    )(parts, recv)


def ring_of_eight(parts, low, high, third, fourth):
    def both(down, up, beside=lambda: ()):
        down, up = move(down, "z", -1), move(up, "z", 1)
        return lax.optimization_barrier((down, up, beside()))

    from_up, from_down, _ = both(low, high)
    down = half_add(parts, 5, from_up, 0)
    up = half_add(parts, 3, from_down, 1)
    from_up, from_down, _ = both(down, up)
    down = wide_add(parts[6], from_up).astype(bf16)
    up = wide_add(parts[2], from_down).astype(bf16)
    from_up, from_down, ready = both(down, up, third)
    down = wide_add(parts[7], from_up).astype(bf16)
    up = wide_add(parts[1], from_down).astype(bf16)
    return both(down, up, lambda: fourth(ready))


def turn_kernel(part, from_up, from_down, out):
    n = out.shape[2] // 2
    own = out.shape[1] - TILE

    def summed(rows):
        return part[0, rows, :].astype(f32) + from_up[rows, :].astype(f32) + from_down[rows, :].astype(f32)

    loss = jnp.sum(jnp.sum(summed(pl.ds(4 * own, TILE))[:, :128], axis=1, keepdims=True), axis=0, keepdims=True)
    loss_rows = in_three(jnp.broadcast_to(loss, (1, 128)), position()[1])
    for k in range(4):
        out[k, pl.ds(0, own), :] = summed(pl.ds(k * own, own)).astype(bf16)
        out[k, pl.ds(own, TILE), pl.ds(0, n)] = loss_rows
        out[k, pl.ds(own, TILE), pl.ds(n, n)] = jnp.zeros_like(loss_rows)


def last_kernel(parts, grad, loss):
    own = grad.shape[0]
    total = parts[0].astype(f32)
    for k in range(1, 4):
        total = total + parts[k].astype(f32)
    grad[...] = total[:own]
    found = jnp.sum(jnp.sum(total[own:, :128], axis=1, keepdims=True), axis=0, keepdims=True)
    loss[...] = jnp.broadcast_to(found * (1.0 / UNITS), loss.shape)


def spread_kernel(parts, down, up, further, keep):
    z = position()[0]
    for k in range(8):
        block = (z + k) % 8
        total = parts[0, block].astype(f32)
        for j in range(1, 4):
            total = total + parts[j, block].astype(f32)
        total = total.astype(bf16)
        if k in (7, 5):
            down[(7, 5).index(k)] = total
        elif k in (1, 3):
            up[(1, 3).index(k)] = total
        elif k == 4:
            further[...] = total
        else:
            keep[{0: 0, 2: 1, 6: 2}[k]] = total


def meet_kernel(keep, from_up, from_down, from_further, down, up, own):
    up[...] = (keep[1].astype(f32) + from_down[1].astype(f32)).astype(bf16)
    down[...] = (keep[2].astype(f32) + from_up[1].astype(f32) + from_further[...].astype(f32)).astype(bf16)
    own[...] = keep[0].astype(f32) + from_up[0].astype(f32) + from_down[0].astype(f32)


def finish_kernel(own, late_up, late_down, out):
    out[...] = own[...] + late_up[...].astype(f32) + late_down[...].astype(f32)


def shards(
    latents,
    noise,
    behavior_velocity,
    timestep,
    reward_rank_integer,
    surviving_source_index,
    surviving_slot_index,
    group_kept_count,
    patch_input_weight,
    modulation_lookup,
    up_projection_weight,
    down_projection_weight,
    velocity_head_weight,
):
    ranks_dp = lax.axis_size(DP)
    surviving = surviving_source_index.shape[0]
    trajs = surviving // ranks_dp
    steps = timestep.shape[1]
    capacity = latents.shape[0]

    def pairs(a):
        return a.reshape(capacity, steps, 32, 128).transpose(0, 2, 1, 3).reshape(capacity, 64, 128)

    width = patch_input_weight.shape[1]
    rows = 8 * 2 * trajs * 8
    one = jax.ShapeDtypeStruct((TRAJS, 80, 128), bf16)
    two = jax.ShapeDtypeStruct((TRAJS, 2, PAIRS, 128), bf16)
    out_first, out_second, own_first, own_second = pl.pallas_call(
        gather_kernel,
        out_shape=(one, two, one, two),
        in_specs=[SMEM, SMEM, HBM, HBM, HBM],
        out_specs=(VMEM, VMEM, VMEM, VMEM),
        scratch_shapes=[pltpu.SemaphoreType.DMA((6 * TRAJS,))],
        name="gather_slots",
    )(
        surviving_slot_index, timestep.T,
        pairs(latents), pairs(noise), pairs(behavior_velocity),
    )
    onward = [(i, i + 1) for i in range(ranks_dp - 1)]
    near = [
        ((d + hop) * 8 + f, d * 8 + f) for d in range(ranks_dp) for f, hop in enumerate(NEAR) if 0 <= d + hop < ranks_dp
    ]
    near_ranks = lax.ppermute(reward_rank_integer, ("z", "x", "y", "c"), near)
    far_ranks = lax.ppermute(reward_rank_integer, DP, [(d + 4, d) for d in range(ranks_dp - 4)])
    came = lax.ppermute(out_first, DP, onward)
    came_late = lax.ppermute(out_second, DP, onward)
    hidden = up_projection_weight.shape[1]
    half = rows // 2
    tokens, stamps, modulated, activated, bend, proj_other, proj_own = pl.pallas_call(
        forward_kernel,
        out_shape=(
            jax.ShapeDtypeStruct((CHUNKS * BLOCK, 128), bf16),
            jax.ShapeDtypeStruct((BLOCK, 128), f32),
            jax.ShapeDtypeStruct((rows, width), bf16),
            jax.ShapeDtypeStruct((rows, hidden), bf16),
            jax.ShapeDtypeStruct((rows, hidden), bf16),
            jax.ShapeDtypeStruct((half, width), bf16),
            jax.ShapeDtypeStruct((half, width), bf16),
        ),
        in_specs=[SMEM, VMEM, VMEM, HBM, HBM, HBM, HBM],
        out_specs=(VMEM, VMEM, HBM, HBM, HBM, HBM, HBM),
        scratch_shapes=[
            pltpu.VMEM(patch_input_weight.shape, bf16),
            pltpu.VMEM(modulation_lookup.shape, f32),
            pltpu.VMEM((TRAJS * 80, 128), f32),
            pltpu.VMEM((CHUNKS * BLOCK, 128), f32),
            pltpu.VMEM((2, 128, width), bf16),
            pltpu.VMEM((2, CHUNKS * BLOCK, width), f32),
            pltpu.VMEM((BLOCK, width), f32),
            pltpu.VMEM((BLOCK, width), f32),
            pltpu.VMEM((width, hidden), bf16),
            pltpu.VMEM((width, hidden), bf16),
            pltpu.VMEM((rows, width), bf16),
            pltpu.VMEM((rows, hidden), bf16),
            pltpu.VMEM((rows, hidden), bf16),
            pltpu.VMEM((rows, width), bf16),
            pltpu.SemaphoreType.DMA((9,)),
        ],
        compiler_params=pltpu.CompilerParams(vmem_limit_bytes=32 << 20),
        name="forward",
    )(surviving_source_index, came, own_first, patch_input_weight, modulation_lookup, up_projection_weight, down_projection_weight)
    got = swap(proj_other, "c", 1)
    piece = rows // 8
    (folded,) = call(fold_kernel, [((4, piece, width), bf16)], 2, name="fold")(
        proj_own.reshape(4, piece, width), got.reshape(4, piece, width)
    )
    gathered = swapped(folded, "y")
    gathered, came_late, near_ranks, far_ranks = lax.optimization_barrier((gathered, came_late, near_ranks, far_ranks))
    closed = pl.pallas_call(
        close_kernel,
        out_shape=jax.ShapeDtypeStruct((4, piece, width + 128), bf16),
        in_specs=[SMEM, VMEM],
        out_specs=VMEM,
        compiler_params=pltpu.CompilerParams(vmem_limit_bytes=6 << 20),
        name="close",
    )(near_ranks, gathered)
    summed_own = swapped(closed, "y")
    summed_other = swap(summed_own, "c", 1)
    own_rows = width // ranks_dp
    m = hidden // 2
    share = 4 * own_rows
    down_parts, down_low, down_high, up_parts = pl.pallas_call(
        backward_kernel,
        out_shape=(
            jax.ShapeDtypeStruct((8, share + TILE, hidden), bf16),
            jax.ShapeDtypeStruct((share + TILE, m), bf16),
            jax.ShapeDtypeStruct((share + TILE, m), bf16),
            jax.ShapeDtypeStruct((4, 8, own_rows, hidden), bf16),
        ),
        in_specs=[SMEM] * 5 + [VMEM] * 6 + [HBM, VMEM, HBM] + [HBM] * 4,
        out_specs=(HBM,) * 4,
        scratch_shapes=[
            pltpu.VMEM(patch_input_weight.shape, bf16),
            pltpu.VMEM(modulation_lookup.shape, f32),
            pltpu.VMEM((CHUNKS * BLOCK, 128), f32),
            pltpu.VMEM((CHUNKS * BLOCK, 128), f32),
            pltpu.VMEM((2, 128, width), bf16),
            pltpu.VMEM((2, width, 128), bf16),
            pltpu.VMEM((2, CHUNKS * BLOCK, width), f32),
            pltpu.VMEM((2, CHUNKS * BLOCK, width), bf16),
            pltpu.VMEM((2, CHUNKS * BLOCK, width), f32),
            pltpu.VMEM((2, CHUNKS * BLOCK, 128), f32),
            pltpu.VMEM((BLOCK, width), f32),
            pltpu.VMEM((CHUNKS * BLOCK, 128), f32),
            pltpu.VMEM((BLOCK, 128), f32),
            pltpu.VMEM((BLOCK, 128), f32),
            pltpu.VMEM((8, 128), jnp.int32),
            pltpu.SMEM((8, 128), jnp.int32),
            pltpu.VMEM((rows, hidden), bf16),
            pltpu.VMEM((rows, hidden), bf16),
            pltpu.VMEM((rows, width), bf16),
            pltpu.VMEM((width, hidden), bf16),
            pltpu.VMEM((rows, width), bf16),
            pltpu.VMEM((8, share + TILE, hidden), bf16),
            pltpu.VMEM((share + TILE, m), bf16),
            pltpu.VMEM((share + TILE, m), bf16),
            pltpu.VMEM((4, 8, own_rows, hidden), bf16),
            pltpu.SemaphoreType.DMA((12,)),
            pltpu.SemaphoreType.DMA((4,)),
        ],
        compiler_params=pltpu.CompilerParams(vmem_limit_bytes=46 << 20),
        name="backward",
    )(
        reward_rank_integer, far_ranks, surviving_source_index, surviving_slot_index, group_kept_count,
        summed_other, summed_own, tokens, stamps, came_late, own_second,
        patch_input_weight, velocity_head_weight, modulation_lookup,
        activated, bend, modulated, down_projection_weight,
    )

    up_gathered = swapped(up_parts, "x")

    chunk = (own_rows, hidden)

    def spread(gathered):
        down, up, further, keep = call(
            spread_kernel,
            [((2, *chunk), bf16), ((2, *chunk), bf16), (chunk, bf16), ((3, *chunk), bf16)],
            1,
            name="spread",
        )(gathered)
        return keep, move(down, "z", -1), move(up, "z", 1), move(further, "z", -2)

    from_z_up, from_z_down, (keep, from_up, from_down, from_further) = ring_of_eight(
        down_parts, down_low, down_high, lambda: up_gathered, spread
    )
    tall = share + TILE
    short = own_rows + TILE
    turned = pl.pallas_call(
        turn_kernel,
        grid=(1,),
        out_shape=jax.ShapeDtypeStruct((4, short, hidden), bf16),
        in_specs=[
            pl.BlockSpec((1, tall, hidden), lambda i: (0, 0, 0)),
            pl.BlockSpec((tall, hidden), lambda i: (0, 0)),
            pl.BlockSpec((tall, hidden), lambda i: (0, 0)),
        ],
        out_specs=pl.BlockSpec((4, short, hidden), lambda i: (0, 0, 0)),
        compiler_params=pltpu.CompilerParams(vmem_limit_bytes=8 << 20),
        name="turn",
    )(down_parts, from_z_up, from_z_down)
    down_grad, loss = call(
        last_kernel, [((own_rows, hidden), f32), ((TILE, 128), f32)], 1, name="last"
    )(swapped(turned, "x"))
    down, up, kept = call(meet_kernel, [(chunk, bf16), (chunk, bf16), (chunk, f32)], 4, name="meet")(
        keep, from_up, from_down, from_further
    )
    (up_grad,) = call(finish_kernel, [(chunk, f32)], 3, name="finish")(
        kept, *lax.optimization_barrier((move(down, "z", -2), move(up, "z", 2)))
    )
    return (up_grad, down_grad, loss[0, 0])


def solution(mesh):
    finer = Mesh(mesh.devices.reshape(8, 4, 4, 2), ("z", "x", "y", "c"))
    dp, fsdp = ("z", "x"), ("y", "c")
    in_specs = (
        P(dp, None, None),
        P(dp, None, None),
        P(dp, None, None),
        P(dp, None),
        P(dp),
        P(),
        P(),
        P(),
        P(),
        P(),
        P(None, fsdp),
        P(None, fsdp),
        P(),
    )
    out_specs = (P(dp, fsdp), P(dp, fsdp), P())
    return jax.shard_map(
        shards, mesh=finer, in_specs=in_specs, out_specs=out_specs, check_vma=False
    )
```

```python
import jax
import jax.numpy as jnp
from jax import lax
from jax.experimental import pallas as pl
from jax.experimental.pallas import tpu as pltpu
from jax.sharding import Mesh
from jax.sharding import PartitionSpec as P

KSTEPS = 10
DP = ("z", "x")
clip_range = 0.2
noise_level = 0.7
norm_eps = 1e-06
bf16 = jnp.bfloat16
f32 = jnp.float32


def move(value, axis, steps):
    count = lax.axis_size(axis)
    return lax.ppermute(value, axis, [(i, (i + steps) % count) for i in range(count)])


def swap(value, axis, bit):
    count = lax.axis_size(axis)
    return lax.ppermute(value, axis, [(i, i ^ bit) for i in range(count)])


TRAJS = 6
PAIRS = 64
TILE = 8
BLOCK = TRAJS * TILE
CHUNKS = 8


def position():
    z, x, y, c = (lax.axis_index(a) for a in ("z", "x", "y", "c"))
    return z, x, y, c, z * 4 + x


def chunk_owner(q):
    _, _, y, c, _ = position()
    return (y + q % 4) % 4 * 2 + (1 - c if q < 4 else c)


def gather_kernel(slot_table, stamps, latents, noise, behavior, out_first, out_second, own_first, own_second, sems):
    copies = []
    owner = position()[4]
    following = jnp.minimum(owner + 1, 31)
    slots = [slot_table[following * TRAJS + j] for j in range(TRAJS)]
    slots += [slot_table[owner * TRAJS + j] for j in range(TRAJS)]
    for j in range(2 * TRAJS):
        slot = slots[j]
        first, second = (out_first, out_second) if j < TRAJS else (own_first, own_second)
        k = j % TRAJS
        for i, (source, target) in enumerate(
            ((latents, first.at[k, pl.ds(0, PAIRS)]), (noise, second.at[k, 0]), (behavior, second.at[k, 1]))
        ):
            copy = pltpu.make_async_copy(source.at[slot], target, sems.at[3 * j + i])
            copy.start()
            copies.append(copy)
    step = lax.broadcasted_iota(jnp.int32, (16, 128), 0) % 2
    for j in range(2 * TRAJS):
        slot = slots[j]
        tile = jnp.where(step == 0, stamps[0, slot], stamps[1, slot])
        first = out_first if j < TRAJS else own_first
        first[j % TRAJS, pl.ds(PAIRS, 16), :] = tile.astype(f32).astype(bf16)
    for copy in copies:
        copy.wait()


def modulation_rows(stamp_tile, lookup, index):
    rows = jnp.zeros((TILE, lookup.shape[2]), f32)
    for k in range(KSTEPS):
        rows = jnp.where(stamp_tile == k, lookup[k, pl.ds(index, 1), :], rows)
    return rows


def widened(weight, wide, dim):
    size = weight.shape[dim]
    wide[...] = jnp.zeros(wide.shape, wide.dtype)
    if dim == 0:
        wide[0, pl.ds(0, size), :] = weight[...]
        wide[1, pl.ds(size, size), :] = weight[...]
    else:
        wide[0, :, pl.ds(0, size)] = weight[...]
        wide[1, :, pl.ds(size, size)] = weight[...]


def gelu_both(v):
    k = 0.7978845608028654
    square = v * v
    t = jnp.tanh(k * (v + 0.044715 * (square * v)))
    half = 0.5 * (1.0 + t)
    return v * half, half + (0.5 * k) * v * (1.0 - t * t) * (1.0 + (3 * 0.044715) * square)


def forward_kernel(
    source, came, mine, weight_in, lookup_in, up_weight, down_weight,
    tokens, stamps, mod_out, act_out, bend_out, proj_other, proj_own,
    weight, lookup, merged, sorted_, wide, emb, scale, shift, up_w, down_w, modulated, activated, bend, proj, sems,
):
    width = weight.shape[1]
    owner = position()[4]
    load_weight = pltpu.make_async_copy(weight_in, weight, sems.at[7])
    load_lookup = pltpu.make_async_copy(lookup_in, lookup, sems.at[8])
    load_weight.start()
    load_lookup.start()
    load_up = pltpu.make_async_copy(up_weight, up_w, sems.at[0])
    load_down = pltpu.make_async_copy(down_weight, down_w, sems.at[1])
    load_up.start()
    load_down.start()
    for j in range(TRAJS):
        away = source[owner * TRAJS + j] != owner
        merged[pl.ds(j * 80, 80), :] = jnp.where(away, came[j].astype(f32), mine[j].astype(f32))
    for q in range(CHUNKS):
        at_owner = chunk_owner(q)
        for j in range(TRAJS):
            at = pl.multiple_of(j * 80 + at_owner * TILE, TILE)
            sorted_[pl.ds(q * BLOCK + j * TILE, TILE), :] = merged[pl.ds(at, TILE), :]
    tokens[...] = sorted_[...].astype(bf16)
    load_weight.wait()
    load_lookup.wait()
    widened(weight, wide, 0)
    for j in range(TRAJS):
        stamp = merged[pl.ds(j * 80 + PAIRS, TILE), :]
        stamps[pl.ds(j * TILE, TILE), :] = stamp
        stamp = stamp[:, :1]
        shift[pl.ds(j * TILE, TILE), :] = modulation_rows(stamp, lookup, 0)
        scale[pl.ds(j * TILE, TILE), :] = 1.0 + modulation_rows(stamp, lookup, 1)
    for par in range(2):
        emb[par] = jnp.dot(tokens[...], wide[par], preferred_element_type=f32)

    def norm(q, carry):
        for par in range(2):
            values = emb[par, pl.ds(pl.multiple_of(q * BLOCK, BLOCK), BLOCK), :]
            center = values - jnp.sum(values, axis=1, keepdims=True) * (1.0 / width)
            variance = jnp.sum(center * center, axis=1, keepdims=True) * (1.0 / width)
            normed = center * lax.rsqrt(variance + norm_eps)
            at = pl.multiple_of(q * (2 * BLOCK) + par * BLOCK, BLOCK)
            modulated[pl.ds(at, BLOCK), :] = (normed * scale[...] + shift[...]).astype(bf16)
        return carry

    lax.fori_loop(0, CHUNKS, norm, 0)
    save_mod = pltpu.make_async_copy(modulated, mod_out, sems.at[2])
    save_mod.start()
    load_up.wait()
    load_down.wait()

    def hidden(r, carry):
        rows = pl.ds(pl.multiple_of(r * 192, 192), 192)
        pre = jnp.dot(modulated[rows, :], up_w[...], preferred_element_type=f32)
        value, slope = gelu_both(pre)
        value = value.astype(bf16)
        activated[rows, :] = value
        bend[rows, :] = slope.astype(bf16)
        proj[rows, :] = lax.dot_general(
            value, down_w[...], (((1,), (1,)), ((), ())), preferred_element_type=f32
        ).astype(bf16)
        return carry

    half = modulated.shape[0] // 2
    lax.fori_loop(0, 2, hidden, 0)
    save_other = pltpu.make_async_copy(proj.at[pl.ds(0, half)], proj_other, sems.at[3])
    save_other.start()
    lax.fori_loop(2, 4, hidden, 0)
    save_own = pltpu.make_async_copy(proj.at[pl.ds(half, half)], proj_own, sems.at[4])
    save_own.start()
    save_act = pltpu.make_async_copy(activated, act_out, sems.at[5])
    save_act.start()
    save_bend = pltpu.make_async_copy(bend, bend_out, sems.at[6])
    save_bend.start()
    for copy in (save_mod, save_other, save_own, save_act, save_bend):
        copy.wait()


def backward_kernel(
    ranks, far_ranks, source, slot, kept,
    other, own, tokens, stamps, came, mine, weight_in, head, lookup_in,
    act_in, bend_in, mod_in, down_in,
    down_parts, down_low, down_high, up_parts,
    weight, lookup, drawn, target, wide, wide_head, emb, rounded, back, inverse, gate, error, slope, coeff,
    table_v, table, act, bend, mod, down_w, upstream, parts, low, high, pieces,
    sems, out_sems,
):
    z, x, y, c, owner = position()
    place = (z, x)
    load_weight = pltpu.make_async_copy(weight_in, weight, sems.at[10])
    load_lookup = pltpu.make_async_copy(lookup_in, lookup, sems.at[11])
    load_weight.start()
    load_lookup.start()
    loads = [
        pltpu.make_async_copy(a, b, sems.at[i])
        for i, (a, b) in enumerate(((act_in, act), (down_in, down_w), (bend_in, bend), (mod_in, mod)))
    ]
    for copy in loads:
        copy.start()
    for q in range(CHUNKS):
        info = (other if q < 4 else own)[(q + y) % 4, pl.ds(0, 16), pl.ds(weight.shape[1], 128)].astype(f32)
        table_v[pl.ds(chunk_owner(q), 1), :] = (info[0:1] * 32.0 + info[1:2]).astype(jnp.int32)
    fetch = pltpu.make_async_copy(table_v, table, sems.at[4])
    fetch.start()
    width = weight.shape[1]
    values = SEQ_VALUES
    load_weight.wait()
    load_lookup.wait()
    widened(weight, wide, 0)
    widened(head, wide_head, 1)
    for j in range(TRAJS):
        stamp = stamps[pl.ds(j * TILE, TILE), :]
        gate[pl.ds(j * TILE, TILE), :] = modulation_rows(stamp[:, :1], lookup, 2)
        level = 1.0 - stamp * (1.0 / KSTEPS)
        coeff[pl.ds(j * TILE, TILE), :] = (
            jnp.sqrt((1.0 / KSTEPS) * (1.0 - level + 1.0 / KSTEPS) / level) / noise_level
        )
        away = source[owner * TRAJS + j] != owner
        picked = jnp.where(away, came[j].astype(f32), mine[j].astype(f32))
        emb[0, pl.ds(0, PAIRS), pl.ds(0, 128)] = picked[0]
        emb[0, pl.ds(PAIRS, PAIRS), pl.ds(0, 128)] = picked[1]
        for q in range(CHUNKS):
            at = pl.multiple_of(chunk_owner(q) * TILE, TILE)
            drawn[pl.ds(q * BLOCK + j * TILE, TILE), :] = emb[0, pl.ds(at, TILE), pl.ds(0, 128)]
            at = pl.multiple_of(PAIRS + chunk_owner(q) * TILE, TILE)
            target[pl.ds(q * BLOCK + j * TILE, TILE), :] = emb[0, pl.ds(at, TILE), pl.ds(0, 128)]
    for par in range(2):
        emb[par] = jnp.dot(tokens[...], wide[par], preferred_element_type=f32)

    def forward(q, summed):
        for par in range(2):
            rows = pl.ds(pl.multiple_of(q * BLOCK, BLOCK), BLOCK)
            mixed = emb[par, rows, :] + gate[...] * summed[
                (q + y) % 4, pl.ds(par * BLOCK, BLOCK), pl.ds(0, width)
            ].astype(f32)
            center = mixed - jnp.sum(mixed, axis=1, keepdims=True) * (1.0 / width)
            variance = jnp.sum(center * center, axis=1, keepdims=True) * (1.0 / width)
            scale = lax.rsqrt(variance + norm_eps)
            final = center * scale
            emb[par, rows, :] = final
            rounded[par, rows, :] = final.astype(bf16)
            inverse[par, rows, :] = jnp.broadcast_to(scale, (BLOCK, 128))

    def first_half(q, carry):
        forward(q, other)
        return carry

    def second_half(q, carry):
        forward(q + 4, own)
        return carry

    lax.fori_loop(0, 4, first_half, 0)
    lax.fori_loop(0, 4, second_half, 0)
    velocity = jnp.dot(rounded[0], wide_head[0], preferred_element_type=f32)
    error[...] = velocity + jnp.dot(rounded[1], wide_head[1], preferred_element_type=f32) - target[...]
    total = jnp.zeros((BLOCK, 128), f32)
    c = coeff[...]
    for q in range(CHUNKS):
        rows = pl.ds(q * BLOCK, BLOCK)
        err = error[rows, :]
        total = total + c * drawn[rows, :] * err + 0.5 * c * c * err * err
    sums = jnp.broadcast_to(jnp.sum(total, axis=1, keepdims=True), (BLOCK, 128))
    losses = jnp.zeros((TILE, 128), f32)
    fetch.wait()
    gains = advantages(table, ranks, far_ranks, source, slot, kept, owner)
    for j in range(TRAJS):
        unit = sums[j * TILE : (j + 1) * TILE]
        unit = unit + pltpu.roll(unit, 4, 0)
        unit = unit + pltpu.roll(unit, 2, 0)
        ratio = jnp.exp(-unit / values)
        clipped = jnp.clip(ratio, 1.0 - clip_range, 1.0 + clip_range)
        plain = ratio * gains[j]
        bounded = clipped * gains[j]
        losses = losses - jnp.minimum(plain, bounded)
        live = jnp.where(plain <= bounded, 1.0, 0.0)
        slope[pl.ds(j * TILE, TILE), :] = -gains[j] * ratio * live * (1.0 / UNITS)
    total = losses[0:1] + losses[1:2]
    loss_rows = in_three(total, place[0])
    bent = slope[...]
    for q in range(CHUNKS):
        rows = pl.ds(q * BLOCK, BLOCK)
        error[rows, :] = bent * (-(c * drawn[rows, :] + c * c * error[rows, :]) / values)
    dvelocity = error[...].astype(bf16)
    for par in range(2):
        back[par] = lax.dot_general(
            dvelocity, wide_head[par], (((1,), (1,)), ((), ())), preferred_element_type=f32
        )

    def backward(q, carry):
        for par in range(2):
            rows = pl.ds(pl.multiple_of(q * BLOCK, BLOCK), BLOCK)
            d = back[par, rows, :]
            final = emb[par, rows, :]
            mean = jnp.sum(d, axis=1, keepdims=True) * (1.0 / width)
            along = jnp.sum(d * final, axis=1, keepdims=True) * (1.0 / width)
            dmixed = inverse[par, rows, :][:, :1] * (d - mean - final * along)
            at = pl.multiple_of(q * (2 * BLOCK) + par * BLOCK, BLOCK)
            upstream[pl.ds(at, BLOCK), :] = (gate[...] * dmixed).astype(bf16)
        return carry

    lax.fori_loop(0, CHUNKS, backward, 0)
    loads[0].wait()
    tokens_all, hidden = act.shape
    n = hidden // 2
    share = width // 8
    contract = (((0,), (0,)), ((), ()))
    low[pl.ds(share, TILE), :] = loss_rows
    high[pl.ds(share, TILE), :] = jnp.zeros_like(loss_rows)
    for k in range(8):
        parts[k, pl.ds(share, TILE), pl.ds(0, n)] = loss_rows
        parts[k, pl.ds(share, TILE), pl.ds(n, n)] = jnp.zeros_like(loss_rows)

    def down_block(i, carry):
        cols = pl.ds(pl.multiple_of(i * 2 * share, 128), 2 * share)
        total = lax.dot_general(upstream[:, cols], act[...], contract, preferred_element_type=f32).astype(bf16)
        for j in range(2):
            k = (2 * i + j + 8 - place[0]) % 8
            piece = total[j * share : (j + 1) * share]
            parts[k, pl.ds(0, share), :] = piece

            @pl.when(k == 4)
            def _():
                low[pl.ds(0, share), :] = piece[:, :n]
                high[pl.ds(0, share), :] = piece[:, n:]

        return carry

    lax.fori_loop(0, 4, down_block, 0)
    saves = [
        pltpu.make_async_copy(a, b, sems.at[5 + i])
        for i, (a, b) in enumerate(((low, down_low), (high, down_high), (parts, down_parts)))
    ]
    for copy in saves:
        copy.start()
    for copy in loads[1:]:
        copy.wait()

    def bent_rows(r, carry):
        rows = pl.ds(pl.multiple_of(r * 192, 192), 192)
        d = jnp.dot(upstream[rows, :], down_w[...], preferred_element_type=f32)
        bend[rows, :] = (d * bend[rows, :].astype(f32)).astype(bf16)
        return carry

    lax.fori_loop(0, tokens_all // 192, bent_rows, 0)
    quarter = share // 4

    def save_pieces(i):
        rows = pl.ds(2 * i, 2)
        return pltpu.make_async_copy(pieces.at[:, rows], up_parts.at[:, rows], out_sems.at[i])

    def up_block(i, carry):
        cols = pl.ds(pl.multiple_of(i * 2 * share, 128), 2 * share)
        total = lax.dot_general(mod[:, cols], bend[...], contract, preferred_element_type=f32).astype(bf16)
        for j in range(8):
            pieces[j % 4, 2 * i + j // 4] = total[j * quarter : (j + 1) * quarter]
        save_pieces(i).start()
        return carry

    lax.fori_loop(0, 4, up_block, 0)
    for i in range(4):
        save_pieces(i).wait()
    for copy in saves:
        copy.wait()


def in_three(value, lane):
    rows = jnp.broadcast_to(value, (TILE, 128))
    first = rows.astype(bf16).astype(f32)
    second = (rows - first).astype(bf16).astype(f32)
    third = (rows - first - second).astype(bf16).astype(f32)
    row = lax.broadcasted_iota(jnp.int32, (TILE, 128), 0)
    col = lax.broadcasted_iota(jnp.int32, (TILE, 128), 1)
    chosen = jnp.where(row == 0, first, jnp.where(row == 1, second, jnp.where(row == 2, third, 0.0)))
    tile = jnp.where(col == lane, chosen, 0.0)
    return jnp.concatenate([tile, jnp.zeros((TILE, 384), f32)], axis=1).astype(bf16)


def advantages(table, ranks, far_ranks, source, slot, kept, owner):
    def rank_of(p):
        d = source[p] - owner
        s = slot[p]
        f = jnp.clip(jnp.where(d < 0, d + 5, d + 4), 0, 7)
        return jnp.where(d == 0, ranks[s], jnp.where(d == 4, far_ranks[s], table[f, s]))

    def seek(g, state):
        end = state[0]
        after = end + kept[g]
        out = [after]
        for j in range(TRAJS):
            p = owner * TRAJS + j
            here = (p >= end) & (p < after)
            out.append(jnp.where(here, end, state[1 + 2 * j]))
            out.append(jnp.where(here, kept[g], state[2 + 2 * j]))
        return tuple(out)

    state = lax.fori_loop(0, kept.shape[0], seek, (jnp.int32(0),) + (jnp.int32(0), jnp.int32(1)) * TRAJS)
    gains = []
    for j in range(TRAJS):
        begin, count = state[1 + 2 * j], state[2 + 2 * j]

        def add(q, sums):
            rank = rank_of(q)
            return sums[0] + rank, sums[1] + rank * rank

        first, second = lax.fori_loop(begin, begin + count, add, (jnp.int32(0), jnp.int32(0)))

        def row(value):
            return jnp.full((1, 128), value, jnp.int32).astype(f32)

        counts = row(count)
        deviation = jnp.sqrt(row(count * second - first * first)) / counts
        gains.append((row(rank_of(owner * TRAJS + j)) - row(first) / counts) / jnp.maximum(deviation, 1.0))
    return gains


NEAR = (-5, -4, -3, -2, -1, 1, 2, 3)
SEQ_VALUES = 4096
UNITS = 384
SMEM = pl.BlockSpec(memory_space=pltpu.SMEM)
VMEM = pl.BlockSpec(memory_space=pltpu.VMEM)
HBM = pl.BlockSpec(memory_space=pltpu.HBM)


def wide_add(*parts):
    total = parts[0].astype(f32)
    for part in parts[1:]:
        total = total + part.astype(f32)
    return total


def call(kernel, shapes, count, **kw):
    return pl.pallas_call(
        kernel,
        out_shape=tuple(jax.ShapeDtypeStruct(shape, dtype) for shape, dtype in shapes),
        in_specs=[VMEM] * count,
        out_specs=(VMEM,) * len(shapes),
        compiler_params=pltpu.CompilerParams(vmem_limit_bytes=6 << 20),
        **kw,
    )


def fold_kernel(mine, got, out):
    y = position()[2]
    for k in range(4):
        out[(y + k) % 4] = (mine[k].astype(f32) + got[k].astype(f32)).astype(bf16)


def close_kernel(ranks, parts, out):
    width = parts.shape[2]
    col = lax.broadcasted_iota(jnp.int32, (16, 128), 1)
    row = lax.broadcasted_iota(jnp.int32, (16, 128), 0)
    values = jnp.zeros((16, 128), jnp.int32)
    for i in range(ranks.shape[0]):
        values = jnp.where(col == i, ranks[i], values)
    values = jnp.where(row == 0, values // 32, jnp.where(row == 1, values % 32, 0)).astype(f32).astype(bf16)
    total = parts[0].astype(f32)
    for k in range(1, 4):
        total = total + parts[k].astype(f32)
    total = total.astype(bf16)
    for k in range(4):
        out[k, :, pl.ds(0, width)] = total
        out[k, :, pl.ds(width, 128)] = jnp.zeros((out.shape[1], 128), bf16)
        out[k, pl.ds(0, 16), pl.ds(width, 128)] = values


def sum_kernel(parts, out):
    total = parts[0].astype(f32)
    for k in range(1, parts.shape[0]):
        total = total + parts[k].astype(f32)
    out[...] = total.astype(out.dtype)


def swapped(value, axis):
    return lax.all_to_all(value, axis, 0, 0, tiled=True)


def half_add_kernel(part, recv, out, *, lead):
    n = recv.shape[1]
    total = (part[0, :, pl.ds(lead * n, n)].astype(f32) + recv[...].astype(f32)).astype(bf16)
    out[:, pl.ds(lead * n, n)] = total
    out[:, pl.ds((1 - lead) * n, n)] = part[0, :, pl.ds((1 - lead) * n, n)]


def half_add(parts, index, recv, lead):
    block = parts.shape[1:]
    return pl.pallas_call(
        lambda *refs: half_add_kernel(*refs, lead=lead),
        grid=(1,),
        out_shape=jax.ShapeDtypeStruct(block, bf16),
        in_specs=[
            pl.BlockSpec((1, *block), lambda i: (index, 0, 0)),
            pl.BlockSpec(recv.shape, lambda i: (0, 0)),
        ],
        out_specs=pl.BlockSpec(block, lambda i: (0, 0)),
        compiler_params=pltpu.CompilerParams(vmem_limit_bytes=6 << 20),
        name="ring_second",
    )(parts, recv)


def ring_of_eight(parts, low, high, third, fourth):
    def both(down, up, beside=lambda: ()):
        down, up = move(down, "z", -1), move(up, "z", 1)
        return lax.optimization_barrier((down, up, beside()))

    from_up, from_down, _ = both(low, high)
    down = half_add(parts, 5, from_up, 0)
    up = half_add(parts, 3, from_down, 1)
    from_up, from_down, _ = both(down, up)
    down = wide_add(parts[6], from_up).astype(bf16)
    up = wide_add(parts[2], from_down).astype(bf16)
    from_up, from_down, ready = both(down, up, third)
    down = wide_add(parts[7], from_up).astype(bf16)
    up = wide_add(parts[1], from_down).astype(bf16)
    return both(down, up, lambda: fourth(ready))


def turn_kernel(part, from_up, from_down, out):
    n = out.shape[2] // 2
    own = out.shape[1] - TILE

    def summed(rows):
        return part[0, rows, :].astype(f32) + from_up[rows, :].astype(f32) + from_down[rows, :].astype(f32)

    loss = jnp.sum(jnp.sum(summed(pl.ds(4 * own, TILE))[:, :128], axis=1, keepdims=True), axis=0, keepdims=True)
    loss_rows = in_three(jnp.broadcast_to(loss, (1, 128)), position()[1])
    for k in range(4):
        out[k, pl.ds(0, own), :] = summed(pl.ds(k * own, own)).astype(bf16)
        out[k, pl.ds(own, TILE), pl.ds(0, n)] = loss_rows
        out[k, pl.ds(own, TILE), pl.ds(n, n)] = jnp.zeros_like(loss_rows)


def last_kernel(parts, grad, loss):
    own = grad.shape[0]
    total = parts[0].astype(f32)
    for k in range(1, 4):
        total = total + parts[k].astype(f32)
    grad[...] = total[:own]
    found = jnp.sum(jnp.sum(total[own:, :128], axis=1, keepdims=True), axis=0, keepdims=True)
    loss[...] = jnp.broadcast_to(found * (1.0 / UNITS), loss.shape)


def spread_kernel(parts, down, up, further, keep):
    z = position()[0]
    for k in range(8):
        block = (z + k) % 8
        total = parts[0, block].astype(f32)
        for j in range(1, 4):
            total = total + parts[j, block].astype(f32)
        total = total.astype(bf16)
        if k in (7, 5):
            down[(7, 5).index(k)] = total
        elif k in (1, 3):
            up[(1, 3).index(k)] = total
        elif k == 4:
            further[...] = total
        else:
            keep[{0: 0, 2: 1, 6: 2}[k]] = total


def meet_kernel(keep, from_up, from_down, from_further, down, up, own):
    up[...] = (keep[1].astype(f32) + from_down[1].astype(f32)).astype(bf16)
    down[...] = (keep[2].astype(f32) + from_up[1].astype(f32) + from_further[...].astype(f32)).astype(bf16)
    own[...] = keep[0].astype(f32) + from_up[0].astype(f32) + from_down[0].astype(f32)


def finish_kernel(own, late_up, late_down, out):
    out[...] = own[...] + late_up[...].astype(f32) + late_down[...].astype(f32)


def shards(
    latents,
    noise,
    behavior_velocity,
    timestep,
    reward_rank_integer,
    surviving_source_index,
    surviving_slot_index,
    group_kept_count,
    patch_input_weight,
    modulation_lookup,
    up_projection_weight,
    down_projection_weight,
    velocity_head_weight,
):
    ranks_dp = lax.axis_size(DP)
    surviving = surviving_source_index.shape[0]
    trajs = surviving // ranks_dp
    steps = timestep.shape[1]
    capacity = latents.shape[0]

    def pairs(a):
        return a.reshape(capacity, steps, 32, 128).transpose(0, 2, 1, 3).reshape(capacity, 64, 128)

    width = patch_input_weight.shape[1]
    rows = 8 * 2 * trajs * 8
    one = jax.ShapeDtypeStruct((TRAJS, 80, 128), bf16)
    two = jax.ShapeDtypeStruct((TRAJS, 2, PAIRS, 128), bf16)
    out_first, out_second, own_first, own_second = pl.pallas_call(
        gather_kernel,
        out_shape=(one, two, one, two),
        in_specs=[SMEM, SMEM, HBM, HBM, HBM],
        out_specs=(VMEM, VMEM, VMEM, VMEM),
        scratch_shapes=[pltpu.SemaphoreType.DMA((6 * TRAJS,))],
        name="gather_slots",
    )(
        surviving_slot_index, timestep.T,
        pairs(latents), pairs(noise), pairs(behavior_velocity),
    )
    onward = [(i, i + 1) for i in range(ranks_dp - 1)]
    near = [
        ((d + hop) * 8 + f, d * 8 + f) for d in range(ranks_dp) for f, hop in enumerate(NEAR) if 0 <= d + hop < ranks_dp
    ]
    near_ranks = lax.ppermute(reward_rank_integer, ("z", "x", "y", "c"), near)
    far_ranks = lax.ppermute(reward_rank_integer, DP, [(d + 4, d) for d in range(ranks_dp - 4)])
    came = lax.ppermute(out_first, DP, onward)
    came_late = lax.ppermute(out_second, DP, onward)
    hidden = up_projection_weight.shape[1]
    half = rows // 2
    tokens, stamps, modulated, activated, bend, proj_other, proj_own = pl.pallas_call(
        forward_kernel,
        out_shape=(
            jax.ShapeDtypeStruct((CHUNKS * BLOCK, 128), bf16),
            jax.ShapeDtypeStruct((BLOCK, 128), f32),
            jax.ShapeDtypeStruct((rows, width), bf16),
            jax.ShapeDtypeStruct((rows, hidden), bf16),
            jax.ShapeDtypeStruct((rows, hidden), bf16),
            jax.ShapeDtypeStruct((half, width), bf16),
            jax.ShapeDtypeStruct((half, width), bf16),
        ),
        in_specs=[SMEM, VMEM, VMEM, HBM, HBM, HBM, HBM],
        out_specs=(VMEM, VMEM, HBM, HBM, HBM, HBM, HBM),
        scratch_shapes=[
            pltpu.VMEM(patch_input_weight.shape, bf16),
            pltpu.VMEM(modulation_lookup.shape, f32),
            pltpu.VMEM((TRAJS * 80, 128), f32),
            pltpu.VMEM((CHUNKS * BLOCK, 128), f32),
            pltpu.VMEM((2, 128, width), bf16),
            pltpu.VMEM((2, CHUNKS * BLOCK, width), f32),
            pltpu.VMEM((BLOCK, width), f32),
            pltpu.VMEM((BLOCK, width), f32),
            pltpu.VMEM((width, hidden), bf16),
            pltpu.VMEM((width, hidden), bf16),
            pltpu.VMEM((rows, width), bf16),
            pltpu.VMEM((rows, hidden), bf16),
            pltpu.VMEM((rows, hidden), bf16),
            pltpu.VMEM((rows, width), bf16),
            pltpu.SemaphoreType.DMA((9,)),
        ],
        compiler_params=pltpu.CompilerParams(vmem_limit_bytes=60 << 20),
        name="forward",
    )(surviving_source_index, came, own_first, patch_input_weight, modulation_lookup, up_projection_weight, down_projection_weight)
    got = swap(proj_other, "c", 1)
    piece = rows // 8
    (folded,) = call(fold_kernel, [((4, piece, width), bf16)], 2, name="fold")(
        proj_own.reshape(4, piece, width), got.reshape(4, piece, width)
    )
    gathered = swapped(folded, "y")
    gathered, came_late, near_ranks, far_ranks = lax.optimization_barrier((gathered, came_late, near_ranks, far_ranks))
    closed = pl.pallas_call(
        close_kernel,
        out_shape=jax.ShapeDtypeStruct((4, piece, width + 128), bf16),
        in_specs=[SMEM, VMEM],
        out_specs=VMEM,
        compiler_params=pltpu.CompilerParams(vmem_limit_bytes=6 << 20),
        name="close",
    )(near_ranks, gathered)
    summed_own = swapped(closed, "y")
    summed_other = swap(summed_own, "c", 1)
    own_rows = width // ranks_dp
    m = hidden // 2
    share = 4 * own_rows
    down_parts, down_low, down_high, up_parts = pl.pallas_call(
        backward_kernel,
        out_shape=(
            jax.ShapeDtypeStruct((8, share + TILE, hidden), bf16),
            jax.ShapeDtypeStruct((share + TILE, m), bf16),
            jax.ShapeDtypeStruct((share + TILE, m), bf16),
            jax.ShapeDtypeStruct((4, 8, own_rows, hidden), bf16),
        ),
        in_specs=[SMEM] * 5 + [VMEM] * 6 + [HBM, VMEM, HBM] + [HBM] * 4,
        out_specs=(HBM,) * 4,
        scratch_shapes=[
            pltpu.VMEM(patch_input_weight.shape, bf16),
            pltpu.VMEM(modulation_lookup.shape, f32),
            pltpu.VMEM((CHUNKS * BLOCK, 128), f32),
            pltpu.VMEM((CHUNKS * BLOCK, 128), f32),
            pltpu.VMEM((2, 128, width), bf16),
            pltpu.VMEM((2, width, 128), bf16),
            pltpu.VMEM((2, CHUNKS * BLOCK, width), f32),
            pltpu.VMEM((2, CHUNKS * BLOCK, width), bf16),
            pltpu.VMEM((2, CHUNKS * BLOCK, width), f32),
            pltpu.VMEM((2, CHUNKS * BLOCK, 128), f32),
            pltpu.VMEM((BLOCK, width), f32),
            pltpu.VMEM((CHUNKS * BLOCK, 128), f32),
            pltpu.VMEM((BLOCK, 128), f32),
            pltpu.VMEM((BLOCK, 128), f32),
            pltpu.VMEM((8, 128), jnp.int32),
            pltpu.SMEM((8, 128), jnp.int32),
            pltpu.VMEM((rows, hidden), bf16),
            pltpu.VMEM((rows, hidden), bf16),
            pltpu.VMEM((rows, width), bf16),
            pltpu.VMEM((width, hidden), bf16),
            pltpu.VMEM((rows, width), bf16),
            pltpu.VMEM((8, share + TILE, hidden), bf16),
            pltpu.VMEM((share + TILE, m), bf16),
            pltpu.VMEM((share + TILE, m), bf16),
            pltpu.VMEM((4, 8, own_rows, hidden), bf16),
            pltpu.SemaphoreType.DMA((12,)),
            pltpu.SemaphoreType.DMA((4,)),
        ],
        compiler_params=pltpu.CompilerParams(vmem_limit_bytes=60 << 20),
        name="backward",
    )(
        reward_rank_integer, far_ranks, surviving_source_index, surviving_slot_index, group_kept_count,
        summed_other, summed_own, tokens, stamps, came_late, own_second,
        patch_input_weight, velocity_head_weight, modulation_lookup,
        activated, bend, modulated, down_projection_weight,
    )

    up_gathered = swapped(up_parts, "x")

    chunk = (own_rows, hidden)

    def spread(gathered):
        down, up, further, keep = call(
            spread_kernel,
            [((2, *chunk), bf16), ((2, *chunk), bf16), (chunk, bf16), ((3, *chunk), bf16)],
            1,
            name="spread",
        )(gathered)
        return keep, move(down, "z", -1), move(up, "z", 1), move(further, "z", -2)

    from_z_up, from_z_down, (keep, from_up, from_down, from_further) = ring_of_eight(
        down_parts, down_low, down_high, lambda: up_gathered, spread
    )
    tall = share + TILE
    short = own_rows + TILE
    turned = pl.pallas_call(
        turn_kernel,
        grid=(1,),
        out_shape=jax.ShapeDtypeStruct((4, short, hidden), bf16),
        in_specs=[
            pl.BlockSpec((1, tall, hidden), lambda i: (0, 0, 0)),
            pl.BlockSpec((tall, hidden), lambda i: (0, 0)),
            pl.BlockSpec((tall, hidden), lambda i: (0, 0)),
        ],
        out_specs=pl.BlockSpec((4, short, hidden), lambda i: (0, 0, 0)),
        compiler_params=pltpu.CompilerParams(vmem_limit_bytes=8 << 20),
        name="turn",
    )(down_parts, from_z_up, from_z_down)
    down_grad, loss = call(
        last_kernel, [((own_rows, hidden), f32), ((TILE, 128), f32)], 1, name="last"
    )(swapped(turned, "x"))
    down, up, kept = call(meet_kernel, [(chunk, bf16), (chunk, bf16), (chunk, f32)], 4, name="meet")(
        keep, from_up, from_down, from_further
    )
    (up_grad,) = call(finish_kernel, [(chunk, f32)], 3, name="finish")(
        kept, *lax.optimization_barrier((move(down, "z", -2), move(up, "z", 2)))
    )
    return (up_grad, down_grad, loss[0, 0])


def solution(mesh):
    finer = Mesh(mesh.devices.reshape(8, 4, 4, 2), ("z", "x", "y", "c"))
    dp, fsdp = ("z", "x"), ("y", "c")
    in_specs = (
        P(dp, None, None),
        P(dp, None, None),
        P(dp, None, None),
        P(dp, None),
        P(dp),
        P(),
        P(),
        P(),
        P(),
        P(),
        P(None, fsdp),
        P(None, fsdp),
        P(),
    )
    out_specs = (P(dp, fsdp), P(dp, fsdp), P())
    return jax.shard_map(
        shards, mesh=finer, in_specs=in_specs, out_specs=out_specs, check_vma=False
    )
```

```python
import jax
import jax.numpy as jnp
from jax import lax
from jax.experimental import pallas as pl
from jax.experimental.pallas import tpu as pltpu
from jax.sharding import Mesh
from jax.sharding import PartitionSpec as P

KSTEPS = 10
DP = ("z", "x")
clip_range = 0.2
noise_level = 0.7
norm_eps = 1e-06
bf16 = jnp.bfloat16
f32 = jnp.float32


def move(value, axis, steps):
    count = lax.axis_size(axis)
    return lax.ppermute(value, axis, [(i, (i + steps) % count) for i in range(count)])


def swap(value, axis, bit):
    count = lax.axis_size(axis)
    return lax.ppermute(value, axis, [(i, i ^ bit) for i in range(count)])


TRAJS = 6
PAIRS = 64
TILE = 8
BLOCK = TRAJS * TILE
CHUNKS = 8


def position():
    z, x, y, c = (lax.axis_index(a) for a in ("z", "x", "y", "c"))
    return z, x, y, c, z * 4 + x


def chunk_owner(q):
    _, _, y, c, _ = position()
    return (y + q % 4) % 4 * 2 + (1 - c if q < 4 else c)


def gather_kernel(slot_table, stamps, latents, noise, behavior, out_first, out_second, own_first, own_second, sems):
    copies = []
    owner = position()[4]
    following = jnp.minimum(owner + 1, 31)
    slots = [slot_table[following * TRAJS + j] for j in range(TRAJS)]
    slots += [slot_table[owner * TRAJS + j] for j in range(TRAJS)]
    for j in range(2 * TRAJS):
        slot = slots[j]
        first, second = (out_first, out_second) if j < TRAJS else (own_first, own_second)
        k = j % TRAJS
        for i, (source, target) in enumerate(
            ((latents, first.at[k, pl.ds(0, PAIRS)]), (noise, second.at[k, 0]), (behavior, second.at[k, 1]))
        ):
            copy = pltpu.make_async_copy(source.at[slot], target, sems.at[3 * j + i])
            copy.start()
            copies.append(copy)
    step = lax.broadcasted_iota(jnp.int32, (16, 128), 0) % 2
    for j in range(2 * TRAJS):
        slot = slots[j]
        tile = jnp.where(step == 0, stamps[0, slot], stamps[1, slot])
        first = out_first if j < TRAJS else own_first
        first[j % TRAJS, pl.ds(PAIRS, 16), :] = tile.astype(f32).astype(bf16)
    for copy in copies:
        copy.wait()


def modulation_rows(stamp_tile, lookup, index):
    rows = jnp.zeros((TILE, lookup.shape[2]), f32)
    for k in range(KSTEPS):
        rows = jnp.where(stamp_tile == k, lookup[k, pl.ds(index, 1), :], rows)
    return rows


def widened(weight, wide):
    size = weight.shape[0]
    wide[...] = jnp.zeros(wide.shape, wide.dtype)
    wide[0, pl.ds(0, size), :] = weight[...]
    wide[1, pl.ds(size, size), :] = weight[...]


def gelu_both(v):
    k = 0.7978845608028654
    square = v * v
    t = jnp.tanh(k * (v + 0.044715 * (square * v)))
    half = 0.5 * (1.0 + t)
    return v * half, half + (0.5 * k) * v * (1.0 - t * t) * (1.0 + (3 * 0.044715) * square)


def forward_kernel(
    source, came, mine, weight_in, lookup_in, up_weight, down_weight,
    tokens, stamps, mod_out, act_out, bend_out, proj_other, proj_own,
    weight, lookup, merged, sorted_, wide, emb, scale, shift, up_w, down_w, modulated, activated, bend, proj, sems,
):
    width = weight.shape[1]
    owner = position()[4]
    load_weight = pltpu.make_async_copy(weight_in, weight, sems.at[7])
    load_lookup = pltpu.make_async_copy(lookup_in, lookup, sems.at[8])
    load_weight.start()
    load_lookup.start()
    load_up = pltpu.make_async_copy(up_weight, up_w, sems.at[0])
    load_down = pltpu.make_async_copy(down_weight, down_w, sems.at[1])
    load_up.start()
    load_down.start()
    for j in range(TRAJS):
        away = source[owner * TRAJS + j] != owner
        merged[pl.ds(j * 80, 80), :] = jnp.where(away, came[j].astype(f32), mine[j].astype(f32))
    for q in range(CHUNKS):
        at_owner = chunk_owner(q)
        for j in range(TRAJS):
            at = pl.multiple_of(j * 80 + at_owner * TILE, TILE)
            sorted_[pl.ds(q * BLOCK + j * TILE, TILE), :] = merged[pl.ds(at, TILE), :]
    tokens[...] = sorted_[...].astype(bf16)
    load_weight.wait()
    load_lookup.wait()
    widened(weight, wide)
    for j in range(TRAJS):
        stamp = merged[pl.ds(j * 80 + PAIRS, TILE), :]
        stamps[pl.ds(j * TILE, TILE), :] = stamp
        stamp = stamp[:, :1]
        shift[pl.ds(j * TILE, TILE), :] = modulation_rows(stamp, lookup, 0)
        scale[pl.ds(j * TILE, TILE), :] = 1.0 + modulation_rows(stamp, lookup, 1)
    for par in range(2):
        emb[par] = jnp.dot(tokens[...], wide[par], preferred_element_type=f32)

    def norm(q, carry):
        for par in range(2):
            values = emb[par, pl.ds(pl.multiple_of(q * BLOCK, BLOCK), BLOCK), :]
            center = values - jnp.sum(values, axis=1, keepdims=True) * (1.0 / width)
            variance = jnp.sum(center * center, axis=1, keepdims=True) * (1.0 / width)
            normed = center * lax.rsqrt(variance + norm_eps)
            at = pl.multiple_of(q * (2 * BLOCK) + par * BLOCK, BLOCK)
            modulated[pl.ds(at, BLOCK), :] = (normed * scale[...] + shift[...]).astype(bf16)
        return carry

    lax.fori_loop(0, CHUNKS, norm, 0)
    save_mod = pltpu.make_async_copy(modulated, mod_out, sems.at[2])
    save_mod.start()
    load_up.wait()
    load_down.wait()

    def hidden(r, carry):
        rows = pl.ds(pl.multiple_of(r * 192, 192), 192)
        pre = jnp.dot(modulated[rows, :], up_w[...], preferred_element_type=f32)
        value, slope = gelu_both(pre)
        value = value.astype(bf16)
        activated[rows, :] = value
        bend[rows, :] = slope.astype(bf16)
        proj[rows, :] = lax.dot_general(
            value, down_w[...], (((1,), (1,)), ((), ())), preferred_element_type=f32
        ).astype(bf16)
        return carry

    half = modulated.shape[0] // 2
    lax.fori_loop(0, 2, hidden, 0)
    save_other = pltpu.make_async_copy(proj.at[pl.ds(0, half)], proj_other, sems.at[3])
    save_other.start()
    lax.fori_loop(2, 4, hidden, 0)
    save_own = pltpu.make_async_copy(proj.at[pl.ds(half, half)], proj_own, sems.at[4])
    save_own.start()
    save_act = pltpu.make_async_copy(activated, act_out, sems.at[5])
    save_act.start()
    save_bend = pltpu.make_async_copy(bend, bend_out, sems.at[6])
    save_bend.start()
    for copy in (save_mod, save_other, save_own, save_act, save_bend):
        copy.wait()


def backward_kernel(
    ranks, far_ranks, source, slot, kept,
    other, own, tokens, stamps, came, mine, weight_in, head, lookup_in,
    act_in, bend_in, mod_in, down_in,
    down_parts, down_low, down_high, up_parts,
    weight, lookup, drawn, target, wide, wide_head, emb, rounded, back, inverse, gate, error, slope, coeff,
    table_v, table, act, bend, mod, down_w, upstream, parts, low, high, pieces,
    sems, out_sems,
):
    z, x, y, c, owner = position()
    place = (z, x)
    load_weight = pltpu.make_async_copy(weight_in, weight, sems.at[10])
    load_lookup = pltpu.make_async_copy(lookup_in, lookup, sems.at[11])
    load_weight.start()
    load_lookup.start()
    loads = [
        pltpu.make_async_copy(a, b, sems.at[i])
        for i, (a, b) in enumerate(((act_in, act), (down_in, down_w), (bend_in, bend), (mod_in, mod)))
    ]
    for copy in loads:
        copy.start()
    for q in range(CHUNKS):
        info = (other if q < 4 else own)[(q + y) % 4, pl.ds(0, 16), pl.ds(weight.shape[1], 128)].astype(f32)
        table_v[pl.ds(chunk_owner(q), 1), :] = (info[0:1] * 32.0 + info[1:2]).astype(jnp.int32)
    fetch = pltpu.make_async_copy(table_v, table, sems.at[4])
    fetch.start()
    width = weight.shape[1]
    values = SEQ_VALUES
    load_weight.wait()
    load_lookup.wait()
    widened(weight, wide)
    widened(head, wide_head)
    for j in range(TRAJS):
        stamp = stamps[pl.ds(j * TILE, TILE), :]
        gate[pl.ds(j * TILE, TILE), :] = modulation_rows(stamp[:, :1], lookup, 2)
        level = 1.0 - stamp * (1.0 / KSTEPS)
        coeff[pl.ds(j * TILE, TILE), :] = (
            jnp.sqrt((1.0 / KSTEPS) * (1.0 - level + 1.0 / KSTEPS) / level) / noise_level
        )
        away = source[owner * TRAJS + j] != owner
        picked = jnp.where(away, came[j].astype(f32), mine[j].astype(f32))
        emb[0, pl.ds(0, PAIRS), pl.ds(0, 128)] = picked[0]
        emb[0, pl.ds(PAIRS, PAIRS), pl.ds(0, 128)] = picked[1]
        for q in range(CHUNKS):
            at = pl.multiple_of(chunk_owner(q) * TILE, TILE)
            drawn[pl.ds(q * BLOCK + j * TILE, TILE), :] = emb[0, pl.ds(at, TILE), pl.ds(0, 128)]
            at = pl.multiple_of(PAIRS + chunk_owner(q) * TILE, TILE)
            target[pl.ds(q * BLOCK + j * TILE, TILE), :] = emb[0, pl.ds(at, TILE), pl.ds(0, 128)]
    for par in range(2):
        emb[par] = jnp.dot(tokens[...], wide[par], preferred_element_type=f32)

    def forward(q, summed):
        for par in range(2):
            rows = pl.ds(pl.multiple_of(q * BLOCK, BLOCK), BLOCK)
            mixed = emb[par, rows, :] + gate[...] * summed[
                (q + y) % 4, pl.ds(par * BLOCK, BLOCK), pl.ds(0, width)
            ].astype(f32)
            center = mixed - jnp.sum(mixed, axis=1, keepdims=True) * (1.0 / width)
            variance = jnp.sum(center * center, axis=1, keepdims=True) * (1.0 / width)
            scale = lax.rsqrt(variance + norm_eps)
            final = center * scale
            emb[par, rows, :] = final
            rounded[par, rows, :] = final.astype(bf16)
            inverse[par, rows, :] = jnp.broadcast_to(scale, (BLOCK, 128))

    def first_half(q, carry):
        forward(q, other)
        return carry

    def second_half(q, carry):
        forward(q + 4, own)
        return carry

    lax.fori_loop(0, 4, first_half, 0)
    lax.fori_loop(0, 4, second_half, 0)
    across = (((1,), (1,)), ((), ()))
    velocity = lax.dot_general(rounded[0], wide_head[0], across, preferred_element_type=f32)
    velocity = velocity + lax.dot_general(rounded[1], wide_head[1], across, preferred_element_type=f32)
    error[...] = velocity - target[...]
    total = jnp.zeros((BLOCK, 128), f32)
    c = coeff[...]
    for q in range(CHUNKS):
        rows = pl.ds(q * BLOCK, BLOCK)
        err = error[rows, :]
        total = total + c * drawn[rows, :] * err + 0.5 * c * c * err * err
    sums = jnp.broadcast_to(jnp.sum(total, axis=1, keepdims=True), (BLOCK, 128))
    losses = jnp.zeros((TILE, 128), f32)
    fetch.wait()
    gains = advantages(table, ranks, far_ranks, source, slot, kept, owner)
    for j in range(TRAJS):
        unit = sums[j * TILE : (j + 1) * TILE]
        unit = unit + pltpu.roll(unit, 4, 0)
        unit = unit + pltpu.roll(unit, 2, 0)
        ratio = jnp.exp(-unit / values)
        clipped = jnp.clip(ratio, 1.0 - clip_range, 1.0 + clip_range)
        plain = ratio * gains[j]
        bounded = clipped * gains[j]
        losses = losses - jnp.minimum(plain, bounded)
        live = jnp.where(plain <= bounded, 1.0, 0.0)
        slope[pl.ds(j * TILE, TILE), :] = -gains[j] * ratio * live * (1.0 / UNITS)
    total = losses[0:1] + losses[1:2]
    loss_rows = in_three(total, place[0])
    bent = slope[...]
    for q in range(CHUNKS):
        rows = pl.ds(q * BLOCK, BLOCK)
        error[rows, :] = bent * (-(c * drawn[rows, :] + c * c * error[rows, :]) / values)
    dvelocity = error[...].astype(bf16)
    for par in range(2):
        back[par] = jnp.dot(dvelocity, wide_head[par], preferred_element_type=f32)

    def backward(q, carry):
        for par in range(2):
            rows = pl.ds(pl.multiple_of(q * BLOCK, BLOCK), BLOCK)
            d = back[par, rows, :]
            final = emb[par, rows, :]
            mean = jnp.sum(d, axis=1, keepdims=True) * (1.0 / width)
            along = jnp.sum(d * final, axis=1, keepdims=True) * (1.0 / width)
            dmixed = inverse[par, rows, :][:, :1] * (d - mean - final * along)
            at = pl.multiple_of(q * (2 * BLOCK) + par * BLOCK, BLOCK)
            upstream[pl.ds(at, BLOCK), :] = (gate[...] * dmixed).astype(bf16)
        return carry

    lax.fori_loop(0, CHUNKS, backward, 0)
    loads[0].wait()
    tokens_all, hidden = act.shape
    n = hidden // 2
    share = width // 8
    contract = (((0,), (0,)), ((), ()))
    low[pl.ds(share, TILE), :] = loss_rows
    high[pl.ds(share, TILE), :] = jnp.zeros_like(loss_rows)
    for k in range(8):
        parts[k, pl.ds(share, TILE), pl.ds(0, n)] = loss_rows
        parts[k, pl.ds(share, TILE), pl.ds(n, n)] = jnp.zeros_like(loss_rows)

    def down_block(i, carry):
        cols = pl.ds(pl.multiple_of(i * 2 * share, 128), 2 * share)
        total = lax.dot_general(upstream[:, cols], act[...], contract, preferred_element_type=f32).astype(bf16)
        for j in range(2):
            k = (2 * i + j + 8 - place[0]) % 8
            piece = total[j * share : (j + 1) * share]
            parts[k, pl.ds(0, share), :] = piece

            @pl.when(k == 4)
            def _():
                low[pl.ds(0, share), :] = piece[:, :n]
                high[pl.ds(0, share), :] = piece[:, n:]

        return carry

    lax.fori_loop(0, 4, down_block, 0)
    saves = [
        pltpu.make_async_copy(a, b, sems.at[5 + i])
        for i, (a, b) in enumerate(((low, down_low), (high, down_high), (parts, down_parts)))
    ]
    for copy in saves:
        copy.start()
    for copy in loads[1:]:
        copy.wait()

    def bent_rows(r, carry):
        rows = pl.ds(pl.multiple_of(r * 192, 192), 192)
        d = jnp.dot(upstream[rows, :], down_w[...], preferred_element_type=f32)
        bend[rows, :] = (d * bend[rows, :].astype(f32)).astype(bf16)
        return carry

    lax.fori_loop(0, tokens_all // 192, bent_rows, 0)
    quarter = share // 4

    def save_pieces(i):
        rows = pl.ds(2 * i, 2)
        return pltpu.make_async_copy(pieces.at[:, rows], up_parts.at[:, rows], out_sems.at[i])

    def up_block(i, carry):
        cols = pl.ds(pl.multiple_of(i * 2 * share, 128), 2 * share)
        total = lax.dot_general(mod[:, cols], bend[...], contract, preferred_element_type=f32).astype(bf16)
        for j in range(8):
            pieces[j % 4, 2 * i + j // 4] = total[j * quarter : (j + 1) * quarter]
        save_pieces(i).start()
        return carry

    lax.fori_loop(0, 4, up_block, 0)
    for i in range(4):
        save_pieces(i).wait()
    for copy in saves:
        copy.wait()


def in_three(value, lane):
    rows = jnp.broadcast_to(value, (TILE, 128))
    first = rows.astype(bf16).astype(f32)
    second = (rows - first).astype(bf16).astype(f32)
    third = (rows - first - second).astype(bf16).astype(f32)
    row = lax.broadcasted_iota(jnp.int32, (TILE, 128), 0)
    col = lax.broadcasted_iota(jnp.int32, (TILE, 128), 1)
    chosen = jnp.where(row == 0, first, jnp.where(row == 1, second, jnp.where(row == 2, third, 0.0)))
    tile = jnp.where(col == lane, chosen, 0.0)
    return jnp.concatenate([tile, jnp.zeros((TILE, 384), f32)], axis=1).astype(bf16)


def advantages(table, ranks, far_ranks, source, slot, kept, owner):
    def rank_of(p):
        d = source[p] - owner
        s = slot[p]
        f = jnp.clip(jnp.where(d < 0, d + 5, d + 4), 0, 7)
        return jnp.where(d == 0, ranks[s], jnp.where(d == 4, far_ranks[s], table[f, s]))

    def seek(g, state):
        end = state[0]
        after = end + kept[g]
        out = [after]
        for j in range(TRAJS):
            p = owner * TRAJS + j
            here = (p >= end) & (p < after)
            out.append(jnp.where(here, end, state[1 + 2 * j]))
            out.append(jnp.where(here, kept[g], state[2 + 2 * j]))
        return tuple(out)

    state = lax.fori_loop(0, kept.shape[0], seek, (jnp.int32(0),) + (jnp.int32(0), jnp.int32(1)) * TRAJS)
    gains = []
    for j in range(TRAJS):
        begin, count = state[1 + 2 * j], state[2 + 2 * j]

        def add(q, sums):
            rank = rank_of(q)
            return sums[0] + rank, sums[1] + rank * rank

        first, second = lax.fori_loop(begin, begin + count, add, (jnp.int32(0), jnp.int32(0)))

        def row(value):
            return jnp.full((1, 128), value, jnp.int32).astype(f32)

        counts = row(count)
        deviation = jnp.sqrt(row(count * second - first * first)) / counts
        gains.append((row(rank_of(owner * TRAJS + j)) - row(first) / counts) / jnp.maximum(deviation, 1.0))
    return gains


NEAR = (-5, -4, -3, -2, -1, 1, 2, 3)
SEQ_VALUES = 4096
UNITS = 384
SMEM = pl.BlockSpec(memory_space=pltpu.SMEM)
VMEM = pl.BlockSpec(memory_space=pltpu.VMEM)
HBM = pl.BlockSpec(memory_space=pltpu.HBM)


def wide_add(*parts):
    total = parts[0].astype(f32)
    for part in parts[1:]:
        total = total + part.astype(f32)
    return total


def call(kernel, shapes, count, limit=6, **kw):
    return pl.pallas_call(
        kernel,
        out_shape=tuple(jax.ShapeDtypeStruct(shape, dtype) for shape, dtype in shapes),
        in_specs=[VMEM] * count,
        out_specs=(VMEM,) * len(shapes),
        compiler_params=pltpu.CompilerParams(vmem_limit_bytes=limit << 20),
        **kw,
    )


def fold_kernel(mine, got, out):
    y = position()[2]
    for k in range(4):
        out[(y + k) % 4] = (mine[k].astype(f32) + got[k].astype(f32)).astype(bf16)


def close_kernel(ranks, parts, out):
    width = parts.shape[2]
    col = lax.broadcasted_iota(jnp.int32, (16, 128), 1)
    row = lax.broadcasted_iota(jnp.int32, (16, 128), 0)
    values = jnp.zeros((16, 128), jnp.int32)
    for i in range(ranks.shape[0]):
        values = jnp.where(col == i, ranks[i], values)
    values = jnp.where(row == 0, values // 32, jnp.where(row == 1, values % 32, 0)).astype(f32).astype(bf16)
    total = parts[0].astype(f32)
    for k in range(1, 4):
        total = total + parts[k].astype(f32)
    total = total.astype(bf16)
    for k in range(4):
        out[k, :, pl.ds(0, width)] = total
        out[k, :, pl.ds(width, 128)] = jnp.zeros((out.shape[1], 128), bf16)
        out[k, pl.ds(0, 16), pl.ds(width, 128)] = values


def sum_kernel(parts, out):
    total = parts[0].astype(f32)
    for k in range(1, parts.shape[0]):
        total = total + parts[k].astype(f32)
    out[...] = total.astype(out.dtype)


def swapped(value, axis):
    return lax.all_to_all(value, axis, 0, 0, tiled=True)


def half_add_kernel(part, recv, out, *, lead):
    n = recv.shape[1]
    total = (part[0, :, pl.ds(lead * n, n)].astype(f32) + recv[...].astype(f32)).astype(bf16)
    out[:, pl.ds(lead * n, n)] = total
    out[:, pl.ds((1 - lead) * n, n)] = part[0, :, pl.ds((1 - lead) * n, n)]


def half_add(parts, index, recv, lead):
    block = parts.shape[1:]
    return pl.pallas_call(
        lambda *refs: half_add_kernel(*refs, lead=lead),
        grid=(1,),
        out_shape=jax.ShapeDtypeStruct(block, bf16),
        in_specs=[
            pl.BlockSpec((1, *block), lambda i: (index, 0, 0)),
            pl.BlockSpec(recv.shape, lambda i: (0, 0)),
        ],
        out_specs=pl.BlockSpec(block, lambda i: (0, 0)),
        compiler_params=pltpu.CompilerParams(vmem_limit_bytes=6 << 20),
        name="ring_second",
    )(parts, recv)


def ring_of_eight(parts, low, high, third, fourth):
    def both(down, up, beside=lambda: ()):
        down, up = move(down, "z", -1), move(up, "z", 1)
        return lax.optimization_barrier((down, up, beside()))

    from_up, from_down, _ = both(low, high)
    down = half_add(parts, 5, from_up, 0)
    up = half_add(parts, 3, from_down, 1)
    from_up, from_down, _ = both(down, up)
    down = wide_add(parts[6], from_up).astype(bf16)
    up = wide_add(parts[2], from_down).astype(bf16)
    from_up, from_down, ready = both(down, up, third)
    down = wide_add(parts[7], from_up).astype(bf16)
    up = wide_add(parts[1], from_down).astype(bf16)
    return both(down, up, lambda: fourth(ready))


def turn_kernel(part, from_up, from_down, out):
    n = out.shape[2] // 2
    own = out.shape[1] - TILE

    def summed(rows):
        return part[0, rows, :].astype(f32) + from_up[rows, :].astype(f32) + from_down[rows, :].astype(f32)

    loss = jnp.sum(jnp.sum(summed(pl.ds(4 * own, TILE))[:, :128], axis=1, keepdims=True), axis=0, keepdims=True)
    loss_rows = in_three(jnp.broadcast_to(loss, (1, 128)), position()[1])
    for k in range(4):
        out[k, pl.ds(0, own), :] = summed(pl.ds(k * own, own)).astype(bf16)
        out[k, pl.ds(own, TILE), pl.ds(0, n)] = loss_rows
        out[k, pl.ds(own, TILE), pl.ds(n, n)] = jnp.zeros_like(loss_rows)


def last_kernel(parts, grad, loss):
    own = grad.shape[0]
    total = parts[0].astype(f32)
    for k in range(1, 4):
        total = total + parts[k].astype(f32)
    grad[...] = total[:own]
    found = jnp.sum(jnp.sum(total[own:, :128], axis=1, keepdims=True), axis=0, keepdims=True)
    loss[...] = jnp.broadcast_to(found * (1.0 / UNITS), loss.shape)


def spread_kernel(parts, down, up, further, keep):
    z = position()[0]
    for k in range(8):
        block = (z + k) % 8
        total = parts[0, block].astype(f32)
        for j in range(1, 4):
            total = total + parts[j, block].astype(f32)
        total = total.astype(bf16)
        if k in (7, 5):
            down[(7, 5).index(k)] = total
        elif k in (1, 3):
            up[(1, 3).index(k)] = total
        elif k == 4:
            further[...] = total
        else:
            keep[{0: 0, 2: 1, 6: 2}[k]] = total


def meet_kernel(keep, from_up, from_down, from_further, down, up, own):
    up[...] = (keep[1].astype(f32) + from_down[1].astype(f32)).astype(bf16)
    down[...] = (keep[2].astype(f32) + from_up[1].astype(f32) + from_further[...].astype(f32)).astype(bf16)
    own[...] = keep[0].astype(f32) + from_up[0].astype(f32) + from_down[0].astype(f32)


def finish_kernel(own, late_up, late_down, out):
    out[...] = own[...] + late_up[...].astype(f32) + late_down[...].astype(f32)


def shards(
    latents,
    noise,
    behavior_velocity,
    timestep,
    reward_rank_integer,
    surviving_source_index,
    surviving_slot_index,
    group_kept_count,
    patch_input_weight,
    modulation_lookup,
    up_projection_weight,
    down_projection_weight,
    velocity_head_weight,
):
    ranks_dp = lax.axis_size(DP)
    surviving = surviving_source_index.shape[0]
    trajs = surviving // ranks_dp
    steps = timestep.shape[1]
    capacity = latents.shape[0]

    def pairs(a):
        return a.reshape(capacity, steps, 32, 128).transpose(0, 2, 1, 3).reshape(capacity, 64, 128)

    width = patch_input_weight.shape[1]
    rows = 8 * 2 * trajs * 8
    one = jax.ShapeDtypeStruct((TRAJS, 80, 128), bf16)
    two = jax.ShapeDtypeStruct((TRAJS, 2, PAIRS, 128), bf16)
    out_first, out_second, own_first, own_second = pl.pallas_call(
        gather_kernel,
        out_shape=(one, two, one, two),
        in_specs=[SMEM, SMEM, HBM, HBM, HBM],
        out_specs=(VMEM, VMEM, VMEM, VMEM),
        scratch_shapes=[pltpu.SemaphoreType.DMA((6 * TRAJS,))],
        name="gather_slots",
    )(
        surviving_slot_index, timestep.T,
        pairs(latents), pairs(noise), pairs(behavior_velocity),
    )
    onward = [(i, i + 1) for i in range(ranks_dp - 1)]
    near = [
        ((d + hop) * 8 + f, d * 8 + f) for d in range(ranks_dp) for f, hop in enumerate(NEAR) if 0 <= d + hop < ranks_dp
    ]
    near_ranks = lax.ppermute(reward_rank_integer, ("z", "x", "y", "c"), near)
    far_ranks = lax.ppermute(reward_rank_integer, DP, [(d + 4, d) for d in range(ranks_dp - 4)])
    came = lax.ppermute(out_first, DP, onward)
    came_late = lax.ppermute(out_second, DP, onward)
    hidden = up_projection_weight.shape[1]
    half = rows // 2
    tokens, stamps, modulated, activated, bend, proj_other, proj_own = pl.pallas_call(
        forward_kernel,
        out_shape=(
            jax.ShapeDtypeStruct((CHUNKS * BLOCK, 128), bf16),
            jax.ShapeDtypeStruct((BLOCK, 128), f32),
            jax.ShapeDtypeStruct((rows, width), bf16),
            jax.ShapeDtypeStruct((rows, hidden), bf16),
            jax.ShapeDtypeStruct((rows, hidden), bf16),
            jax.ShapeDtypeStruct((half, width), bf16),
            jax.ShapeDtypeStruct((half, width), bf16),
        ),
        in_specs=[SMEM, VMEM, VMEM, HBM, HBM, HBM, HBM],
        out_specs=(VMEM, VMEM, HBM, HBM, HBM, HBM, HBM),
        scratch_shapes=[
            pltpu.VMEM(patch_input_weight.shape, bf16),
            pltpu.VMEM(modulation_lookup.shape, f32),
            pltpu.VMEM((TRAJS * 80, 128), f32),
            pltpu.VMEM((CHUNKS * BLOCK, 128), f32),
            pltpu.VMEM((2, 128, width), bf16),
            pltpu.VMEM((2, CHUNKS * BLOCK, width), f32),
            pltpu.VMEM((BLOCK, width), f32),
            pltpu.VMEM((BLOCK, width), f32),
            pltpu.VMEM((width, hidden), bf16),
            pltpu.VMEM((width, hidden), bf16),
            pltpu.VMEM((rows, width), bf16),
            pltpu.VMEM((rows, hidden), bf16),
            pltpu.VMEM((rows, hidden), bf16),
            pltpu.VMEM((rows, width), bf16),
            pltpu.SemaphoreType.DMA((9,)),
        ],
        compiler_params=pltpu.CompilerParams(vmem_limit_bytes=60 << 20),
        name="forward",
    )(surviving_source_index, came, own_first, patch_input_weight, modulation_lookup, up_projection_weight, down_projection_weight)
    got = swap(proj_other, "c", 1)
    piece = rows // 8
    (folded,) = call(fold_kernel, [((4, piece, width), bf16)], 2, name="fold")(
        proj_own.reshape(4, piece, width), got.reshape(4, piece, width)
    )
    gathered = swapped(folded, "y")
    gathered, came_late, near_ranks, far_ranks = lax.optimization_barrier((gathered, came_late, near_ranks, far_ranks))
    closed = pl.pallas_call(
        close_kernel,
        out_shape=jax.ShapeDtypeStruct((4, piece, width + 128), bf16),
        in_specs=[SMEM, VMEM],
        out_specs=VMEM,
        compiler_params=pltpu.CompilerParams(vmem_limit_bytes=6 << 20),
        name="close",
    )(near_ranks, gathered)
    summed_own = swapped(closed, "y")
    summed_other = swap(summed_own, "c", 1)
    own_rows = width // ranks_dp
    m = hidden // 2
    share = 4 * own_rows
    down_parts, down_low, down_high, up_parts = pl.pallas_call(
        backward_kernel,
        out_shape=(
            jax.ShapeDtypeStruct((8, share + TILE, hidden), bf16),
            jax.ShapeDtypeStruct((share + TILE, m), bf16),
            jax.ShapeDtypeStruct((share + TILE, m), bf16),
            jax.ShapeDtypeStruct((4, 8, own_rows, hidden), bf16),
        ),
        in_specs=[SMEM] * 5 + [VMEM] * 6 + [HBM, VMEM, HBM] + [HBM] * 4,
        out_specs=(HBM,) * 4,
        scratch_shapes=[
            pltpu.VMEM(patch_input_weight.shape, bf16),
            pltpu.VMEM(modulation_lookup.shape, f32),
            pltpu.VMEM((CHUNKS * BLOCK, 128), f32),
            pltpu.VMEM((CHUNKS * BLOCK, 128), f32),
            pltpu.VMEM((2, 128, width), bf16),
            pltpu.VMEM((2, 128, width), bf16),
            pltpu.VMEM((2, CHUNKS * BLOCK, width), f32),
            pltpu.VMEM((2, CHUNKS * BLOCK, width), bf16),
            pltpu.VMEM((2, CHUNKS * BLOCK, width), f32),
            pltpu.VMEM((2, CHUNKS * BLOCK, 128), f32),
            pltpu.VMEM((BLOCK, width), f32),
            pltpu.VMEM((CHUNKS * BLOCK, 128), f32),
            pltpu.VMEM((BLOCK, 128), f32),
            pltpu.VMEM((BLOCK, 128), f32),
            pltpu.VMEM((8, 128), jnp.int32),
            pltpu.SMEM((8, 128), jnp.int32),
            pltpu.VMEM((rows, hidden), bf16),
            pltpu.VMEM((rows, hidden), bf16),
            pltpu.VMEM((rows, width), bf16),
            pltpu.VMEM((width, hidden), bf16),
            pltpu.VMEM((rows, width), bf16),
            pltpu.VMEM((8, share + TILE, hidden), bf16),
            pltpu.VMEM((share + TILE, m), bf16),
            pltpu.VMEM((share + TILE, m), bf16),
            pltpu.VMEM((4, 8, own_rows, hidden), bf16),
            pltpu.SemaphoreType.DMA((12,)),
            pltpu.SemaphoreType.DMA((4,)),
        ],
        compiler_params=pltpu.CompilerParams(vmem_limit_bytes=60 << 20),
        name="backward",
    )(
        reward_rank_integer, far_ranks, surviving_source_index, surviving_slot_index, group_kept_count,
        summed_other, summed_own, tokens, stamps, came_late, own_second,
        patch_input_weight, velocity_head_weight.T, modulation_lookup,
        activated, bend, modulated, down_projection_weight,
    )

    up_gathered = swapped(up_parts, "x")

    chunk = (own_rows, hidden)

    def spread(gathered):
        down, up, further, keep = call(
            spread_kernel,
            [((2, *chunk), bf16), ((2, *chunk), bf16), (chunk, bf16), ((3, *chunk), bf16)],
            1,
            limit=60,
            name="spread",
        )(gathered)
        return keep, move(down, "z", -1), move(up, "z", 1), move(further, "z", -2)

    from_z_up, from_z_down, (keep, from_up, from_down, from_further) = ring_of_eight(
        down_parts, down_low, down_high, lambda: up_gathered, spread
    )
    down, up, kept = call(meet_kernel, [(chunk, bf16), (chunk, bf16), (chunk, f32)], 4, limit=60, name="meet")(
        keep, from_up, from_down, from_further
    )
    from_z_up, from_z_down, down, up = lax.optimization_barrier((from_z_up, from_z_down, down, up))
    tall = share + TILE
    short = own_rows + TILE
    turned = pl.pallas_call(
        turn_kernel,
        grid=(1,),
        out_shape=jax.ShapeDtypeStruct((4, short, hidden), bf16),
        in_specs=[
            pl.BlockSpec((1, tall, hidden), lambda i: (0, 0, 0)),
            pl.BlockSpec((tall, hidden), lambda i: (0, 0)),
            pl.BlockSpec((tall, hidden), lambda i: (0, 0)),
        ],
        out_specs=pl.BlockSpec((4, short, hidden), lambda i: (0, 0, 0)),
        compiler_params=pltpu.CompilerParams(vmem_limit_bytes=8 << 20),
        name="turn",
    )(down_parts, from_z_up, from_z_down)
    down_grad, loss = call(
        last_kernel, [((own_rows, hidden), f32), ((TILE, 128), f32)], 1, name="last"
    )(swapped(turned, "x"))
    (up_grad,) = call(finish_kernel, [(chunk, f32)], 3, name="finish")(
        kept, *lax.optimization_barrier((move(down, "z", -2), move(up, "z", 2)))
    )
    return (up_grad, down_grad, loss[0, 0])


def solution(mesh):
    finer = Mesh(mesh.devices.reshape(8, 4, 4, 2), ("z", "x", "y", "c"))
    dp, fsdp = ("z", "x"), ("y", "c")
    in_specs = (
        P(dp, None, None),
        P(dp, None, None),
        P(dp, None, None),
        P(dp, None),
        P(dp),
        P(),
        P(),
        P(),
        P(),
        P(),
        P(None, fsdp),
        P(None, fsdp),
        P(),
    )
    out_specs = (P(dp, fsdp), P(dp, fsdp), P())
    return jax.shard_map(
        shards, mesh=finer, in_specs=in_specs, out_specs=out_specs, check_vma=False
    )
```

```python
import jax
import jax.numpy as jnp
from jax import lax
from jax.experimental import pallas as pl
from jax.experimental.pallas import tpu as pltpu
from jax.sharding import Mesh
from jax.sharding import PartitionSpec as P

KSTEPS = 10
DP = ("z", "x")
clip_range = 0.2
noise_level = 0.7
norm_eps = 1e-06
bf16 = jnp.bfloat16
f32 = jnp.float32


def move(value, axis, steps):
    count = lax.axis_size(axis)
    return lax.ppermute(value, axis, [(i, (i + steps) % count) for i in range(count)])


def swap(value, axis, bit):
    count = lax.axis_size(axis)
    return lax.ppermute(value, axis, [(i, i ^ bit) for i in range(count)])


TRAJS = 6
PAIRS = 64
TILE = 8
BLOCK = TRAJS * TILE
CHUNKS = 8


def position():
    z, x, y, c = (lax.axis_index(a) for a in ("z", "x", "y", "c"))
    return z, x, y, c, z * 4 + x


def chunk_owner(q):
    _, _, y, c, _ = position()
    return (y + q % 4) % 4 * 2 + (1 - c if q < 4 else c)


def gather_kernel(slot_table, stamps, latents, noise, behavior, out_first, out_second, own_first, own_second, sems):
    copies = []
    owner = position()[4]
    following = jnp.minimum(owner + 1, 31)
    slots = [slot_table[following * TRAJS + j] for j in range(TRAJS)]
    slots += [slot_table[owner * TRAJS + j] for j in range(TRAJS)]
    for j in range(2 * TRAJS):
        slot = slots[j]
        first, second = (out_first, out_second) if j < TRAJS else (own_first, own_second)
        k = j % TRAJS
        for i, (source, target) in enumerate(
            ((latents, first.at[k, pl.ds(0, PAIRS)]), (noise, second.at[k, 0]), (behavior, second.at[k, 1]))
        ):
            copy = pltpu.make_async_copy(source.at[slot], target, sems.at[3 * j + i])
            copy.start()
            copies.append(copy)
    step = lax.broadcasted_iota(jnp.int32, (16, 128), 0) % 2
    for j in range(2 * TRAJS):
        slot = slots[j]
        tile = jnp.where(step == 0, stamps[0, slot], stamps[1, slot])
        first = out_first if j < TRAJS else own_first
        first[j % TRAJS, pl.ds(PAIRS, 16), :] = tile.astype(f32).astype(bf16)
    for copy in copies:
        copy.wait()


def modulation_rows(stamp_tile, lookup, index):
    rows = jnp.zeros((TILE, lookup.shape[2]), f32)
    for k in range(KSTEPS):
        rows = jnp.where(stamp_tile == k, lookup[k, pl.ds(index, 1), :], rows)
    return rows


def widened(weight, wide):
    size = weight.shape[0]
    wide[...] = jnp.zeros(wide.shape, wide.dtype)
    wide[0, pl.ds(0, size), :] = weight[...]
    wide[1, pl.ds(size, size), :] = weight[...]


def gelu_both(v):
    k = 0.7978845608028654
    square = v * v
    t = jnp.tanh(k * (v + 0.044715 * (square * v)))
    half = 0.5 * (1.0 + t)
    return v * half, half + (0.5 * k) * v * (1.0 - t * t) * (1.0 + (3 * 0.044715) * square)


def forward_kernel(
    source, came, mine, weight_in, lookup_in, up_weight, down_weight,
    tokens, stamps, mod_out, act_out, bend_out, proj_other, proj_own,
    weight, lookup, merged, sorted_, wide, emb, scale, shift, up_w, down_w, modulated, activated, bend, proj, sems,
):
    width = weight.shape[1]
    owner = position()[4]
    load_weight = pltpu.make_async_copy(weight_in, weight, sems.at[7])
    load_lookup = pltpu.make_async_copy(lookup_in, lookup, sems.at[8])
    load_weight.start()
    load_lookup.start()
    load_up = pltpu.make_async_copy(up_weight, up_w, sems.at[0])
    load_down = pltpu.make_async_copy(down_weight, down_w, sems.at[1])
    load_up.start()
    load_down.start()
    for j in range(TRAJS):
        away = source[owner * TRAJS + j] != owner
        merged[pl.ds(j * 80, 80), :] = jnp.where(away, came[j].astype(f32), mine[j].astype(f32))
    for q in range(CHUNKS):
        at_owner = chunk_owner(q)
        for j in range(TRAJS):
            at = pl.multiple_of(j * 80 + at_owner * TILE, TILE)
            sorted_[pl.ds(q * BLOCK + j * TILE, TILE), :] = merged[pl.ds(at, TILE), :]
    tokens[...] = sorted_[...].astype(bf16)
    load_weight.wait()
    load_lookup.wait()
    widened(weight, wide)
    for j in range(TRAJS):
        stamp = merged[pl.ds(j * 80 + PAIRS, TILE), :]
        stamps[pl.ds(j * TILE, TILE), :] = stamp
        stamp = stamp[:, :1]
        shift[pl.ds(j * TILE, TILE), :] = modulation_rows(stamp, lookup, 0)
        scale[pl.ds(j * TILE, TILE), :] = 1.0 + modulation_rows(stamp, lookup, 1)
    for par in range(2):
        emb[par] = jnp.dot(tokens[...], wide[par], preferred_element_type=f32)

    def norm(q, carry):
        for par in range(2):
            values = emb[par, pl.ds(pl.multiple_of(q * BLOCK, BLOCK), BLOCK), :]
            center = values - jnp.sum(values, axis=1, keepdims=True) * (1.0 / width)
            variance = jnp.sum(center * center, axis=1, keepdims=True) * (1.0 / width)
            normed = center * lax.rsqrt(variance + norm_eps)
            at = pl.multiple_of(q * (2 * BLOCK) + par * BLOCK, BLOCK)
            modulated[pl.ds(at, BLOCK), :] = (normed * scale[...] + shift[...]).astype(bf16)
        return carry

    lax.fori_loop(0, CHUNKS, norm, 0)
    save_mod = pltpu.make_async_copy(modulated, mod_out, sems.at[2])
    save_mod.start()
    load_up.wait()
    load_down.wait()

    def hidden(r, carry):
        rows = pl.ds(pl.multiple_of(r * 192, 192), 192)
        pre = jnp.dot(modulated[rows, :], up_w[...], preferred_element_type=f32)
        value, slope = gelu_both(pre)
        value = value.astype(bf16)
        activated[rows, :] = value
        bend[rows, :] = slope.astype(bf16)
        proj[rows, :] = lax.dot_general(
            value, down_w[...], (((1,), (1,)), ((), ())), preferred_element_type=f32
        ).astype(bf16)
        return carry

    half = modulated.shape[0] // 2
    lax.fori_loop(0, 2, hidden, 0, unroll=True)
    save_other = pltpu.make_async_copy(proj.at[pl.ds(0, half)], proj_other, sems.at[3])
    save_other.start()
    lax.fori_loop(2, 4, hidden, 0, unroll=True)
    save_own = pltpu.make_async_copy(proj.at[pl.ds(half, half)], proj_own, sems.at[4])
    save_own.start()
    save_act = pltpu.make_async_copy(activated, act_out, sems.at[5])
    save_act.start()
    save_bend = pltpu.make_async_copy(bend, bend_out, sems.at[6])
    save_bend.start()
    for copy in (save_mod, save_other, save_own, save_act, save_bend):
        copy.wait()


def backward_kernel(
    ranks, far_ranks, source, slot, kept,
    other, own, tokens, stamps, came, mine, weight_in, head, lookup_in,
    act_in, bend_in, mod_in, down_in,
    down_parts, down_low, down_high, up_parts,
    weight, lookup, drawn, target, wide, wide_head, emb, rounded, back, inverse, gate, error, slope, coeff,
    table_v, table, act, bend, mod, down_w, upstream, parts, low, high, pieces,
    sems, out_sems,
):
    z, x, y, c, owner = position()
    place = (z, x)
    load_weight = pltpu.make_async_copy(weight_in, weight, sems.at[10])
    load_lookup = pltpu.make_async_copy(lookup_in, lookup, sems.at[11])
    load_weight.start()
    load_lookup.start()
    loads = [
        pltpu.make_async_copy(a, b, sems.at[i])
        for i, (a, b) in enumerate(((act_in, act), (down_in, down_w), (bend_in, bend), (mod_in, mod)))
    ]
    for copy in loads:
        copy.start()
    for q in range(CHUNKS):
        info = (other if q < 4 else own)[(q + y) % 4, pl.ds(0, 16), pl.ds(weight.shape[1], 128)].astype(f32)
        table_v[pl.ds(chunk_owner(q), 1), :] = (info[0:1] * 32.0 + info[1:2]).astype(jnp.int32)
    fetch = pltpu.make_async_copy(table_v, table, sems.at[4])
    fetch.start()
    width = weight.shape[1]
    values = SEQ_VALUES
    load_weight.wait()
    load_lookup.wait()
    widened(weight, wide)
    widened(head, wide_head)
    for j in range(TRAJS):
        stamp = stamps[pl.ds(j * TILE, TILE), :]
        gate[pl.ds(j * TILE, TILE), :] = modulation_rows(stamp[:, :1], lookup, 2)
        level = 1.0 - stamp * (1.0 / KSTEPS)
        coeff[pl.ds(j * TILE, TILE), :] = (
            jnp.sqrt((1.0 / KSTEPS) * (1.0 - level + 1.0 / KSTEPS) / level) / noise_level
        )
        away = source[owner * TRAJS + j] != owner
        picked = jnp.where(away, came[j].astype(f32), mine[j].astype(f32))
        emb[0, pl.ds(0, PAIRS), pl.ds(0, 128)] = picked[0]
        emb[0, pl.ds(PAIRS, PAIRS), pl.ds(0, 128)] = picked[1]
        for q in range(CHUNKS):
            at = pl.multiple_of(chunk_owner(q) * TILE, TILE)
            drawn[pl.ds(q * BLOCK + j * TILE, TILE), :] = emb[0, pl.ds(at, TILE), pl.ds(0, 128)]
            at = pl.multiple_of(PAIRS + chunk_owner(q) * TILE, TILE)
            target[pl.ds(q * BLOCK + j * TILE, TILE), :] = emb[0, pl.ds(at, TILE), pl.ds(0, 128)]
    for par in range(2):
        emb[par] = jnp.dot(tokens[...], wide[par], preferred_element_type=f32)

    def forward(q, summed):
        for par in range(2):
            rows = pl.ds(pl.multiple_of(q * BLOCK, BLOCK), BLOCK)
            mixed = emb[par, rows, :] + gate[...] * summed[
                (q + y) % 4, pl.ds(par * BLOCK, BLOCK), pl.ds(0, width)
            ].astype(f32)
            center = mixed - jnp.sum(mixed, axis=1, keepdims=True) * (1.0 / width)
            variance = jnp.sum(center * center, axis=1, keepdims=True) * (1.0 / width)
            scale = lax.rsqrt(variance + norm_eps)
            final = center * scale
            emb[par, rows, :] = final
            rounded[par, rows, :] = final.astype(bf16)
            inverse[par, rows, :] = jnp.broadcast_to(scale, (BLOCK, 128))

    def first_half(q, carry):
        forward(q, other)
        return carry

    def second_half(q, carry):
        forward(q + 4, own)
        return carry

    lax.fori_loop(0, 4, first_half, 0)
    lax.fori_loop(0, 4, second_half, 0)
    across = (((1,), (1,)), ((), ()))
    velocity = lax.dot_general(rounded[0], wide_head[0], across, preferred_element_type=f32)
    velocity = velocity + lax.dot_general(rounded[1], wide_head[1], across, preferred_element_type=f32)
    error[...] = velocity - target[...]
    total = jnp.zeros((BLOCK, 128), f32)
    c = coeff[...]
    for q in range(CHUNKS):
        rows = pl.ds(q * BLOCK, BLOCK)
        err = error[rows, :]
        total = total + c * drawn[rows, :] * err + 0.5 * c * c * err * err
    sums = jnp.broadcast_to(jnp.sum(total, axis=1, keepdims=True), (BLOCK, 128))
    losses = jnp.zeros((TILE, 128), f32)
    fetch.wait()
    gains = advantages(table, ranks, far_ranks, source, slot, kept, owner)
    for j in range(TRAJS):
        unit = sums[j * TILE : (j + 1) * TILE]
        unit = unit + pltpu.roll(unit, 4, 0)
        unit = unit + pltpu.roll(unit, 2, 0)
        ratio = jnp.exp(-unit / values)
        clipped = jnp.clip(ratio, 1.0 - clip_range, 1.0 + clip_range)
        plain = ratio * gains[j]
        bounded = clipped * gains[j]
        losses = losses - jnp.minimum(plain, bounded)
        live = jnp.where(plain <= bounded, 1.0, 0.0)
        slope[pl.ds(j * TILE, TILE), :] = -gains[j] * ratio * live * (1.0 / UNITS)
    total = losses[0:1] + losses[1:2]
    loss_rows = in_three(total, place[0])
    bent = slope[...]
    for q in range(CHUNKS):
        rows = pl.ds(q * BLOCK, BLOCK)
        error[rows, :] = bent * (-(c * drawn[rows, :] + c * c * error[rows, :]) / values)
    dvelocity = error[...].astype(bf16)
    for par in range(2):
        back[par] = jnp.dot(dvelocity, wide_head[par], preferred_element_type=f32)

    def backward(q, carry):
        for par in range(2):
            rows = pl.ds(pl.multiple_of(q * BLOCK, BLOCK), BLOCK)
            d = back[par, rows, :]
            final = emb[par, rows, :]
            mean = jnp.sum(d, axis=1, keepdims=True) * (1.0 / width)
            along = jnp.sum(d * final, axis=1, keepdims=True) * (1.0 / width)
            dmixed = inverse[par, rows, :][:, :1] * (d - mean - final * along)
            at = pl.multiple_of(q * (2 * BLOCK) + par * BLOCK, BLOCK)
            upstream[pl.ds(at, BLOCK), :] = (gate[...] * dmixed).astype(bf16)
        return carry

    lax.fori_loop(0, CHUNKS, backward, 0)
    loads[0].wait()
    tokens_all, hidden = act.shape
    n = hidden // 2
    share = width // 8
    contract = (((0,), (0,)), ((), ()))
    low[pl.ds(share, TILE), :] = loss_rows
    high[pl.ds(share, TILE), :] = jnp.zeros_like(loss_rows)
    for k in range(8):
        parts[k, pl.ds(share, TILE), pl.ds(0, n)] = loss_rows
        parts[k, pl.ds(share, TILE), pl.ds(n, n)] = jnp.zeros_like(loss_rows)

    def down_block(i, carry):
        cols = pl.ds(pl.multiple_of(i * 2 * share, 128), 2 * share)
        total = lax.dot_general(upstream[:, cols], act[...], contract, preferred_element_type=f32).astype(bf16)
        for j in range(2):
            k = (2 * i + j + 8 - place[0]) % 8
            piece = total[j * share : (j + 1) * share]
            parts[k, pl.ds(0, share), :] = piece

            @pl.when(k == 4)
            def _():
                low[pl.ds(0, share), :] = piece[:, :n]
                high[pl.ds(0, share), :] = piece[:, n:]

        return carry

    lax.fori_loop(0, 4, down_block, 0)
    saves = [
        pltpu.make_async_copy(a, b, sems.at[5 + i])
        for i, (a, b) in enumerate(((low, down_low), (high, down_high), (parts, down_parts)))
    ]
    for copy in saves:
        copy.start()
    for copy in loads[1:]:
        copy.wait()

    def bent_rows(r, carry):
        rows = pl.ds(pl.multiple_of(r * 192, 192), 192)
        d = jnp.dot(upstream[rows, :], down_w[...], preferred_element_type=f32)
        bend[rows, :] = (d * bend[rows, :].astype(f32)).astype(bf16)
        return carry

    lax.fori_loop(0, tokens_all // 192, bent_rows, 0, unroll=2)
    quarter = share // 4

    def save_pieces(i):
        rows = pl.ds(2 * i, 2)
        return pltpu.make_async_copy(pieces.at[:, rows], up_parts.at[:, rows], out_sems.at[i])

    def up_block(i, carry):
        cols = pl.ds(pl.multiple_of(i * 2 * share, 128), 2 * share)
        total = lax.dot_general(mod[:, cols], bend[...], contract, preferred_element_type=f32).astype(bf16)
        for j in range(8):
            pieces[j % 4, 2 * i + j // 4] = total[j * quarter : (j + 1) * quarter]
        save_pieces(i).start()
        return carry

    lax.fori_loop(0, 4, up_block, 0)
    for i in range(4):
        save_pieces(i).wait()
    for copy in saves:
        copy.wait()


def in_three(value, lane):
    rows = jnp.broadcast_to(value, (TILE, 128))
    first = rows.astype(bf16).astype(f32)
    second = (rows - first).astype(bf16).astype(f32)
    third = (rows - first - second).astype(bf16).astype(f32)
    row = lax.broadcasted_iota(jnp.int32, (TILE, 128), 0)
    col = lax.broadcasted_iota(jnp.int32, (TILE, 128), 1)
    chosen = jnp.where(row == 0, first, jnp.where(row == 1, second, jnp.where(row == 2, third, 0.0)))
    tile = jnp.where(col == lane, chosen, 0.0)
    return jnp.concatenate([tile, jnp.zeros((TILE, 384), f32)], axis=1).astype(bf16)


def advantages(table, ranks, far_ranks, source, slot, kept, owner):
    def rank_of(p):
        d = source[p] - owner
        s = slot[p]
        f = jnp.clip(jnp.where(d < 0, d + 5, d + 4), 0, 7)
        return jnp.where(d == 0, ranks[s], jnp.where(d == 4, far_ranks[s], table[f, s]))

    def seek(g, state):
        end = state[0]
        after = end + kept[g]
        out = [after]
        for j in range(TRAJS):
            p = owner * TRAJS + j
            here = (p >= end) & (p < after)
            out.append(jnp.where(here, end, state[1 + 2 * j]))
            out.append(jnp.where(here, kept[g], state[2 + 2 * j]))
        return tuple(out)

    state = lax.fori_loop(0, kept.shape[0], seek, (jnp.int32(0),) + (jnp.int32(0), jnp.int32(1)) * TRAJS)
    gains = []
    for j in range(TRAJS):
        begin, count = state[1 + 2 * j], state[2 + 2 * j]

        def add(q, sums):
            rank = rank_of(q)
            return sums[0] + rank, sums[1] + rank * rank

        first, second = lax.fori_loop(begin, begin + count, add, (jnp.int32(0), jnp.int32(0)))

        def row(value):
            return jnp.full((1, 128), value, jnp.int32).astype(f32)

        counts = row(count)
        deviation = jnp.sqrt(row(count * second - first * first)) / counts
        gains.append((row(rank_of(owner * TRAJS + j)) - row(first) / counts) / jnp.maximum(deviation, 1.0))
    return gains


NEAR = (-5, -4, -3, -2, -1, 1, 2, 3)
SEQ_VALUES = 4096
UNITS = 384
SMEM = pl.BlockSpec(memory_space=pltpu.SMEM)
VMEM = pl.BlockSpec(memory_space=pltpu.VMEM)
HBM = pl.BlockSpec(memory_space=pltpu.HBM)


def wide_add(*parts):
    total = parts[0].astype(f32)
    for part in parts[1:]:
        total = total + part.astype(f32)
    return total


def call(kernel, shapes, count, **kw):
    return pl.pallas_call(
        kernel,
        out_shape=tuple(jax.ShapeDtypeStruct(shape, dtype) for shape, dtype in shapes),
        in_specs=[VMEM] * count,
        out_specs=(VMEM,) * len(shapes),
        compiler_params=pltpu.CompilerParams(vmem_limit_bytes=6 << 20),
        **kw,
    )


def fold_kernel(mine, got, out):
    y = position()[2]
    for k in range(4):
        out[(y + k) % 4] = (mine[k].astype(f32) + got[k].astype(f32)).astype(bf16)


def close_kernel(ranks, parts, out):
    width = parts.shape[2]
    col = lax.broadcasted_iota(jnp.int32, (16, 128), 1)
    row = lax.broadcasted_iota(jnp.int32, (16, 128), 0)
    values = jnp.zeros((16, 128), jnp.int32)
    for i in range(ranks.shape[0]):
        values = jnp.where(col == i, ranks[i], values)
    values = jnp.where(row == 0, values // 32, jnp.where(row == 1, values % 32, 0)).astype(f32).astype(bf16)
    total = parts[0].astype(f32)
    for k in range(1, 4):
        total = total + parts[k].astype(f32)
    total = total.astype(bf16)
    for k in range(4):
        out[k, :, pl.ds(0, width)] = total
        out[k, :, pl.ds(width, 128)] = jnp.zeros((out.shape[1], 128), bf16)
        out[k, pl.ds(0, 16), pl.ds(width, 128)] = values


def sum_kernel(parts, out):
    total = parts[0].astype(f32)
    for k in range(1, parts.shape[0]):
        total = total + parts[k].astype(f32)
    out[...] = total.astype(out.dtype)


def swapped(value, axis):
    return lax.all_to_all(value, axis, 0, 0, tiled=True)


def half_add_kernel(part, recv, out, *, lead):
    n = recv.shape[1]
    total = (part[0, :, pl.ds(lead * n, n)].astype(f32) + recv[...].astype(f32)).astype(bf16)
    out[:, pl.ds(lead * n, n)] = total
    out[:, pl.ds((1 - lead) * n, n)] = part[0, :, pl.ds((1 - lead) * n, n)]


def half_add(parts, index, recv, lead):
    block = parts.shape[1:]
    return pl.pallas_call(
        lambda *refs: half_add_kernel(*refs, lead=lead),
        grid=(1,),
        out_shape=jax.ShapeDtypeStruct(block, bf16),
        in_specs=[
            pl.BlockSpec((1, *block), lambda i: (index, 0, 0)),
            pl.BlockSpec(recv.shape, lambda i: (0, 0)),
        ],
        out_specs=pl.BlockSpec(block, lambda i: (0, 0)),
        compiler_params=pltpu.CompilerParams(vmem_limit_bytes=6 << 20),
        name="ring_second",
    )(parts, recv)


def ring_of_eight(parts, low, high, third, fourth):
    def both(down, up, beside=lambda: ()):
        down, up = move(down, "z", -1), move(up, "z", 1)
        return lax.optimization_barrier((down, up, beside()))

    from_up, from_down, _ = both(low, high)
    down = half_add(parts, 5, from_up, 0)
    up = half_add(parts, 3, from_down, 1)
    from_up, from_down, _ = both(down, up)
    down = wide_add(parts[6], from_up).astype(bf16)
    up = wide_add(parts[2], from_down).astype(bf16)
    from_up, from_down, ready = both(down, up, third)
    down = wide_add(parts[7], from_up).astype(bf16)
    up = wide_add(parts[1], from_down).astype(bf16)
    return both(down, up, lambda: fourth(ready))


def turn_kernel(part, from_up, from_down, out):
    n = out.shape[2] // 2
    own = out.shape[1] - TILE

    def summed(rows):
        return part[0, rows, :].astype(f32) + from_up[rows, :].astype(f32) + from_down[rows, :].astype(f32)

    loss = jnp.sum(jnp.sum(summed(pl.ds(4 * own, TILE))[:, :128], axis=1, keepdims=True), axis=0, keepdims=True)
    loss_rows = in_three(jnp.broadcast_to(loss, (1, 128)), position()[1])
    for k in range(4):
        out[k, pl.ds(0, own), :] = summed(pl.ds(k * own, own)).astype(bf16)
        out[k, pl.ds(own, TILE), pl.ds(0, n)] = loss_rows
        out[k, pl.ds(own, TILE), pl.ds(n, n)] = jnp.zeros_like(loss_rows)


def last_kernel(parts, grad, loss):
    own = grad.shape[0]
    total = parts[0].astype(f32)
    for k in range(1, 4):
        total = total + parts[k].astype(f32)
    grad[...] = total[:own]
    found = jnp.sum(jnp.sum(total[own:, :128], axis=1, keepdims=True), axis=0, keepdims=True)
    loss[...] = jnp.broadcast_to(found * (1.0 / UNITS), loss.shape)


def spread_kernel(parts, down, up, further, keep):
    z = position()[0]
    for k in range(8):
        block = (z + k) % 8
        total = parts[0, block].astype(f32)
        for j in range(1, 4):
            total = total + parts[j, block].astype(f32)
        total = total.astype(bf16)
        if k in (7, 5):
            down[(7, 5).index(k)] = total
        elif k in (1, 3):
            up[(1, 3).index(k)] = total
        elif k == 4:
            further[...] = total
        else:
            keep[{0: 0, 2: 1, 6: 2}[k]] = total


def meet_kernel(keep, from_up, from_down, from_further, down, up, own):
    up[...] = (keep[1].astype(f32) + from_down[1].astype(f32)).astype(bf16)
    down[...] = (keep[2].astype(f32) + from_up[1].astype(f32) + from_further[...].astype(f32)).astype(bf16)
    own[...] = keep[0].astype(f32) + from_up[0].astype(f32) + from_down[0].astype(f32)


def finish_kernel(own, late_up, late_down, out):
    out[...] = own[...] + late_up[...].astype(f32) + late_down[...].astype(f32)


def shards(
    latents,
    noise,
    behavior_velocity,
    timestep,
    reward_rank_integer,
    surviving_source_index,
    surviving_slot_index,
    group_kept_count,
    patch_input_weight,
    modulation_lookup,
    up_projection_weight,
    down_projection_weight,
    velocity_head_weight,
):
    ranks_dp = lax.axis_size(DP)
    surviving = surviving_source_index.shape[0]
    trajs = surviving // ranks_dp
    steps = timestep.shape[1]
    capacity = latents.shape[0]

    def pairs(a):
        return a.reshape(capacity, steps, 32, 128).transpose(0, 2, 1, 3).reshape(capacity, 64, 128)

    width = patch_input_weight.shape[1]
    rows = 8 * 2 * trajs * 8
    one = jax.ShapeDtypeStruct((TRAJS, 80, 128), bf16)
    two = jax.ShapeDtypeStruct((TRAJS, 2, PAIRS, 128), bf16)
    out_first, out_second, own_first, own_second = pl.pallas_call(
        gather_kernel,
        out_shape=(one, two, one, two),
        in_specs=[SMEM, SMEM, HBM, HBM, HBM],
        out_specs=(VMEM, VMEM, VMEM, VMEM),
        scratch_shapes=[pltpu.SemaphoreType.DMA((6 * TRAJS,))],
        name="gather_slots",
    )(
        surviving_slot_index, timestep.T,
        pairs(latents), pairs(noise), pairs(behavior_velocity),
    )
    onward = [(i, i + 1) for i in range(ranks_dp - 1)]
    near = [
        ((d + hop) * 8 + f, d * 8 + f) for d in range(ranks_dp) for f, hop in enumerate(NEAR) if 0 <= d + hop < ranks_dp
    ]
    near_ranks = lax.ppermute(reward_rank_integer, ("z", "x", "y", "c"), near)
    far_ranks = lax.ppermute(reward_rank_integer, DP, [(d + 4, d) for d in range(ranks_dp - 4)])
    came = lax.ppermute(out_first, DP, onward)
    came_late = lax.ppermute(out_second, DP, onward)
    hidden = up_projection_weight.shape[1]
    half = rows // 2
    tokens, stamps, modulated, activated, bend, proj_other, proj_own = pl.pallas_call(
        forward_kernel,
        out_shape=(
            jax.ShapeDtypeStruct((CHUNKS * BLOCK, 128), bf16),
            jax.ShapeDtypeStruct((BLOCK, 128), f32),
            jax.ShapeDtypeStruct((rows, width), bf16),
            jax.ShapeDtypeStruct((rows, hidden), bf16),
            jax.ShapeDtypeStruct((rows, hidden), bf16),
            jax.ShapeDtypeStruct((half, width), bf16),
            jax.ShapeDtypeStruct((half, width), bf16),
        ),
        in_specs=[SMEM, VMEM, VMEM, HBM, HBM, HBM, HBM],
        out_specs=(VMEM, VMEM, HBM, HBM, HBM, HBM, HBM),
        scratch_shapes=[
            pltpu.VMEM(patch_input_weight.shape, bf16),
            pltpu.VMEM(modulation_lookup.shape, f32),
            pltpu.VMEM((TRAJS * 80, 128), f32),
            pltpu.VMEM((CHUNKS * BLOCK, 128), f32),
            pltpu.VMEM((2, 128, width), bf16),
            pltpu.VMEM((2, CHUNKS * BLOCK, width), f32),
            pltpu.VMEM((BLOCK, width), f32),
            pltpu.VMEM((BLOCK, width), f32),
            pltpu.VMEM((width, hidden), bf16),
            pltpu.VMEM((width, hidden), bf16),
            pltpu.VMEM((rows, width), bf16),
            pltpu.VMEM((rows, hidden), bf16),
            pltpu.VMEM((rows, hidden), bf16),
            pltpu.VMEM((rows, width), bf16),
            pltpu.SemaphoreType.DMA((9,)),
        ],
        compiler_params=pltpu.CompilerParams(vmem_limit_bytes=60 << 20),
        name="forward",
    )(surviving_source_index, came, own_first, patch_input_weight, modulation_lookup, up_projection_weight, down_projection_weight)
    got = swap(proj_other, "c", 1)
    piece = rows // 8
    (folded,) = call(fold_kernel, [((4, piece, width), bf16)], 2, name="fold")(
        proj_own.reshape(4, piece, width), got.reshape(4, piece, width)
    )
    gathered = swapped(folded, "y")
    gathered, came_late, near_ranks, far_ranks = lax.optimization_barrier((gathered, came_late, near_ranks, far_ranks))
    closed = pl.pallas_call(
        close_kernel,
        out_shape=jax.ShapeDtypeStruct((4, piece, width + 128), bf16),
        in_specs=[SMEM, VMEM],
        out_specs=VMEM,
        compiler_params=pltpu.CompilerParams(vmem_limit_bytes=6 << 20),
        name="close",
    )(near_ranks, gathered)
    summed_own = swapped(closed, "y")
    summed_other = swap(summed_own, "c", 1)
    own_rows = width // ranks_dp
    m = hidden // 2
    share = 4 * own_rows
    down_parts, down_low, down_high, up_parts = pl.pallas_call(
        backward_kernel,
        out_shape=(
            jax.ShapeDtypeStruct((8, share + TILE, hidden), bf16),
            jax.ShapeDtypeStruct((share + TILE, m), bf16),
            jax.ShapeDtypeStruct((share + TILE, m), bf16),
            jax.ShapeDtypeStruct((4, 8, own_rows, hidden), bf16),
        ),
        in_specs=[SMEM] * 5 + [VMEM] * 6 + [HBM, VMEM, HBM] + [HBM] * 4,
        out_specs=(HBM,) * 4,
        scratch_shapes=[
            pltpu.VMEM(patch_input_weight.shape, bf16),
            pltpu.VMEM(modulation_lookup.shape, f32),
            pltpu.VMEM((CHUNKS * BLOCK, 128), f32),
            pltpu.VMEM((CHUNKS * BLOCK, 128), f32),
            pltpu.VMEM((2, 128, width), bf16),
            pltpu.VMEM((2, 128, width), bf16),
            pltpu.VMEM((2, CHUNKS * BLOCK, width), f32),
            pltpu.VMEM((2, CHUNKS * BLOCK, width), bf16),
            pltpu.VMEM((2, CHUNKS * BLOCK, width), f32),
            pltpu.VMEM((2, CHUNKS * BLOCK, 128), f32),
            pltpu.VMEM((BLOCK, width), f32),
            pltpu.VMEM((CHUNKS * BLOCK, 128), f32),
            pltpu.VMEM((BLOCK, 128), f32),
            pltpu.VMEM((BLOCK, 128), f32),
            pltpu.VMEM((8, 128), jnp.int32),
            pltpu.SMEM((8, 128), jnp.int32),
            pltpu.VMEM((rows, hidden), bf16),
            pltpu.VMEM((rows, hidden), bf16),
            pltpu.VMEM((rows, width), bf16),
            pltpu.VMEM((width, hidden), bf16),
            pltpu.VMEM((rows, width), bf16),
            pltpu.VMEM((8, share + TILE, hidden), bf16),
            pltpu.VMEM((share + TILE, m), bf16),
            pltpu.VMEM((share + TILE, m), bf16),
            pltpu.VMEM((4, 8, own_rows, hidden), bf16),
            pltpu.SemaphoreType.DMA((12,)),
            pltpu.SemaphoreType.DMA((4,)),
        ],
        compiler_params=pltpu.CompilerParams(vmem_limit_bytes=60 << 20),
        name="backward",
    )(
        reward_rank_integer, far_ranks, surviving_source_index, surviving_slot_index, group_kept_count,
        summed_other, summed_own, tokens, stamps, came_late, own_second,
        patch_input_weight, velocity_head_weight.T, modulation_lookup,
        activated, bend, modulated, down_projection_weight,
    )

    up_gathered = swapped(up_parts, "x")

    chunk = (own_rows, hidden)

    def spread(gathered):
        down, up, further, keep = call(
            spread_kernel,
            [((2, *chunk), bf16), ((2, *chunk), bf16), (chunk, bf16), ((3, *chunk), bf16)],
            1,
            name="spread",
        )(gathered)
        return keep, move(down, "z", -1), move(up, "z", 1), move(further, "z", -2)

    from_z_up, from_z_down, (keep, from_up, from_down, from_further) = ring_of_eight(
        down_parts, down_low, down_high, lambda: up_gathered, spread
    )
    tall = share + TILE
    short = own_rows + TILE
    turned = pl.pallas_call(
        turn_kernel,
        grid=(1,),
        out_shape=jax.ShapeDtypeStruct((4, short, hidden), bf16),
        in_specs=[
            pl.BlockSpec((1, tall, hidden), lambda i: (0, 0, 0)),
            pl.BlockSpec((tall, hidden), lambda i: (0, 0)),
            pl.BlockSpec((tall, hidden), lambda i: (0, 0)),
        ],
        out_specs=pl.BlockSpec((4, short, hidden), lambda i: (0, 0, 0)),
        compiler_params=pltpu.CompilerParams(vmem_limit_bytes=8 << 20),
        name="turn",
    )(down_parts, from_z_up, from_z_down)
    down_grad, loss = call(
        last_kernel, [((own_rows, hidden), f32), ((TILE, 128), f32)], 1, name="last"
    )(swapped(turned, "x"))
    down, up, kept = call(meet_kernel, [(chunk, bf16), (chunk, bf16), (chunk, f32)], 4, name="meet")(
        keep, from_up, from_down, from_further
    )
    (up_grad,) = call(finish_kernel, [(chunk, f32)], 3, name="finish")(
        kept, *lax.optimization_barrier((move(down, "z", -2), move(up, "z", 2)))
    )
    return (up_grad, down_grad, loss[0, 0])


def solution(mesh):
    finer = Mesh(mesh.devices.reshape(8, 4, 4, 2), ("z", "x", "y", "c"))
    dp, fsdp = ("z", "x"), ("y", "c")
    in_specs = (
        P(dp, None, None),
        P(dp, None, None),
        P(dp, None, None),
        P(dp, None),
        P(dp),
        P(),
        P(),
        P(),
        P(),
        P(),
        P(None, fsdp),
        P(None, fsdp),
        P(),
    )
    out_specs = (P(dp, fsdp), P(dp, fsdp), P())
    return jax.shard_map(
        shards, mesh=finer, in_specs=in_specs, out_specs=out_specs, check_vma=False
    )
```
